32 devices in a mesh: tm: 4 (over z), space: 8 (over y, x, core).
Axes of the slice: x: 2, y: 2, z: 4, core: 2. Of those that a mesh axis runs over, the one named last changes fastest.
Arguments:
- initial: float32 [32, 256, 512], P('space'), may hold values from -6 to 6
- iterate: float32 [4, 32, 256, 512], P('tm', 'space'), may hold values from -6 to 6
- diffusivity: float32 [32, 256, 512], P('space'), may hold values from 0.25 to 1
Outputs:
- corrected: float32 [4, 32, 256, 512], P('tm', 'space')
The draws below stay inside these ranges and needn't reach their ends.
All inputs are finite; a program needn't handle non-finite values.
Results may differ from the reference program's by a relative error of at most 0.0001.
Values sent between devices are 32-bit elements; how exact they have to be, the bound alone decides.
No kernel may reach another device: no remote copies, remote signals or barrier semaphores. Data moves between devices by JAX's collectives and lax.ppermute only.
A program may use at most 128 MiB of HBM per device.

```python
import math
import jax
import jax.numpy as jnp

NY = 256
NX = 512
STEPS = 4
NZ = 32
INTERVALS = 4
N_TM = 4


def block_scale(own_key, shape, pieces, smallest, high):
    loudness, own = 1.0, jax.random.fold_in(own_key, 6)
    for position, shards_of in pieces:
        draws = jnp.exp(jax.random.uniform(jax.random.fold_in(own, position), (shards_of,), jnp.float32, smallest / len(pieces), high / len(pieces)))
        loudness = loudness * jnp.repeat(draws, shape[position] // shards_of).reshape([-1 if axis == position else 1 for axis in range(len(shape))])
    return loudness


def gaussian(own_key, shape, scale, reach, shards=(), dtype=jnp.bfloat16):
    factor_of = block_scale(own_key, shape, shards, -0.22, 0.18) if shards else 1.0
    drawn = jax.random.normal(own_key, shape, jnp.float32) * scale * factor_of
    return jnp.minimum(jnp.maximum(drawn, -reach), reach).astype(dtype)


def setup_inputs(seed: int = 0) -> dict:
    splits = jax.random.split(jax.random.key(seed), 4)
    return {
        "initial": gaussian(splits[0], (NZ, NY, NX), 1.0, 6.0, ((0, 8),), jnp.float32),
        "iterate": gaussian(splits[1], (INTERVALS, NZ, NY, NX), 1.0, 6.0, ((0, 4), (1, 8)), jnp.float32),
        "diffusivity": jnp.clip(jnp.exp(math.log(1.0) - 1.3862944 * jax.random.uniform(splits[2], (NZ, NY, NX), jnp.float32) ** block_scale(splits[2], (NZ, NY, NX), ((0, 8),), -0.2, 0.2)), 0.25, 1.0),
    }


courant = 0.15


def advance(values, diffusivity):
    center = values[1:-1]
    coeff = diffusivity[1:-1]
    flux = (coeff + diffusivity[2:]) * (values[2:] - center) + (coeff + diffusivity[:-2]) * (values[:-2] - center)
    side_values = jnp.pad(center, ((0, 0), (1, 1), (0, 0)))
    side_coeff = jnp.pad(coeff, ((0, 0), (1, 1), (0, 0)))
    flux = flux + (coeff + side_coeff[:, 2:]) * (side_values[:, 2:] - center) + (coeff + side_coeff[:, :-2]) * (side_values[:, :-2] - center)
    cross_values = jnp.pad(center, ((0, 0), (0, 0), (1, 1)))
    cross_coeff = jnp.pad(coeff, ((0, 0), (0, 0), (1, 1)))
    flux = flux + (coeff + cross_coeff[:, :, 2:]) * (cross_values[:, :, 2:] - center) + (coeff + cross_coeff[:, :, :-2]) * (cross_values[:, :, :-2] - center)
    return center + (0.5 * courant) * flux


def zpad(values):
    return jnp.pad(values, ((1, 1), (0, 0), (0, 0)))


def restrict(values):
    depth_z, depth_y, depth_x = values.shape
    return values.reshape(depth_z // 2, 2, depth_y // 2, 2, depth_x // 2, 2).mean(axis=(1, 3, 5))


def prolong(values):
    depth_z, depth_y, depth_x = values.shape
    spread = jnp.broadcast_to(values[:, None, :, None, :, None], (depth_z, 2, depth_y, 2, depth_x, 2))
    return spread.reshape(2 * depth_z, 2 * depth_y, 2 * depth_x)


def reference(initial, iterate, diffusivity):
    padded_diff = zpad(diffusivity)
    padded_coarse = zpad(restrict(diffusivity))
    error = jnp.zeros((NZ // 2, NY // 2, NX // 2), jnp.float32)
    outputs = []
    begin_state = initial
    for interval in range(N_TM):
        state = begin_state
        for number in range(STEPS):
            state = advance(zpad(state), padded_diff)
        residual = state - iterate[interval]
        error = advance(zpad(error), padded_coarse) + restrict(residual)
        outputs.append(iterate[interval] + prolong(error))
        begin_state = iterate[interval]
    return jnp.stack(outputs)
```

```python
import functools

import jax
import jax.numpy as jnp
from jax import lax
from jax.experimental import pallas as pl
from jax.experimental.pallas import tpu as pltpu
from jax.sharding import PartitionSpec as P

STEPS = 4
courant = 0.15
GAIN = 0.5 * courant
MARGIN = 16
F32 = jnp.float32
VMEM = pltpu.VMEM


def params(limit):
    return pltpu.CompilerParams(vmem_limit_bytes=limit)


def whole(count):
    return [pl.BlockSpec(memory_space=VMEM)] * count


def shape(*dims):
    return jax.ShapeDtypeStruct(dims, F32)


def split_dot(x, selection):
    high = x.astype(jnp.bfloat16)
    rest = x - high.astype(F32)
    middle = rest.astype(jnp.bfloat16)
    low = (rest - middle.astype(F32)).astype(jnp.bfloat16)
    dot = functools.partial(jnp.dot, preferred_element_type=F32)
    return dot(high, selection) + dot(middle, selection) + dot(low, selection)


def pairing(width):
    fine = lax.broadcasted_iota(jnp.int32, (width, width // 2), 0)
    coarse = lax.broadcasted_iota(jnp.int32, (width, width // 2), 1)
    return jnp.where((fine == 2 * coarse) | (fine == 2 * coarse + 1), 1.0, 0.0).astype(jnp.bfloat16)


def spreading(width):
    coarse = lax.broadcasted_iota(jnp.int32, (width // 2, width), 0)
    fine = lax.broadcasted_iota(jnp.int32, (width // 2, width), 1)
    return jnp.where((fine == 2 * coarse) | (fine == 2 * coarse + 1), 1.0, 0.0).astype(jnp.bfloat16)


def block_mean(first, second, rows_scr, select):
    rows = first.shape[0]
    lanes = split_dot(first + second, select)
    parts = []
    for j in range(lanes.shape[1] // 128):
        rows_scr[j, 0:rows, :] = lanes[:, 128 * j : 128 * j + 128]
        even = rows_scr[j, pl.ds(0, rows // 2, 2), :]
        odd = rows_scr[j, pl.ds(1, rows // 2, 2), :]
        parts.append(0.125 * (even + odd))
    return jnp.concatenate(parts, axis=1)


def tile_masks(lanes):
    sub = lax.broadcasted_iota(jnp.int32, (8, lanes), 0)
    lane = lax.broadcasted_iota(jnp.int32, (8, lanes), 1)
    return sub, lane


def weights_plane(load, store, rows, lanes, dot_low=True):
    sub, lane = tile_masks(lanes)
    tiles = rows // 8
    zero = jnp.zeros((8, lanes), F32)
    for i in range(tiles):
        c = load(0, i)
        down = load(0, i - 1) if i > 0 else zero
        up = load(0, i + 1) if i + 1 < tiles else zero
        cym = jnp.where(sub == 0, pltpu.roll(down, 1, 0), pltpu.roll(c, 1, 0))
        cyp = jnp.where(sub == 7, pltpu.roll(up, 7, 0), pltpu.roll(c, 7, 0))
        cxm = jnp.where(lane == 0, 0.0, pltpu.roll(c, 1, 1))
        cxp = jnp.where(lane == lanes - 1, 0.0, pltpu.roll(c, lanes - 1, 1))
        czm = load(-1, i)
        czp = load(1, i)
        gain = jnp.where(c > 0.0, GAIN, 0.0)
        store(0, i, 1.0 - GAIN * (6.0 * c + (cxm + cxp) + (cym + cyp) + (czm + czp)))
        wxm = gain * (c + cxm)
        wxp = gain * (c + cxp)
        wym = gain * (c + cym)
        wyp = gain * (c + cyp)
        store(1, i, jnp.where(lane == 0, 0.0, wxm))
        store(2, i, jnp.where(lane == lanes - 1, 0.0, wxp))
        store(3, i, jnp.where(sub == 0, 0.0, wym) if i == 0 else wym)
        store(4, i, jnp.where(sub == 7, 0.0, wyp) if i + 1 == tiles else wyp)
        store(5, i, gain * (c + czm))
        store(6, i, gain * (c + czp))


def step_plane(weight, load, store, rows, lanes):
    sub, _ = tile_masks(lanes)
    tiles = rows // 8
    center = load(0, 0)
    below = center
    for i in range(tiles):
        above = load(0, i + 1) if i + 1 < tiles else center
        ym = jnp.where(sub == 0, pltpu.roll(below, 1, 0), pltpu.roll(center, 1, 0))
        yp = jnp.where(sub == 7, pltpu.roll(above, 7, 0), pltpu.roll(center, 7, 0))
        xm = pltpu.roll(center, 1, 1)
        xp = pltpu.roll(center, lanes - 1, 1)
        out = weight(0, i) * center
        out = out + (weight(1, i) * xm + weight(2, i) * xp)
        out = out + (weight(3, i) * ym + weight(4, i) * yp)
        out = out + (weight(5, i) * load(-1, i) + weight(6, i) * load(1, i))
        store(i, out)
        below, center = center, above


def tile(i):
    return slice(8 * i, 8 * i + 8)


def fine_kernel(planes, flag_ref, c_ref, partner_ref, other_ref, first_ref, second_ref, own_ref, to_partner_ref, to_other_ref,
                coarse_ref, c_scr, w_scr, a_scr, b_scr, cc_scr, rows_scr, keep_scr):
    half, upper, last = flag_ref[0], flag_ref[1], flag_ref[2]
    rows, lanes = c_ref.shape[1:]
    own_rows = rows - MARGIN
    depth = 3 * planes
    select = pairing(lanes)
    at_partner = upper * (2 * planes)
    at_other = (1 - upper) * (2 * planes)
    c_scr[planes : 2 * planes] = c_ref[...]
    c_scr[pl.ds(at_partner, planes)] = partner_ref[...]
    c_scr[pl.ds(at_other, planes)] = other_ref[...]

    def weigh(z, _):
        below, above = jnp.maximum(z - 1, 0), jnp.minimum(z + 1, depth - 1)

        def load(dz, i):
            at = z if dz == 0 else (below if dz < 0 else above)
            return c_scr[at, tile(i), :]

        def store(k, i, w):
            w_scr[k, z, tile(i), :] = w

        weights_plane(load, store, rows, lanes)
        return 0

    lax.fori_loop(0, depth, weigh, 0)

    coarse_planes = depth // 2
    for q in range(coarse_planes):
        cc_scr[q] = block_mean(c_scr[2 * q], c_scr[2 * q + 1], rows_scr, select)
    coarse_rows, coarse_lanes = rows // 2, lanes // 2
    reach = planes // 2
    for q in range(reach):
        at = reach + q

        def load(dz, i):
            return cc_scr[at + dz, tile(i), :]

        def store(k, i, w):
            coarse_ref[k, q, tile(i), :] = w

        weights_plane(load, store, coarse_rows, coarse_lanes)

    for field, source in enumerate((first_ref, second_ref)):
        zeros = jnp.zeros((planes, rows, lanes), F32)
        a_scr[0:planes] = zeros
        a_scr[2 * planes :] = zeros
        b_scr[0 : planes - 1] = zeros[1:]
        b_scr[2 * planes + 1 :] = zeros[1:]
        edge = pl.multiple_of(own_rows * (1 - half), 8)
        a_scr[planes : 2 * planes, pl.ds(edge, MARGIN), :] = jnp.zeros((planes, MARGIN, lanes), F32)
        a_scr[planes : 2 * planes, pl.ds(pl.multiple_of(MARGIN * half, 8), own_rows), :] = source[...]
        kept = []
        for q in range(reach):
            kept.append(block_mean(a_scr[planes + 2 * q], a_scr[planes + 2 * q + 1], rows_scr, select))
        for number in range(STEPS):
            v_in, v_out = (a_scr, b_scr) if number % 2 == 0 else (b_scr, a_scr)

            def advance(z, _):
                below, above = jnp.maximum(z - 1, 0), jnp.minimum(z + 1, depth - 1)

                def load(dz, i):
                    at = z if dz == 0 else (below if dz < 0 else above)
                    return v_in[at, tile(i), :]

                def weight(k, i):
                    return w_scr[k, z, tile(i), :]

                def store(i, v):
                    v_out[z, tile(i), :] = v

                step_plane(weight, load, store, rows, lanes)
                return 0

            lax.fori_loop(planes - 1 - number, 2 * planes + 1 + number, advance, 0)
        result = a_scr if STEPS % 2 == 0 else b_scr
        means = [block_mean(result[2 * q], result[2 * q + 1], rows_scr, select) for q in range(coarse_planes)]

        scale = 1.0 if field == 1 else jnp.where(last == 1, 0.0, 1.0).astype(F32)
        zero = jnp.zeros((8, coarse_lanes), F32)
        for q in range(reach):
            keep_scr[q] = kept[q] * scale
        for q in range(reach):
            def load(dz, i):
                at = q + dz
                if at < 0 or at >= reach:
                    return zero
                return keep_scr[at, tile(i), :]

            def weight(k, i):
                return coarse_ref[k, q, tile(i), :]

            def store(i, v):
                own_ref[field, q, tile(i), :] = means[reach + q][8 * i : 8 * i + 8] - v

            step_plane(weight, load, store, coarse_rows, coarse_lanes)
        low_c, high_c = cc_scr[reach - 1], cc_scr[2 * reach]
        low_w = jnp.where(low_c > 0.0, GAIN * (low_c + cc_scr[reach]), 0.0)
        high_w = jnp.where(high_c > 0.0, GAIN * (high_c + cc_scr[2 * reach - 1]), 0.0)
        low = means[:reach]
        high = means[2 * reach :]
        low[-1] = low[-1] - low_w * keep_scr[0]
        high[0] = high[0] - high_w * keep_scr[reach - 1]

        @pl.when(upper == 1)
        def _():
            for q in range(reach):
                to_partner_ref[field, q] = high[q]
                to_other_ref[field, q] = low[q]

        @pl.when(upper == 0)
        def _():
            for q in range(reach):
                to_partner_ref[field, q] = low[q]
                to_other_ref[field, q] = high[q]


def edges(flag_ref, val, to_partner_ref, to_other_ref):
    upper = flag_ref[1]

    @pl.when(upper == 1)
    def _():
        to_partner_ref[0] = val[-1]
        to_other_ref[0] = val[0]

    @pl.when(upper == 0)
    def _():
        to_partner_ref[0] = val[0]
        to_other_ref[0] = val[-1]


def sum_kernel(flag_ref, own_ref, partner_ref, other_ref, val_ref, extra_ref, to_partner_ref, to_other_ref):
    val = own_ref[0] + partner_ref[0] + other_ref[0]
    val_ref[...] = val
    extra_ref[...] = own_ref[1] + partner_ref[1] + other_ref[1]
    edges(flag_ref, val, to_partner_ref, to_other_ref)


def chain_kernel(slot, flag_ref, weight_ref, val_ref, partner_ref, other_ref, extra_ref, next_ref, to_partner_ref, to_other_ref,
                 wide):
    upper = flag_ref[1]
    add = flag_ref[slot].astype(F32)
    planes, rows, lanes = val_ref.shape
    wide[1 : planes + 1] = val_ref[...]
    wide[upper * (planes + 1)] = partner_ref[0]
    wide[(1 - upper) * (planes + 1)] = other_ref[0]
    for q in range(planes):
        def load(dz, i):
            return wide[1 + q + dz, tile(i), :]

        def weight(k, i):
            return weight_ref[k, q, tile(i), :]

        def store(i, v):
            next_ref[q, tile(i), :] = v + add * extra_ref[q, tile(i), :]

        step_plane(weight, load, store, rows, lanes)
    edges(flag_ref, next_ref[...], to_partner_ref, to_other_ref)


def final_kernel(parts, overlap, iterate_ref, *refs):
    pieces, out_ref, rows_scr, fine_scr = refs[: 2 * parts], refs[2 * parts], refs[2 * parts + 1], refs[2 * parts + 2]
    planes, rows, lanes = iterate_ref.shape
    select, spread = pairing(lanes), spreading(lanes)
    own = rows // 4
    for q in range(planes // 2):
        low = sum(ref[q] for ref in pieces[1:parts]) + pieces[0][q]
        high = sum(ref[q] for ref in pieces[parts + 1 :]) + pieces[parts][q]
        both = low[own - overlap :] + high[: 2 * overlap]
        error = jnp.concatenate([low[: own - overlap], both, high[2 * overlap :]], axis=0)
        error = error - block_mean(iterate_ref[2 * q], iterate_ref[2 * q + 1], rows_scr, select)
        wide = split_dot(error, spread)
        for j in range(lanes // 128):
            column = slice(128 * j, 128 * j + 128)
            fine_scr[j, pl.ds(0, rows // 2, 2), :] = wide[:, column]
            fine_scr[j, pl.ds(1, rows // 2, 2), :] = wide[:, column]
            for part in range(2):
                out_ref[2 * q + part, :, column] = iterate_ref[2 * q + part, :, column] + fine_scr[j]


def swap_pairs(count, first):
    pairs = []
    for i in range(first, count - 1, 2):
        pairs += [(i, i + 1), (i + 1, i)]
    return pairs


def local(initial, iterate, diffusivity):
    layers, slabs = lax.axis_size("tm"), lax.axis_size("space")
    t, s = lax.axis_index("tm"), lax.axis_index("space")
    planes, all_rows, lanes = initial.shape
    assert layers % 2 == 0 and slabs % 2 == 0 and planes == STEPS
    half, group, last_group = t % 2, t // 2, layers // 2 - 1
    last = group == last_group
    own_rows = all_rows // 2
    rows = own_rows + MARGIN
    coarse_rows = rows // 2
    reach = planes // 2
    coarse_lanes = lanes // 2
    upper = 1 - s % 2

    def partner_swap(x):
        return lax.ppermute(x, "space", swap_pairs(slabs, 0))

    def other_swap(x):
        return lax.ppermute(x, "space", swap_pairs(slabs, 1))

    c = lax.dynamic_slice_in_dim(diffusivity, half * (all_rows - rows), rows, axis=1)
    c_other = other_swap(c)
    c_partner = partner_swap(c)
    to_row_partner = lax.dynamic_slice_in_dim(iterate[0], (1 - half) * own_rows, own_rows, axis=1)
    row_pairs = swap_pairs(layers, 0)
    row_pairs.remove((layers - 1, layers - 2))
    received = lax.ppermute(to_row_partner, "tm", row_pairs)
    kept = lax.dynamic_slice_in_dim(iterate[0], half * own_rows, own_rows, axis=1)
    start = lax.dynamic_slice_in_dim(initial, half * own_rows, own_rows, axis=1)
    first = jnp.where(last, start, jnp.where(half == 0, kept, received))
    second = jnp.where(last == (half == 0), kept, received)

    flags = [half, upper, last.astype(jnp.int32)]
    for number in range(1, layers):
        flags.append(jnp.where(last, number == layers - 1, number == 1).astype(jnp.int32))
    flags = jnp.stack([f.astype(jnp.int32) for f in flags])
    smem = pl.BlockSpec(memory_space=pltpu.SMEM)

    fields = shape(2, reach, coarse_rows, coarse_lanes)
    own, to_partner, to_other, weights = pl.pallas_call(
        functools.partial(fine_kernel, planes),
        out_shape=(fields, fields, fields, shape(7, reach, coarse_rows, coarse_lanes)),
        in_specs=[smem] + whole(5),
        out_specs=tuple(whole(4)),
        scratch_shapes=[
            VMEM((3 * planes, rows, lanes), F32),
            VMEM((7, 3 * planes, rows, lanes), F32),
            VMEM((3 * planes, rows, lanes), F32),
            VMEM((3 * planes, rows, lanes), F32),
            VMEM((3 * reach, coarse_rows, coarse_lanes), F32),
            VMEM((coarse_lanes // 128, rows, 128), F32),
            VMEM((reach, coarse_rows, coarse_lanes), F32),
        ],
        compiler_params=params(60 * 1024 * 1024),
        name="fine",
    )(flags, c, c_partner, c_other, first, second)

    from_other = other_swap(to_other)
    from_partner = partner_swap(to_partner)
    plane = shape(1, coarse_rows, coarse_lanes)
    block = shape(reach, coarse_rows, coarse_lanes)
    val, extra, to_partner, to_other = pl.pallas_call(
        sum_kernel,
        out_shape=(block, block, plane, plane),
        in_specs=[smem] + whole(3),
        out_specs=tuple(whole(4)),
        name="gather",
    )(flags, own, from_partner, from_other)

    low, high = [], []

    def deliver(val, number):
        for side, into in ((0, low), (1, high)):
            pairs = [(2 * last_group + side, number)]
            for p in range(last_group):
                if 2 * p + 1 + number < layers:
                    pairs.append((2 * p + side, 2 * p + 1 + number))
            into.append(lax.ppermute(val, "tm", pairs))

    deliver(val, 0)
    for number in range(1, layers):
        from_other = other_swap(to_other)
        from_partner = partner_swap(to_partner)
        val, to_partner, to_other = pl.pallas_call(
            functools.partial(chain_kernel, 2 + number),
            out_shape=(block, plane, plane),
            in_specs=[smem] + whole(5),
            out_specs=tuple(whole(3)),
            scratch_shapes=[VMEM((reach + 2, coarse_rows, coarse_lanes), F32)],
            name=f"chain{number}",
        )(flags, weights, val, from_partner, from_other, extra)
        deliver(val, number)

    corrected = pl.pallas_call(
        functools.partial(final_kernel, layers, MARGIN // 2),
        out_shape=shape(planes, all_rows, lanes),
        in_specs=whole(1 + 2 * layers),
        out_specs=pl.BlockSpec(memory_space=VMEM),
        scratch_shapes=[VMEM((coarse_lanes // 128, all_rows, 128), F32), VMEM((lanes // 128, all_rows, 128), F32)],
        compiler_params=params(40 * 1024 * 1024),
        name="final",
    )(iterate[0], *low, *high)
    return corrected[None]


def solution(mesh):
    placed = (P("space", None, None), P("tm", "space", None, None), P("space", None, None))
    return jax.shard_map(
        local, mesh=mesh, in_specs=placed, out_specs=P("tm", "space", None, None), check_vma=False
    )
```

```python
import functools

import jax
import jax.numpy as jnp
from jax import lax
from jax.experimental import pallas as pl
from jax.experimental.pallas import tpu as pltpu
from jax.sharding import PartitionSpec as P

STEPS = 4
courant = 0.15
GAIN = 0.5 * courant
MARGIN = 16
F32 = jnp.float32
VMEM = pltpu.VMEM
MIB = 1024 * 1024
VMEM_LIMITS = {"inner": 44 * MIB, "outer": 48 * MIB, "small": 10 * MIB, "final": 16 * MIB}


def params(limit):
    return pltpu.CompilerParams(vmem_limit_bytes=limit)


def whole(count):
    return [pl.BlockSpec(memory_space=VMEM)] * count


def shape(*dims):
    return jax.ShapeDtypeStruct(dims, F32)


def split_dot(x, selection):
    high = x.astype(jnp.bfloat16)
    rest = x - high.astype(F32)
    middle = rest.astype(jnp.bfloat16)
    low = (rest - middle.astype(F32)).astype(jnp.bfloat16)
    dot = functools.partial(jnp.dot, preferred_element_type=F32)
    return dot(high, selection) + dot(middle, selection) + dot(low, selection)


def pairing(width):
    fine = lax.broadcasted_iota(jnp.int32, (width, width // 2), 0)
    coarse = lax.broadcasted_iota(jnp.int32, (width, width // 2), 1)
    return jnp.where((fine == 2 * coarse) | (fine == 2 * coarse + 1), 1.0, 0.0).astype(jnp.bfloat16)


def spreading(width):
    coarse = lax.broadcasted_iota(jnp.int32, (width // 2, width), 0)
    fine = lax.broadcasted_iota(jnp.int32, (width // 2, width), 1)
    return jnp.where((fine == 2 * coarse) | (fine == 2 * coarse + 1), 1.0, 0.0).astype(jnp.bfloat16)


def block_mean(first, second, rows_scr, select):
    rows = first.shape[0]
    lanes = split_dot(first + second, select)
    parts = []
    for j in range(lanes.shape[1] // 128):
        rows_scr[j, 0:rows, :] = lanes[:, 128 * j : 128 * j + 128]
        even = rows_scr[j, pl.ds(0, rows // 2, 2), :]
        odd = rows_scr[j, pl.ds(1, rows // 2, 2), :]
        parts.append(0.125 * (even + odd))
    return jnp.concatenate(parts, axis=1)


def tile_masks(lanes):
    sub = lax.broadcasted_iota(jnp.int32, (8, lanes), 0)
    lane = lax.broadcasted_iota(jnp.int32, (8, lanes), 1)
    return sub, lane


def weights_plane(load, store, rows, lanes, dot_low=True):
    sub, lane = tile_masks(lanes)
    tiles = rows // 8
    zero = jnp.zeros((8, lanes), F32)
    for i in range(tiles):
        c = load(0, i)
        down = load(0, i - 1) if i > 0 else zero
        up = load(0, i + 1) if i + 1 < tiles else zero
        cym = jnp.where(sub == 0, pltpu.roll(down, 1, 0), pltpu.roll(c, 1, 0))
        cyp = jnp.where(sub == 7, pltpu.roll(up, 7, 0), pltpu.roll(c, 7, 0))
        cxm = jnp.where(lane == 0, 0.0, pltpu.roll(c, 1, 1))
        cxp = jnp.where(lane == lanes - 1, 0.0, pltpu.roll(c, lanes - 1, 1))
        czm = load(-1, i)
        czp = load(1, i)
        gain = jnp.where(c > 0.0, GAIN, 0.0)
        store(0, i, 1.0 - GAIN * (6.0 * c + (cxm + cxp) + (cym + cyp) + (czm + czp)))
        wxm = gain * (c + cxm)
        wxp = gain * (c + cxp)
        wym = gain * (c + cym)
        wyp = gain * (c + cyp)
        store(1, i, jnp.where(lane == 0, 0.0, wxm))
        store(2, i, jnp.where(lane == lanes - 1, 0.0, wxp))
        store(3, i, jnp.where(sub == 0, 0.0, wym) if i == 0 else wym)
        store(4, i, jnp.where(sub == 7, 0.0, wyp) if i + 1 == tiles else wyp)
        store(5, i, gain * (c + czm))
        store(6, i, gain * (c + czp))


def step_plane(weight, load, store, rows, lanes, fields=1):
    sub, _ = tile_masks(lanes)
    tiles = rows // 8
    center = [load(f, 0, 0) for f in range(fields)]
    below = list(center)
    for i in range(tiles):
        w = [weight(k, i) for k in range(7)]
        for f in range(fields):
            mid = center[f]
            above = load(f, 0, i + 1) if i + 1 < tiles else mid
            ym = jnp.where(sub == 0, pltpu.roll(below[f], 1, 0), pltpu.roll(mid, 1, 0))
            yp = jnp.where(sub == 7, pltpu.roll(above, 7, 0), pltpu.roll(mid, 7, 0))
            xm = pltpu.roll(mid, 1, 1)
            xp = pltpu.roll(mid, lanes - 1, 1)
            out = w[0] * mid
            out = out + (w[1] * xm + w[2] * xp)
            out = out + (w[3] * ym + w[4] * yp)
            out = out + (w[5] * load(f, -1, i) + w[6] * load(f, 1, i))
            store(f, i, out)
            below[f], center[f] = mid, above


def tile(i):
    return slice(8 * i, 8 * i + 8)


def at_row(value, step):
    return pl.multiple_of(value * step, 8)


def propagate(planes, flag_ref, c_scr, w_scr, a_scr, b_scr, cc_scr, cw_scr, rows_scr, keep_scr):
    last = flag_ref[2]
    depth, rows, lanes = c_scr.shape
    select = pairing(lanes)
    coarse_planes, reach = depth // 2, planes // 2
    coarse_rows, coarse_lanes = rows // 2, lanes // 2
    last_plane = depth - 1

    def weigh(z, _):
        below, above = jnp.maximum(z - 1, 0), jnp.minimum(z + 1, last_plane)

        def load(dz, i):
            at = z if dz == 0 else (below if dz < 0 else above)
            return c_scr[at, tile(i), :]

        def store(k, i, w):
            w_scr[k, z, tile(i), :] = w

        weights_plane(load, store, rows, lanes)
        return 0

    lax.fori_loop(0, depth, weigh, 0)

    def restrict_c(q, _):
        cc_scr[q] = block_mean(c_scr[2 * q], c_scr[2 * q + 1], rows_scr, select)
        return 0

    lax.fori_loop(0, coarse_planes, restrict_c, 0)
    for q in range(reach):
        def load(dz, i):
            return cc_scr[reach + q + dz, tile(i), :]

        def store(k, i, w):
            cw_scr[k, q, tile(i), :] = w

        weights_plane(load, store, coarse_rows, coarse_lanes)

    def keep(n, _):
        field, q = n // reach, n % reach
        keep_scr[n] = block_mean(
            a_scr[field, planes + 2 * q], a_scr[field, planes + 2 * q + 1], rows_scr, select
        )
        return 0

    lax.fori_loop(0, 2 * reach, keep, 0)
    for number in range(STEPS):
        v_in, v_out = (a_scr, b_scr) if number % 2 == 0 else (b_scr, a_scr)

        def advance(z, _):
            below, above = jnp.maximum(z - 1, 0), jnp.minimum(z + 1, last_plane)

            def load(f, dz, i):
                at = z if dz == 0 else (below if dz < 0 else above)
                return v_in[f, at, tile(i), :]

            def weight(k, i):
                return w_scr[k, z, tile(i), :]

            def store(f, i, v):
                v_out[f, z, tile(i), :] = v

            step_plane(weight, load, store, rows, lanes, 2)
            return 0

        lax.fori_loop(planes - 1 - number, 2 * planes + 1 + number, advance, 0)
    result = a_scr if STEPS % 2 == 0 else b_scr

    def restrict_v(n, _):
        field, q = n // coarse_planes, n % coarse_planes
        mean = block_mean(result[field, 2 * q], result[field, 2 * q + 1], rows_scr, select)
        b_scr[field, q, 0:coarse_rows, 0:coarse_lanes] = mean
        return 0

    lax.fori_loop(0, 2 * coarse_planes, restrict_v, 0)

    scale = jnp.where(last == 1, 0.0, 1.0).astype(F32)
    for q in range(reach):
        keep_scr[q] = keep_scr[q] * scale
    zero = jnp.zeros((8, coarse_lanes), F32)
    low_c, high_c = cc_scr[reach - 1], cc_scr[2 * reach]
    low_w = jnp.where(low_c > 0.0, GAIN * (low_c + cc_scr[reach]), 0.0)
    high_w = jnp.where(high_c > 0.0, GAIN * (high_c + cc_scr[2 * reach - 1]), 0.0)
    for q in range(reach):
        def load(f, dz, i):
            at = q + dz
            return zero if at < 0 or at >= reach else keep_scr[f * reach + at, tile(i), :]

        def weight(k, i):
            return cw_scr[k, q, tile(i), :]

        def store(f, i, v):
            b_scr[f, reach + q, tile(i), 0:coarse_lanes] = b_scr[f, reach + q, tile(i), 0:coarse_lanes] - v

        step_plane(weight, load, store, coarse_rows, coarse_lanes, 2)
    planes_of = []
    for f in range(2):
        mean = [b_scr[f, q, 0:coarse_rows, 0:coarse_lanes] for q in range(coarse_planes)]
        mean[reach - 1] = mean[reach - 1] - low_w * keep_scr[f * reach]
        mean[2 * reach] = mean[2 * reach] - high_w * keep_scr[f * reach + reach - 1]
        planes_of.append(mean)
    return planes_of


def place_fields(flag_ref, planes, own_at, count, row_at, first_row, iterate_ref, initial_ref, received_ref, a_scr, b_scr):
    half, last = flag_ref[0], flag_ref[2]
    a_scr[...] = jnp.zeros(a_scr.shape, F32)
    edge = jnp.zeros((2, planes - 1) + b_scr.shape[2:], F32)
    b_scr[:, 0 : planes - 1] = edge
    b_scr[:, 2 * planes + 1 :] = edge
    own = pl.ds(own_at, count)
    source = pl.ds(row_at, count)
    first_kept = (last == 0) & (half == 0)
    second_kept = (last == 1) == (half == 0)

    @pl.when(last == 1)
    def _():
        a_scr[0, planes : 2 * planes, own, :] = initial_ref[:, source, :]

    @pl.when(first_kept)
    def _():
        a_scr[0, planes : 2 * planes, own, :] = iterate_ref[:, source, :]

    @pl.when((last == 0) & (half == 1))
    def _():
        a_scr[0, planes : 2 * planes, own, :] = received_ref[...]

    @pl.when(second_kept)
    def _():
        a_scr[1, planes : 2 * planes, own, :] = iterate_ref[:, source, :]

    @pl.when(jnp.logical_not(second_kept))
    def _():
        a_scr[1, planes : 2 * planes, own, :] = received_ref[...]


def inner_kernel(planes, flag_ref, c_ref, partner_ref, other_ref, iterate_ref, initial_ref, received_ref,
                 own_ref, up_ref, down_ref, weight_ref, c_scr, w_scr, a_scr, b_scr, cc_scr, cw_scr, rows_scr, keep_scr):
    half, upper = flag_ref[0], flag_ref[1]
    rows = c_scr.shape[1]
    count = received_ref.shape[1]
    window = pl.ds(at_row(1 - half, c_ref.shape[1] - rows), rows)
    c_scr[planes : 2 * planes] = c_ref[:, window, :]
    c_scr[pl.ds(upper * (2 * planes), planes)] = partner_ref[:, window, :]
    c_scr[pl.ds((1 - upper) * (2 * planes), planes)] = other_ref[...]
    middle = iterate_ref.shape[1] // 2
    row_at = pl.multiple_of(middle - count + half * count, 8)
    place_fields(flag_ref, planes, MARGIN, count, row_at, None, iterate_ref, initial_ref, received_ref, a_scr, b_scr)
    fields = propagate(planes, flag_ref, c_scr, w_scr, a_scr, b_scr, cc_scr, cw_scr, rows_scr, keep_scr)
    reach = planes // 2
    for f, mean in enumerate(fields):
        for q in range(reach):
            down_ref[f, q] = mean[q]
            own_ref[f, q] = mean[reach + q]
            up_ref[f, q] = mean[2 * reach + q]
    weight_ref[...] = cw_scr[...]


def outer_kernel(planes, flag_ref, c_ref, partner_ref, other_ref, rest_ref, iterate_ref, initial_ref, received_ref,
                 in_own_ref, in_up_ref, in_down_ref, in_weight_ref, own_ref, to_partner_ref, to_other_ref, weight_ref,
                 c_scr, w_scr, a_scr, b_scr, cc_scr, cw_scr, rows_scr, keep_scr):
    half, upper = flag_ref[0], flag_ref[1]
    rows = c_scr.shape[1]
    count = received_ref.shape[1]
    all_rows = c_ref.shape[1]
    inner, rest = other_ref.shape[1], rest_ref.shape[1]
    shared = rows - rest
    window = pl.ds(at_row(half, all_rows - rows), rows)
    c_scr[planes : 2 * planes] = c_ref[:, window, :]
    c_scr[pl.ds(upper * (2 * planes), planes)] = partner_ref[:, window, :]
    far = pl.ds((1 - upper) * (2 * planes), planes)
    c_scr[far, pl.ds(at_row(half, shared), rest), :] = rest_ref[...]
    c_scr[far, pl.ds(at_row(1 - half, rest), shared), :] = other_ref[:, pl.ds(at_row(half, inner - shared), shared), :]
    row_at = at_row(half, iterate_ref.shape[1] - count)
    place_fields(flag_ref, planes, at_row(half, MARGIN), count, row_at, None, iterate_ref, initial_ref, received_ref,
                 a_scr, b_scr)
    fields = propagate(planes, flag_ref, c_scr, w_scr, a_scr, b_scr, cc_scr, cw_scr, rows_scr, keep_scr)
    reach = planes // 2
    outer_at = pl.ds(at_row(half, (all_rows - rows) // 2), rows // 2)
    inner_at = pl.ds(at_row(1 - half, (all_rows - inner) // 2), inner // 2)

    def put(ref, f, q, outer, inner_ref):
        ref[f, q] = jnp.zeros(ref.shape[2:], F32)
        ref[f, q, outer_at, :] = outer
        ref[f, q, inner_at, :] = ref[f, q, inner_at, :] + inner_ref[f, q]

    for f, mean in enumerate(fields):
        for q in range(reach):
            put(own_ref, f, q, mean[reach + q], in_own_ref)

    @pl.when(upper == 1)
    def _():
        for f, mean in enumerate(fields):
            for q in range(reach):
                put(to_partner_ref, f, q, mean[2 * reach + q], in_up_ref)
                put(to_other_ref, f, q, mean[q], in_down_ref)

    @pl.when(upper == 0)
    def _():
        for f, mean in enumerate(fields):
            for q in range(reach):
                put(to_partner_ref, f, q, mean[q], in_down_ref)
                put(to_other_ref, f, q, mean[2 * reach + q], in_up_ref)

    kept = inner // 2 - 8
    from_outer = all_rows // 2 - kept
    for k in range(7):
        for q in range(reach):
            weight_ref[k, q, pl.ds(at_row(1 - half, from_outer), kept), :] = in_weight_ref[k, q, pl.ds(at_row(1 - half, 8), kept), :]
            weight_ref[k, q, pl.ds(at_row(half, kept), from_outer), :] = cw_scr[k, q, pl.ds(at_row(half, 8), from_outer), :]


def edges(flag_ref, val, to_partner_ref, to_other_ref):
    upper = flag_ref[1]

    @pl.when(upper == 1)
    def _():
        to_partner_ref[0] = val[-1]
        to_other_ref[0] = val[0]

    @pl.when(upper == 0)
    def _():
        to_partner_ref[0] = val[0]
        to_other_ref[0] = val[-1]


def sum_kernel(flag_ref, own_ref, partner_ref, other_ref, val_ref, extra_ref, to_partner_ref, to_other_ref):
    val = own_ref[0] + partner_ref[0] + other_ref[0]
    val_ref[...] = val
    extra_ref[...] = own_ref[1] + partner_ref[1] + other_ref[1]
    edges(flag_ref, val, to_partner_ref, to_other_ref)


def chain_kernel(add_slot, send_slots, more, flag_ref, weight_ref, partner_ref, other_ref, extra_ref, *refs):
    earlier = refs[: more + 1]
    val_ref = earlier[-1]
    next_ref, to_partner_ref, to_other_ref = refs[more + 1 : more + 4]
    sends, wide = refs[more + 4 : -1], refs[-1]
    upper = flag_ref[1]
    add = flag_ref[add_slot].astype(F32)
    planes, rows, lanes = val_ref.shape
    wide[1 : planes + 1] = val_ref[...]
    wide[upper * (planes + 1)] = partner_ref[0]
    wide[(1 - upper) * (planes + 1)] = other_ref[0]
    for q in range(planes):
        def load(f, dz, i):
            return wide[1 + q + dz, tile(i), :]

        def weight(k, i):
            return weight_ref[k, q, tile(i), :]

        def store(f, i, v):
            next_ref[q, tile(i), :] = v + add * extra_ref[q, tile(i), :]

        step_plane(weight, load, store, rows, lanes)
    edges(flag_ref, next_ref[...], to_partner_ref, to_other_ref)
    for slot, ref in zip(send_slots, sends):
        which = flag_ref[slot]

        @pl.when(which < 0)
        def _():
            ref[...] = jnp.zeros(ref.shape, F32)

        for m, source in enumerate([*earlier, next_ref]):
            @pl.when(which == m)
            def _():
                ref[...] = source[...]


def final_kernel(slots, flag_ref, iterate_ref, *refs):
    count = len(slots)
    pieces, out_ref, rows_scr, fine_scr, error_scr = refs[:count], *refs[count:]
    planes, rows, lanes = iterate_ref.shape
    select, spread = pairing(lanes), spreading(lanes)
    piece_rows = pieces[0].shape[1]
    for q in range(planes // 2):
        error_scr[...] = -block_mean(iterate_ref[2 * q], iterate_ref[2 * q + 1], rows_scr, select)
        for slot, ref in zip(slots, pieces):
            at = pl.ds(at_row(flag_ref[slot], rows // 2 - piece_rows), piece_rows)
            error_scr[at, :] = error_scr[at, :] + ref[q]
        wide = split_dot(error_scr[...], spread)
        for j in range(lanes // 128):
            column = slice(128 * j, 128 * j + 128)
            fine_scr[j, pl.ds(0, rows // 2, 2), :] = wide[:, column]
            fine_scr[j, pl.ds(1, rows // 2, 2), :] = wide[:, column]
            for part in range(2):
                out_ref[2 * q + part, :, column] = iterate_ref[2 * q + part, :, column] + fine_scr[j]


def swap_pairs(count, first):
    pairs = []
    for i in range(first, count - 1, 2):
        pairs += [(i, i + 1), (i + 1, i)]
    return pairs


def roles(layers):
    last_group = layers // 2 - 1
    rows = []
    for t in range(layers):
        half, last = t % 2, int(t // 2 == last_group)
        adds = [int(number == (layers - 1 if last else 1)) for number in range(1, layers)]
        sends = []
        for shift in range(layers):
            k = (t + shift) % layers
            m = k if last else k - 1 - (t - half)
            sends.append(m if m >= 0 else -1)
        halves = [(t - shift) % layers % 2 for shift in range(layers)]
        rows.append([half, last, *adds, *sends, *halves])
    return rows


def local(initial, iterate, diffusivity):
    layers, slabs = lax.axis_size("tm"), lax.axis_size("space")
    t, s = lax.axis_index("tm"), lax.axis_index("space")
    planes, all_rows, lanes = initial.shape
    assert layers % 2 == 0 and slabs % 2 == 0 and planes == STEPS
    half = t % 2
    own_rows = all_rows // 2
    rows = own_rows + MARGIN
    inner_own = (3 * own_rows // 8) // 16 * 16
    outer_own = own_rows - inner_own
    inner_rows, outer_rows = inner_own + 2 * MARGIN, outer_own + MARGIN
    coarse_rows, coarse_lanes = rows // 2, lanes // 2
    reach = planes // 2
    upper = 1 - s % 2
    field = iterate[0]

    def partner_swap(x):
        return lax.ppermute(x, "space", swap_pairs(slabs, 0))

    def other_swap(x):
        return lax.ppermute(x, "space", swap_pairs(slabs, 1))

    def rows_of(x, start, count):
        return lax.dynamic_slice_in_dim(x, start, count, axis=1)

    base = half * (all_rows - rows)
    other_inner = other_swap(rows_of(diffusivity, base + (1 - half) * (rows - inner_rows), inner_rows))
    c = rows_of(diffusivity, base, rows)
    c_partner = partner_swap(c)
    row_pairs = swap_pairs(layers, 0)
    row_pairs.remove((layers - 1, layers - 2))
    got_inner = lax.ppermute(rows_of(field, own_rows - half * inner_own, inner_own), "tm", row_pairs)
    other_rest = other_swap(rows_of(diffusivity, base + half * inner_rows, rows - inner_rows))
    got_outer = lax.ppermute(rows_of(field, (1 - half) * (all_rows - outer_own), outer_own), "tm", row_pairs)

    table = roles(layers)
    mine = jnp.asarray(table, jnp.int32)[t]
    flags = jnp.concatenate([mine[:1], jnp.reshape(upper, (1,)).astype(jnp.int32), mine[1:]])
    add_at, send_at, half_at = 3, 2 + layers, 2 + 2 * layers
    smem = pl.BlockSpec(memory_space=pltpu.SMEM)

    def propagation(kernel, own, window, ins, out_rows, name):
        fields = shape(2, reach, out_rows, coarse_lanes)
        return pl.pallas_call(
            functools.partial(kernel, planes),
            out_shape=(fields, fields, fields, shape(7, reach, out_rows, coarse_lanes)),
            in_specs=[smem] + whole(len(ins)),
            out_specs=tuple(whole(4)),
            scratch_shapes=[
                VMEM((3 * planes, window, lanes), F32),
                VMEM((7, 3 * planes, window, lanes), F32),
                VMEM((2, 3 * planes, window, lanes), F32),
                VMEM((2, 3 * planes, window, lanes), F32),
                VMEM((3 * reach, window // 2, coarse_lanes), F32),
                VMEM((7, reach, window // 2, coarse_lanes), F32),
                VMEM((coarse_lanes // 128, window, 128), F32),
                VMEM((2 * reach, window // 2, coarse_lanes), F32),
            ],
            compiler_params=params(VMEM_LIMITS[name]),
            name=name,
        )(flags, *ins)

    inner = propagation(
        inner_kernel, inner_own, inner_rows, (c, c_partner, other_inner, field, initial, got_inner), inner_rows // 2, "inner"
    )
    own, to_partner, to_other, weights = propagation(
        outer_kernel, outer_own, outer_rows,
        (c, c_partner, other_inner, other_rest, field, initial, got_outer, *inner), coarse_rows, "outer",
    )

    from_other = other_swap(to_other)
    from_partner = partner_swap(to_partner)
    plane = shape(1, coarse_rows, coarse_lanes)
    block = shape(reach, coarse_rows, coarse_lanes)
    val, extra, to_partner, to_other = pl.pallas_call(
        sum_kernel,
        out_shape=(block, block, plane, plane),
        in_specs=[smem] + whole(3),
        out_specs=tuple(whole(4)),
        compiler_params=params(VMEM_LIMITS["small"]),
        name="gather",
    )(flags, own, from_partner, from_other)

    ready = [max(row[1 + layers + shift] for row in table) for shift in range(layers)]
    arrived = [None] * layers
    values = [val]
    for number in range(1, layers):
        from_other = other_swap(to_other)
        from_partner = partner_swap(to_partner)
        shifts = [shift for shift in range(layers) if max(ready[shift], 1) == number]
        earlier = values if shifts else values[-1:]
        val, to_partner, to_other, *sends = pl.pallas_call(
            functools.partial(chain_kernel, add_at + number - 1, [send_at + shift for shift in shifts], len(earlier) - 1),
            out_shape=(block, plane, plane, *[block] * len(shifts)),
            in_specs=[smem] + whole(4 + len(earlier)),
            out_specs=tuple(whole(3 + len(shifts))),
            scratch_shapes=[VMEM((reach + 2, coarse_rows, coarse_lanes), F32)],
            compiler_params=params(VMEM_LIMITS["small"]),
            name=f"chain{number}",
        )(flags, weights, from_partner, from_other, extra, *earlier)
        values.append(val)
        for shift, send in zip(shifts, sends):
            pairs = [
                (source, (source + shift) % layers)
                for source in range(layers)
                if table[source][1 + layers + shift] >= 0
            ]
            arrived[shift] = lax.ppermute(send, "tm", pairs) if shift else send

    corrected = pl.pallas_call(
        functools.partial(final_kernel, [half_at + shift for shift in range(layers)]),
        out_shape=shape(planes, all_rows, lanes),
        in_specs=[smem] + whole(1 + layers),
        out_specs=pl.BlockSpec(memory_space=VMEM),
        scratch_shapes=[
            VMEM((coarse_lanes // 128, all_rows, 128), F32),
            VMEM((lanes // 128, all_rows, 128), F32),
            VMEM((all_rows // 2, coarse_lanes), F32),
        ],
        compiler_params=params(VMEM_LIMITS["final"]),
        name="final",
    )(flags, field, *arrived)
    return corrected[None]


def solution(mesh):
    placed = (P("space", None, None), P("tm", "space", None, None), P("space", None, None))
    return jax.shard_map(
        local, mesh=mesh, in_specs=placed, out_specs=P("tm", "space", None, None), check_vma=False
    )
```

```python
import functools

import jax
import jax.numpy as jnp
from jax import lax
from jax.experimental import pallas as pl
from jax.experimental.pallas import tpu as pltpu
from jax.sharding import PartitionSpec as P

STEPS = 4
courant = 0.15
GAIN = 0.5 * courant
MARGIN = 16
F32 = jnp.float32
VMEM = pltpu.VMEM
MIB = 1024 * 1024
VMEM_LIMITS = {"fine": 51 * MIB, "small": 10 * MIB, "final": 16 * MIB}


def params(limit):
    return pltpu.CompilerParams(vmem_limit_bytes=limit)


def whole(count):
    return [pl.BlockSpec(memory_space=VMEM)] * count


def shape(*dims):
    return jax.ShapeDtypeStruct(dims, F32)


def split_dot(x, selection):
    high = x.astype(jnp.bfloat16)
    rest = x - high.astype(F32)
    middle = rest.astype(jnp.bfloat16)
    low = (rest - middle.astype(F32)).astype(jnp.bfloat16)
    dot = functools.partial(jnp.dot, preferred_element_type=F32)
    return dot(high, selection) + dot(middle, selection) + dot(low, selection)


def pairing(width):
    fine = lax.broadcasted_iota(jnp.int32, (width, width // 2), 0)
    coarse = lax.broadcasted_iota(jnp.int32, (width, width // 2), 1)
    return jnp.where((fine == 2 * coarse) | (fine == 2 * coarse + 1), 1.0, 0.0).astype(jnp.bfloat16)


def spreading(width):
    coarse = lax.broadcasted_iota(jnp.int32, (width // 2, width), 0)
    fine = lax.broadcasted_iota(jnp.int32, (width // 2, width), 1)
    return jnp.where((fine == 2 * coarse) | (fine == 2 * coarse + 1), 1.0, 0.0).astype(jnp.bfloat16)


def natural_mean(first, second, rows_scr, select):
    rows = first.shape[0]
    lanes = split_dot(first + second, select)
    parts = []
    for j in range(lanes.shape[1] // 128):
        rows_scr[j, 0:rows, :] = lanes[:, 128 * j : 128 * j + 128]
        even = rows_scr[j, pl.ds(0, rows // 2, 2), :]
        odd = rows_scr[j, pl.ds(1, rows // 2, 2), :]
        parts.append(0.125 * (even + odd))
    return jnp.concatenate(parts, axis=1)


def tile(i):
    return slice(8 * i, 8 * i + 8)


def dealt_mean(load, tiles, select):
    sums = [
        (load(0, 2 * i) + load(1, 2 * i)) + (load(0, 2 * i + 1) + load(1, 2 * i + 1)) for i in range(tiles // 2)
    ]
    return 0.125 * split_dot(jnp.concatenate(sums, axis=0), select)


def weights_plane(load, store, rows, lanes):
    sub = lax.broadcasted_iota(jnp.int32, (8, 128), 0)
    lane = lax.broadcasted_iota(jnp.int32, (8, 128), 1)
    tiles, blocks = rows // 8, lanes // 128

    def cut(x):
        return [x[:, 128 * j : 128 * j + 128] for j in range(blocks)]

    c = cut(load(0, 0))
    below = [pltpu.roll(x, 1, 0) for x in cut(load(0, tiles - 1))]
    wrapped = [pltpu.roll(x, 7, 0) for x in c]
    for i in range(tiles):
        above = cut(load(0, i + 1)) if i + 1 < tiles else wrapped
        czm, czp = cut(load(-1, i)), cut(load(1, i))
        right = [pltpu.roll(x, 1, 1) for x in c]
        left = [pltpu.roll(x, 127, 1) for x in c]
        w = [[] for _ in range(7)]
        for j in range(blocks):
            mid = c[j]
            xm = mid + jnp.where(lane == 0, right[j - 1] if j else 0.0, right[j])
            xp = mid + jnp.where(lane == 127, left[j + 1] if j + 1 < blocks else 0.0, left[j])
            ym = mid + (jnp.where(sub == 0, 0.0, below[j]) if i == 0 else below[j])
            yp = mid + (jnp.where(sub == 7, 0.0, above[j]) if i + 1 == tiles else above[j])
            zm, zp = mid + czm[j], mid + czp[j]
            w[0].append(1.0 - ((xm + xp) + (ym + yp) + (zm + zp)))
            w[1].append(xm if j else jnp.where(lane == 0, 0.0, xm))
            w[2].append(xp if j + 1 < blocks else jnp.where(lane == 127, 0.0, xp))
            w[3].append(jnp.where(sub == 0, 0.0, ym) if i == 0 else ym)
            w[4].append(jnp.where(sub == 7, 0.0, yp) if i + 1 == tiles else yp)
            inside = mid > 0.0
            w[5].append(jnp.where(inside, zm, 0.0))
            w[6].append(jnp.where(inside, zp, 0.0))
        for k in range(7):
            store(k, i, jnp.concatenate(w[k], axis=1))
        below, c = c, above


def step_plane(weight, load, store, rows, lanes, fields=1):
    tiles = rows // 8
    below = [pltpu.roll(load(f, 0, tiles - 1), 1, 0) for f in range(fields)]
    center = [load(f, 0, 0) for f in range(fields)]
    wrapped = [pltpu.roll(v, 7, 0) for v in center]
    for i in range(tiles):
        w = [weight(k, i) for k in range(7)]
        for f in range(fields):
            mid = center[f]
            above = load(f, 0, i + 1) if i + 1 < tiles else wrapped[f]
            xm = pltpu.roll(mid, 1, 1)
            xp = pltpu.roll(mid, lanes - 1, 1)
            out = w[0] * mid
            out = out + (w[1] * xm + w[2] * xp)
            out = out + (w[3] * below[f] + w[4] * above)
            out = out + (w[5] * load(f, -1, i) + w[6] * load(f, 1, i))
            store(f, i, out)
            below[f], center[f] = mid, above


def at_row(value, step):
    return pl.multiple_of(value * step, 8)


def slice_kernel(c_hbm, iterate_hbm, c_ref, send_ref, sem):
    half = lax.rem(lax.axis_index("tm"), 2)
    own = send_ref.shape[1]
    window = pl.ds(at_row(half, c_hbm.shape[1] - c_ref.shape[1]), c_ref.shape[1])
    send = pltpu.make_async_copy(iterate_hbm.at[:, pl.ds(at_row(1 - half, own), own), :], send_ref, sem.at[0])
    keep = pltpu.make_async_copy(c_hbm.at[:, window, :], c_ref, sem.at[1])
    send.start()
    keep.start()
    send.wait()
    keep.wait()


def fine_kernel(planes, flag_ref, c_hbm, partner_hbm, other_hbm, iterate_hbm, initial_hbm, received_hbm,
                own_ref, to_partner_ref, to_other_ref, coarse_ref,
                c_raw, v_raw, c_scr, w_scr, a_scr, b_scr, cc_scr, keep_scr, c_sem, v_sem):
    half, upper, last = flag_ref[0], flag_ref[1], flag_ref[2]
    depth, rows, lanes = c_scr.shape
    own_rows = rows - MARGIN
    tiles = rows // 8
    columns = [slice(128 * j, 128 * j + 128) for j in range(lanes // 128)]
    select = pairing(lanes)
    coarse_planes, reach = depth // 2, planes // 2
    coarse_rows, coarse_lanes = rows // 2, lanes // 2
    last_plane = depth - 1

    slabs = ((c_hbm, planes), (partner_hbm, upper * (2 * planes)), (other_hbm, (1 - upper) * (2 * planes)))
    c_copies = [
        pltpu.make_async_copy(ref.at[:, :, column], c_raw.at[pl.ds(at, planes), j], c_sem.at[n, j])
        for n, (ref, at) in enumerate(slabs)
        for j, column in enumerate(columns)
    ]
    for copy in c_copies:
        copy.start()
    into = pl.ds(at_row(half, MARGIN), own_rows)
    source = pl.ds(at_row(half, own_rows), own_rows)

    def fetch(ref, f):
        for j in range(len(columns)):
            pltpu.make_async_copy(ref[j], v_raw.at[f, :, j, into, :], v_sem.at[f, j]).start()

    def halves(ref):
        return [ref.at[:, source, column] for column in columns]

    received = [received_hbm.at[:, :, column] for column in columns]

    first_kept = (last == 0) & (half == 0)
    first_got = (last == 0) & (half == 1)
    second_kept = (last == 1) == (half == 0)
    for f, choices in enumerate(
        (
            ((last == 1, halves(initial_hbm)), (first_kept, halves(iterate_hbm)), (first_got, received)),
            ((second_kept, halves(iterate_hbm)), (jnp.logical_not(second_kept), received)),
        )
    ):
        for condition, ref in choices:
            @pl.when(condition)
            def _():
                fetch(ref, f)

    outside = pl.ds(at_row(1 - half, own_rows), MARGIN)
    v_raw[:, :, :, outside, :] = jnp.zeros(v_raw.shape[:3] + (MARGIN, 128), F32)
    idle = jnp.zeros((2, planes) + a_scr.shape[2:], F32)
    a_scr[:, 0:planes] = idle
    a_scr[:, 2 * planes :] = idle
    b_scr[:, 0 : planes - 1] = idle[:, 1:]
    b_scr[:, 2 * planes + 1 :] = idle[:, 1:]
    for copy in c_copies:
        copy.wait()

    def deal_c(z, _):
        for j, column in enumerate(columns):
            for i in range(tiles):
                c_scr[z, tile(i), column] = GAIN * c_raw[z, j, pl.ds(i, 8, tiles), :]
        return 0

    lax.fori_loop(0, depth, deal_c, 0)

    def weigh(z, _):
        below, above = jnp.maximum(z - 1, 0), jnp.minimum(z + 1, last_plane)

        def load(dz, i):
            at = z if dz == 0 else (below if dz < 0 else above)
            return c_scr[at, tile(i), :]

        def store(k, i, w):
            w_scr[k, z, tile(i), :] = w

        weights_plane(load, store, rows, lanes)
        return 0

    lax.fori_loop(0, depth, weigh, 0)

    def restrict_c(q, _):
        cc_scr[q] = dealt_mean(lambda dz, i: c_scr[2 * q + dz, tile(i), :], tiles, select)
        return 0

    lax.fori_loop(reach - 1, 2 * reach + 1, restrict_c, 0)
    for q in range(reach):
        def load(dz, i):
            return cc_scr[reach + q + dz, tile(i), :]

        def store(k, i, w):
            coarse_ref[k, q, tile(i), :] = w

        weights_plane(load, store, coarse_rows, coarse_lanes)

    for f in range(2):
        for j in range(len(columns)):
            pltpu.make_async_copy(received[j], v_raw.at[f, :, j, into, :], v_sem.at[f, j]).wait()

    def deal_v(z, _):
        for f in range(2):
            for j, column in enumerate(columns):
                for i in range(tiles):
                    a_scr[f, planes + z, tile(i), column] = v_raw[f, z, j, pl.ds(i, 8, tiles), :]
        return 0

    lax.fori_loop(0, planes, deal_v, 0)

    def keep(n, _):
        f, q = n // reach, n % reach
        keep_scr[n] = dealt_mean(lambda dz, i: a_scr[f, planes + 2 * q + dz, tile(i), :], tiles, select)
        return 0

    lax.fori_loop(0, 2 * reach, keep, 0)
    for number in range(STEPS):
        v_in, v_out = (a_scr, b_scr) if number % 2 == 0 else (b_scr, a_scr)

        def advance(z, _):
            below, above = jnp.maximum(z - 1, 0), jnp.minimum(z + 1, last_plane)

            def load(f, dz, i):
                at = z if dz == 0 else (below if dz < 0 else above)
                return v_in[f, at, tile(i), :]

            def weight(k, i):
                return w_scr[k, z, tile(i), :]

            def store(f, i, v):
                v_out[f, z, tile(i), :] = v

            step_plane(weight, load, store, rows, lanes, 2)
            return 0

        lax.fori_loop(planes - 1 - number, 2 * planes + 1 + number, advance, 0)
    result = a_scr if STEPS % 2 == 0 else b_scr

    scale = jnp.where(last == 1, 0.0, 1.0).astype(F32)
    for q in range(reach):
        keep_scr[q] = keep_scr[q] * scale
    zero = jnp.zeros((8, coarse_lanes), F32)
    for q in range(reach):
        def load(f, dz, i):
            at = q + dz
            return zero if at < 0 or at >= reach else keep_scr[f * reach + at, tile(i), :]

        def weight(k, i):
            return coarse_ref[k, q, tile(i), :]

        def store(f, i, v):
            own_ref[f, q, tile(i), :] = v

        step_plane(weight, load, store, coarse_rows, coarse_lanes, 2)

    def mean_of(f, q):
        return dealt_mean(lambda dz, i: result[f, 2 * q + dz, tile(i), :], tiles, select)

    low_c, high_c = cc_scr[reach - 1], cc_scr[2 * reach]
    low_w = jnp.where(low_c > 0.0, low_c + cc_scr[reach], 0.0)
    high_w = jnp.where(high_c > 0.0, high_c + cc_scr[2 * reach - 1], 0.0)
    for f in range(2):
        for q in range(reach):
            own_ref[f, q] = mean_of(f, reach + q) - own_ref[f, q]
        for q in range(reach):
            low, high = mean_of(f, q), mean_of(f, 2 * reach + q)
            if q == reach - 1:
                low = low - low_w * keep_scr[f * reach]
            if q == 0:
                high = high - high_w * keep_scr[f * reach + reach - 1]

            @pl.when(upper == 1)
            def _():
                to_partner_ref[f, q] = high
                to_other_ref[f, q] = low

            @pl.when(upper == 0)
            def _():
                to_partner_ref[f, q] = low
                to_other_ref[f, q] = high


def edges(flag_ref, val, to_partner_ref, to_other_ref):
    upper = flag_ref[1]

    @pl.when(upper == 1)
    def _():
        to_partner_ref[0] = val[-1]
        to_other_ref[0] = val[0]

    @pl.when(upper == 0)
    def _():
        to_partner_ref[0] = val[0]
        to_other_ref[0] = val[-1]


def sum_kernel(flag_ref, own_ref, partner_ref, other_ref, val_ref, extra_ref, to_partner_ref, to_other_ref):
    val = own_ref[0] + partner_ref[0] + other_ref[0]
    val_ref[...] = val
    extra_ref[...] = own_ref[1] + partner_ref[1] + other_ref[1]
    edges(flag_ref, val, to_partner_ref, to_other_ref)


def chain_kernel(add_slot, send_slots, more, flag_ref, weight_ref, partner_ref, other_ref, extra_ref, *refs):
    earlier = refs[: more + 1]
    val_ref = earlier[-1]
    next_ref, to_partner_ref, to_other_ref = refs[more + 1 : more + 4]
    sends, wide = refs[more + 4 : -1], refs[-1]
    upper = flag_ref[1]
    add = flag_ref[add_slot].astype(F32)
    planes, rows, lanes = val_ref.shape
    wide[1 : planes + 1] = val_ref[...]
    wide[upper * (planes + 1)] = partner_ref[0]
    wide[(1 - upper) * (planes + 1)] = other_ref[0]
    for q in range(planes):
        def load(f, dz, i):
            return wide[1 + q + dz, tile(i), :]

        def weight(k, i):
            return weight_ref[k, q, tile(i), :]

        def store(f, i, v):
            next_ref[q, tile(i), :] = v + add * extra_ref[q, tile(i), :]

        step_plane(weight, load, store, rows, lanes)
    edges(flag_ref, next_ref[...], to_partner_ref, to_other_ref)
    for slot, ref in zip(send_slots, sends):
        which = flag_ref[slot]

        @pl.when(which < 0)
        def _():
            ref[...] = jnp.zeros(ref.shape, F32)

        for m, source in enumerate([*earlier, next_ref]):
            @pl.when(which == m)
            def _():
                ref[...] = source[...]


def final_kernel(slots, flag_ref, iterate_ref, *refs):
    count = len(slots)
    pieces, out_ref, rows_scr, fine_scr, sum_scr, error_scr = refs[:count], *refs[count:]
    planes, rows, lanes = iterate_ref.shape
    select, spread = pairing(lanes), spreading(lanes)
    piece_rows = pieces[0].shape[1]
    tiles = piece_rows // 8
    sum_scr[...] = jnp.zeros(sum_scr.shape, F32)
    for slot, ref in zip(slots, pieces):
        side = flag_ref[slot]
        sum_scr[side] = sum_scr[side] + ref[...]
    for q in range(planes // 2):
        for j in range(lanes // 256):
            column = slice(128 * j, 128 * j + 128)
            error_scr[j] = jnp.zeros(error_scr.shape[1:], F32)
            for side in range(2):
                base = side * (rows // 2 - piece_rows)
                for i in range(tiles):
                    at = pl.ds(base + i, 8, tiles)
                    error_scr[j, at, :] = error_scr[j, at, :] + sum_scr[side, q, tile(i), column]
        error = jnp.concatenate([error_scr[j] for j in range(lanes // 256)], axis=1)
        error = error - natural_mean(iterate_ref[2 * q], iterate_ref[2 * q + 1], rows_scr, select)
        wide = split_dot(error, spread)
        for j in range(lanes // 128):
            column = slice(128 * j, 128 * j + 128)
            fine_scr[j, pl.ds(0, rows // 2, 2), :] = wide[:, column]
            fine_scr[j, pl.ds(1, rows // 2, 2), :] = wide[:, column]
            for part in range(2):
                out_ref[2 * q + part, :, column] = iterate_ref[2 * q + part, :, column] + fine_scr[j]


def swap_pairs(count, first):
    pairs = []
    for i in range(first, count - 1, 2):
        pairs += [(i, i + 1), (i + 1, i)]
    return pairs


def roles(layers):
    last_group = layers // 2 - 1
    rows = []
    for t in range(layers):
        half, last = t % 2, int(t // 2 == last_group)
        adds = [int(number == (layers - 1 if last else 1)) for number in range(1, layers)]
        sends = []
        for shift in range(layers):
            k = (t + shift) % layers
            m = k if last else k - 1 - (t - half)
            sends.append(m if m >= 0 else -1)
        halves = [(t - shift) % layers % 2 for shift in range(layers)]
        rows.append([half, last, *adds, *sends, *halves])
    return rows


def local(initial, iterate, diffusivity):
    layers, slabs = lax.axis_size("tm"), lax.axis_size("space")
    t, s = lax.axis_index("tm"), lax.axis_index("space")
    planes, all_rows, lanes = initial.shape
    assert layers % 2 == 0 and slabs % 2 == 0 and planes == STEPS
    half = t % 2
    own_rows = all_rows // 2
    rows = own_rows + MARGIN
    coarse_rows, coarse_lanes = rows // 2, lanes // 2
    last_plane = depth - 1

    slabs = ((c_hbm, planes), (partner_hbm, upper * (2 * planes)), (other_hbm, (1 - upper) * (2 * planes)))
    c_copies = [
        pltpu.make_async_copy(ref.at[:, :, column], c_raw.at[pl.ds(at, planes), j], c_sem.at[n, j])
        for n, (ref, at) in enumerate(slabs)
        for j, column in enumerate(columns)
    ]
    for copy in c_copies:
        copy.start()
    into = pl.ds(at_row(half, MARGIN), own_rows)
    source = pl.ds(at_row(half, own_rows), own_rows)

    def fetch(ref, f):
        for j in range(len(columns)):
            pltpu.make_async_copy(ref[j], v_raw.at[f, :, j, into, :], v_sem.at[f, j]).start()

    def halves(ref):
        return [ref.at[:, source, column] for column in columns]

    received = [received_hbm.at[:, :, column] for column in columns]

    first_kept = (last == 0) & (half == 0)
    first_got = (last == 0) & (half == 1)
    second_kept = (last == 1) == (half == 0)
    for f, choices in enumerate(
        (
            ((last == 1, halves(initial_hbm)), (first_kept, halves(iterate_hbm)), (first_got, received)),
            ((second_kept, halves(iterate_hbm)), (jnp.logical_not(second_kept), received)),
        )
    ):
        for condition, ref in choices:
            @pl.when(condition)
            def _():
                fetch(ref, f)

    outside = pl.ds(at_row(1 - half, own_rows), MARGIN)
    v_raw[:, :, :, outside, :] = jnp.zeros(v_raw.shape[:3] + (MARGIN, 128), F32)
    idle = jnp.zeros((2, planes) + a_scr.shape[2:], F32)
    a_scr[:, 0:planes] = idle
    a_scr[:, 2 * planes :] = idle
    b_scr[:, 0 : planes - 1] = idle[:, 1:]
    b_scr[:, 2 * planes + 1 :] = idle[:, 1:]
    for copy in c_copies:
        copy.wait()

    def deal_c(z, _):
        for j, column in enumerate(columns):
            for i in range(tiles):
                c_scr[z, tile(i), column] = GAIN * c_raw[z, j, pl.ds(i, 8, tiles), :]
        return 0

    lax.fori_loop(0, depth, deal_c, 0)

    def weigh(z, _):
        below, above = jnp.maximum(z - 1, 0), jnp.minimum(z + 1, last_plane)

        def load(dz, i):
            at = z if dz == 0 else (below if dz < 0 else above)
            return c_scr[at, tile(i), :]

        def store(k, i, w):
            w_scr[k, z, tile(i), :] = w

        weights_plane(load, store, rows, lanes)
        return 0

    lax.fori_loop(0, depth, weigh, 0)

    def restrict_c(q, _):
        cc_scr[q] = dealt_mean(lambda dz, i: c_scr[2 * q + dz, tile(i), :], tiles, select)
        return 0

    lax.fori_loop(reach - 1, 2 * reach + 1, restrict_c, 0)
    for q in range(reach):
        def load(dz, i):
            return cc_scr[reach + q + dz, tile(i), :]

        def store(k, i, w):
            coarse_ref[k, q, tile(i), :] = w

        weights_plane(load, store, coarse_rows, coarse_lanes)

    for f in range(2):
        for j in range(len(columns)):
            pltpu.make_async_copy(received[j], v_raw.at[f, :, j, into, :], v_sem.at[f, j]).wait()

    def deal_v(z, _):
        for f in range(2):
            for j, column in enumerate(columns):
                for i in range(tiles):
                    a_scr[f, planes + z, tile(i), column] = v_raw[f, z, j, pl.ds(i, 8, tiles), :]
        return 0

    lax.fori_loop(0, planes, deal_v, 0)

    def keep(n, _):
        f, q = n // reach, n % reach
        keep_scr[n] = dealt_mean(lambda dz, i: a_scr[f, planes + 2 * q + dz, tile(i), :], tiles, select)
        return 0

    lax.fori_loop(0, 2 * reach, keep, 0)
    for number in range(STEPS):
        v_in, v_out = (a_scr, b_scr) if number % 2 == 0 else (b_scr, a_scr)

        def advance(z, _):
            below, above = jnp.maximum(z - 1, 0), jnp.minimum(z + 1, last_plane)

            def load(f, dz, i):
                at = z if dz == 0 else (below if dz < 0 else above)
                return v_in[f, at, tile(i), :]

            def weight(k, i):
                return w_scr[k, z, tile(i), :]

            def store(f, i, v):
                v_out[f, z, tile(i), :] = v

            step_plane(weight, load, store, rows, lanes, 2)
            return 0

        lax.fori_loop(planes - 1 - number, 2 * planes + 1 + number, advance, 0)
    result = a_scr if STEPS % 2 == 0 else b_scr

    scale = jnp.where(last == 1, 0.0, 1.0).astype(F32)
    for q in range(reach):
        keep_scr[q] = keep_scr[q] * scale
    zero = jnp.zeros((8, coarse_lanes), F32)
    for q in range(reach):
        def load(f, dz, i):
            at = q + dz
            return zero if at < 0 or at >= reach else keep_scr[f * reach + at, tile(i), :]

        def weight(k, i):
            return coarse_ref[k, q, tile(i), :]

        def store(f, i, v):
            own_ref[f, q, tile(i), :] = v

        step_plane(weight, load, store, coarse_rows, coarse_lanes, 2)

    def mean_of(f, q):
        return dealt_mean(lambda dz, i: result[f, 2 * q + dz, tile(i), :], tiles, select)

    low_c, high_c = cc_scr[reach - 1], cc_scr[2 * reach]
    low_w = jnp.where(low_c > 0.0, low_c + cc_scr[reach], 0.0)
    high_w = jnp.where(high_c > 0.0, high_c + cc_scr[2 * reach - 1], 0.0)
    for f in range(2):
        for q in range(reach):
            own_ref[f, q] = mean_of(f, reach + q) - own_ref[f, q]
        for q in range(reach):
            low, high = mean_of(f, q), mean_of(f, 2 * reach + q)
            if q == reach - 1:
                low = low - low_w * keep_scr[f * reach]
            if q == 0:
                high = high - high_w * keep_scr[f * reach + reach - 1]

            @pl.when(upper == 1)
            def _():
                to_partner_ref[f, q] = high
                to_other_ref[f, q] = low

            @pl.when(upper == 0)
            def _():
                to_partner_ref[f, q] = low
                to_other_ref[f, q] = high


def edges(flag_ref, val, to_partner_ref, to_other_ref):
    upper = flag_ref[1]

    @pl.when(upper == 1)
    def _():
        to_partner_ref[0] = val[-1]
        to_other_ref[0] = val[0]

    @pl.when(upper == 0)
    def _():
        to_partner_ref[0] = val[0]
        to_other_ref[0] = val[-1]


def sum_kernel(flag_ref, own_ref, partner_ref, other_ref, val_ref, extra_ref, to_partner_ref, to_other_ref):
    val = own_ref[0] + partner_ref[0] + other_ref[0]
    val_ref[...] = val
    extra_ref[...] = own_ref[1] + partner_ref[1] + other_ref[1]
    edges(flag_ref, val, to_partner_ref, to_other_ref)


def chain_kernel(add_slot, send_slots, more, flag_ref, weight_ref, partner_ref, other_ref, extra_ref, *refs):
    earlier = refs[: more + 1]
    val_ref = earlier[-1]
    next_ref, to_partner_ref, to_other_ref = refs[more + 1 : more + 4]
    sends, wide = refs[more + 4 : -1], refs[-1]
    upper = flag_ref[1]
    add = flag_ref[add_slot].astype(F32)
    planes, rows, lanes = val_ref.shape
    wide[1 : planes + 1] = val_ref[...]
    wide[upper * (planes + 1)] = partner_ref[0]
    wide[(1 - upper) * (planes + 1)] = other_ref[0]
    for q in range(planes):
        def load(f, dz, i):
            return wide[1 + q + dz, tile(i), :]

        def weight(k, i):
            return weight_ref[k, q, tile(i), :]

        def store(f, i, v):
            next_ref[q, tile(i), :] = v + add * extra_ref[q, tile(i), :]

        step_plane(weight, load, store, rows, lanes)
    edges(flag_ref, next_ref[...], to_partner_ref, to_other_ref)
    for slot, ref in zip(send_slots, sends):
        which = flag_ref[slot]

        @pl.when(which < 0)
        def _():
            ref[...] = jnp.zeros(ref.shape, F32)

        for m, source in enumerate([*earlier, next_ref]):
            @pl.when(which == m)
            def _():
                ref[...] = source[...]


def final_kernel(slots, flag_ref, iterate_ref, *refs):
    count = len(slots)
    pieces, out_ref, rows_scr, fine_scr, sum_scr, error_scr = refs[:count], *refs[count:]
    planes, rows, lanes = iterate_ref.shape
    select, spread = pairing(lanes), spreading(lanes)
    piece_rows = pieces[0].shape[1]
    tiles = piece_rows // 8
    sum_scr[...] = jnp.zeros(sum_scr.shape, F32)
    for slot, ref in zip(slots, pieces):
        side = flag_ref[slot]
        sum_scr[side] = sum_scr[side] + ref[...]
    for q in range(planes // 2):
        for j in range(lanes // 256):
            column = slice(128 * j, 128 * j + 128)
            error_scr[j] = jnp.zeros(error_scr.shape[1:], F32)
            for side in range(2):
                base = side * (rows // 2 - piece_rows)
                for i in range(tiles):
                    at = pl.ds(base + i, 8, tiles)
                    error_scr[j, at, :] = error_scr[j, at, :] + sum_scr[side, q, tile(i), column]
        error = jnp.concatenate([error_scr[j] for j in range(lanes // 256)], axis=1)
        error = error - natural_mean(iterate_ref[2 * q], iterate_ref[2 * q + 1], rows_scr, select)
        wide = split_dot(error, spread)
        for j in range(lanes // 128):
            column = slice(128 * j, 128 * j + 128)
            fine_scr[j, pl.ds(0, rows // 2, 2), :] = wide[:, column]
            fine_scr[j, pl.ds(1, rows // 2, 2), :] = wide[:, column]
            for part in range(2):
                out_ref[2 * q + part, :, column] = iterate_ref[2 * q + part, :, column] + fine_scr[j]


def swap_pairs(count, first):
    pairs = []
    for i in range(first, count - 1, 2):
        pairs += [(i, i + 1), (i + 1, i)]
    return pairs


def roles(layers):
    last_group = layers // 2 - 1
    rows = []
    for t in range(layers):
        half, last = t % 2, int(t // 2 == last_group)
        adds = [int(number == (layers - 1 if last else 1)) for number in range(1, layers)]
        sends = []
        for shift in range(layers):
            k = (t + shift) % layers
            m = k if last else k - 1 - (t - half)
            sends.append(m if m >= 0 else -1)
        halves = [(t - shift) % layers % 2 for shift in range(layers)]
        rows.append([half, last, *adds, *sends, *halves])
    return rows


def local(initial, iterate, diffusivity):
    layers, slabs = lax.axis_size("tm"), lax.axis_size("space")
    t, s = lax.axis_index("tm"), lax.axis_index("space")
    planes, all_rows, lanes = initial.shape
    assert layers % 2 == 0 and slabs % 2 == 0 and planes == STEPS
    half = t % 2
    own_rows = all_rows // 2
    rows = own_rows + MARGIN
    inner_own = (3 * own_rows // 8) // 16 * 16
    outer_own = own_rows - inner_own
    inner_rows, outer_rows = inner_own + 2 * MARGIN, outer_own + MARGIN
    coarse_rows, coarse_lanes = rows // 2, lanes // 2
    reach = planes // 2
    upper = 1 - s % 2
    field = iterate[0]

    def partner_swap(x):
        return lax.ppermute(x, "space", swap_pairs(slabs, 0))

    def other_swap(x):
        return lax.ppermute(x, "space", swap_pairs(slabs, 1))

    anywhere = pl.BlockSpec(memory_space=pl.ANY)
    in_hbm = pl.BlockSpec(memory_space=pltpu.HBM)
    c, to_row_partner = pl.pallas_call(
        slice_kernel,
        out_shape=(shape(planes, rows, lanes), shape(planes, own_rows, lanes)),
        in_specs=[in_hbm] * 2,
        out_specs=tuple(whole(2)),
        scratch_shapes=[pltpu.SemaphoreType.DMA((2,))],
        compiler_params=params(VMEM_LIMITS["small"]),
        name="slices",
    )(diffusivity, field)
    row_pairs = swap_pairs(layers, 0)
    row_pairs.remove((layers - 1, layers - 2))
    received = lax.ppermute(to_row_partner, "tm", row_pairs)
    c_other = other_swap(c)
    c_partner = partner_swap(c)

    table = roles(layers)
    mine = jnp.asarray(table, jnp.int32)[t]
    flags = jnp.concatenate([mine[:1], jnp.reshape(upper, (1,)).astype(jnp.int32), mine[1:]])
    add_at, send_at, half_at = 3, 2 + layers, 2 + 2 * layers
    smem = pl.BlockSpec(memory_space=pltpu.SMEM)

    fields = shape(2, reach, coarse_rows, coarse_lanes)
    blocks = lanes // 128
    own, to_partner, to_other, weights = pl.pallas_call(
        functools.partial(fine_kernel, planes),
        out_shape=(fields, fields, fields, shape(7, reach, coarse_rows, coarse_lanes)),
        in_specs=[smem] + [anywhere] * 3 + [in_hbm] * 2 + [anywhere],
        out_specs=tuple(whole(4)),
        scratch_shapes=[
            VMEM((3 * planes, blocks, rows, 128), F32),
            VMEM((2, planes, blocks, rows, 128), F32),
            VMEM((3 * planes, rows, lanes), F32),
            VMEM((7, 3 * planes, rows, lanes), F32),
            VMEM((2, 3 * planes, rows, lanes), F32),
            VMEM((2, 3 * planes, rows, lanes), F32),
            VMEM((3 * reach, coarse_rows, coarse_lanes), F32),
            VMEM((2 * reach, coarse_rows, coarse_lanes), F32),
            pltpu.SemaphoreType.DMA((3, blocks)),
            pltpu.SemaphoreType.DMA((2, blocks)),
        ],
        compiler_params=params(VMEM_LIMITS["fine"]),
        name="fine",
    )(flags, c, c_partner, c_other, field, initial, received)

    from_other = other_swap(to_other)
    from_partner = partner_swap(to_partner)
    plane = shape(1, coarse_rows, coarse_lanes)
    block = shape(reach, coarse_rows, coarse_lanes)
    val, extra, to_partner, to_other = pl.pallas_call(
        sum_kernel,
        out_shape=(block, block, plane, plane),
        in_specs=[smem] + whole(3),
        out_specs=tuple(whole(4)),
        compiler_params=params(VMEM_LIMITS["small"]),
        name="gather",
    )(flags, own, from_partner, from_other)

    ready = [max(row[1 + layers + shift] for row in table) for shift in range(layers)]
    arrived = [None] * layers
    values = [val]
    for number in range(1, layers):
        from_other = other_swap(to_other)
        from_partner = partner_swap(to_partner)
        shifts = [shift for shift in range(layers) if max(ready[shift], 1) == number]
        earlier = values if shifts else values[-1:]
        val, to_partner, to_other, *sends = pl.pallas_call(
            functools.partial(chain_kernel, add_at + number - 1, [send_at + shift for shift in shifts], len(earlier) - 1),
            out_shape=(block, plane, plane, *[block] * len(shifts)),
            in_specs=[smem] + whole(4 + len(earlier)),
            out_specs=tuple(whole(3 + len(shifts))),
            scratch_shapes=[VMEM((reach + 2, coarse_rows, coarse_lanes), F32)],
            compiler_params=params(VMEM_LIMITS["small"]),
            name=f"chain{number}",
        )(flags, weights, from_partner, from_other, extra, *earlier)
        values.append(val)
        for shift, send in zip(shifts, sends):
            pairs = [
                (source, (source + shift) % layers)
                for source in range(layers)
                if table[source][1 + layers + shift] >= 0
            ]
            arrived[shift] = lax.ppermute(send, "tm", pairs) if shift else send

    corrected = pl.pallas_call(
        functools.partial(final_kernel, [half_at + shift for shift in range(layers)]),
        out_shape=shape(planes, all_rows, lanes),
        in_specs=[smem] + whole(1 + layers),
        out_specs=pl.BlockSpec(memory_space=VMEM),
        scratch_shapes=[
            VMEM((coarse_lanes // 128, all_rows, 128), F32),
            VMEM((lanes // 128, all_rows, 128), F32),
            VMEM((2, reach, coarse_rows, coarse_lanes), F32),
            VMEM((coarse_lanes // 128, all_rows // 2, 128), F32),
        ],
        compiler_params=params(VMEM_LIMITS["final"]),
        name="final",
    )(flags, field, *arrived)
    return corrected[None]


def solution(mesh):
    placed = (P("space", None, None), P("tm", "space", None, None), P("space", None, None))
    return jax.shard_map(
        local, mesh=mesh, in_specs=placed, out_specs=P("tm", "space", None, None), check_vma=False
    )
```

```python
import functools

import jax
import jax.numpy as jnp
from jax import lax
from jax.experimental import pallas as pl
from jax.experimental.pallas import tpu as pltpu
from jax.sharding import PartitionSpec as P


STEPS = 4
courant = 0.15
GAIN = 0.5 * courant
MARGIN = 16
F32 = jnp.float32
VMEM = pltpu.VMEM
MIB = 1024 * 1024
VMEM_LIMITS = {"slices": 50 * MIB, "fine": 50 * MIB, "small": 10 * MIB, "final": 16 * MIB}


def params(limit):
    return pltpu.CompilerParams(vmem_limit_bytes=limit)


def whole(count):
    return [pl.BlockSpec(memory_space=VMEM)] * count


def shape(*dims):
    return jax.ShapeDtypeStruct(dims, F32)


def split_dot(x, selection):
    high = x.astype(jnp.bfloat16)
    rest = x - high.astype(F32)
    middle = rest.astype(jnp.bfloat16)
    low = (rest - middle.astype(F32)).astype(jnp.bfloat16)
    dot = functools.partial(jnp.dot, preferred_element_type=F32)
    return dot(high, selection) + dot(middle, selection) + dot(low, selection)


def pairing(width):
    fine = lax.broadcasted_iota(jnp.int32, (width, width // 2), 0)
    coarse = lax.broadcasted_iota(jnp.int32, (width, width // 2), 1)
    return jnp.where((fine == 2 * coarse) | (fine == 2 * coarse + 1), 1.0, 0.0).astype(jnp.bfloat16)


def spreading(width):
    coarse = lax.broadcasted_iota(jnp.int32, (width // 2, width), 0)
    fine = lax.broadcasted_iota(jnp.int32, (width // 2, width), 1)
    return jnp.where((fine == 2 * coarse) | (fine == 2 * coarse + 1), 1.0, 0.0).astype(jnp.bfloat16)


def natural_mean(first, second, rows_scr, select):
    rows = first.shape[0]
    lanes = split_dot(first + second, select)
    parts = []
    for j in range(lanes.shape[1] // 128):
        rows_scr[j, 0:rows, :] = lanes[:, 128 * j : 128 * j + 128]
        even = rows_scr[j, pl.ds(0, rows // 2, 2), :]
        odd = rows_scr[j, pl.ds(1, rows // 2, 2), :]
        parts.append(0.125 * (even + odd))
    return jnp.concatenate(parts, axis=1)


def tile(i):
    return slice(8 * i, 8 * i + 8)


def dealt_mean(load, tiles, select):
    sums = [
        (load(0, 2 * i) + load(1, 2 * i)) + (load(0, 2 * i + 1) + load(1, 2 * i + 1)) for i in range(tiles // 2)
    ]
    return 0.125 * split_dot(jnp.concatenate(sums, axis=0), select)


def weights_plane(load, store, rows, lanes):
    sub = lax.broadcasted_iota(jnp.int32, (8, 128), 0)
    lane = lax.broadcasted_iota(jnp.int32, (8, 128), 1)
    tiles, blocks = rows // 8, lanes // 128

    def cut(x):
        return [x[:, 128 * j : 128 * j + 128] for j in range(blocks)]

    c = cut(load(0, 0))
    below = [pltpu.roll(x, 1, 0) for x in cut(load(0, tiles - 1))]
    wrapped = [pltpu.roll(x, 7, 0) for x in c]
    for i in range(tiles):
        above = cut(load(0, i + 1)) if i + 1 < tiles else wrapped
        czm, czp = cut(load(-1, i)), cut(load(1, i))
        right = [pltpu.roll(x, 1, 1) for x in c]
        left = [pltpu.roll(x, 127, 1) for x in c]
        w = [[] for _ in range(7)]
        for j in range(blocks):
            mid = c[j]
            xm = mid + jnp.where(lane == 0, right[j - 1] if j else 0.0, right[j])
            xp = mid + jnp.where(lane == 127, left[j + 1] if j + 1 < blocks else 0.0, left[j])
            ym = mid + (jnp.where(sub == 0, 0.0, below[j]) if i == 0 else below[j])
            yp = mid + (jnp.where(sub == 7, 0.0, above[j]) if i + 1 == tiles else above[j])
            zm, zp = mid + czm[j], mid + czp[j]
            w[0].append(1.0 - ((xm + xp) + (ym + yp) + (zm + zp)))
            w[1].append(xm if j else jnp.where(lane == 0, 0.0, xm))
            w[2].append(xp if j + 1 < blocks else jnp.where(lane == 127, 0.0, xp))
            w[3].append(jnp.where(sub == 0, 0.0, ym) if i == 0 else ym)
            w[4].append(jnp.where(sub == 7, 0.0, yp) if i + 1 == tiles else yp)
            inside = mid > 0.0
            w[5].append(jnp.where(inside, zm, 0.0))
            w[6].append(jnp.where(inside, zp, 0.0))
        for k in range(7):
            store(k, i, jnp.concatenate(w[k], axis=1))
        below, c = c, above


def step_plane(weight, load, store, rows, lanes, fields=1):
    tiles = rows // 8
    below = [pltpu.roll(load(f, 0, tiles - 1), 1, 0) for f in range(fields)]
    center = [load(f, 0, 0) for f in range(fields)]
    wrapped = [pltpu.roll(v, 7, 0) for v in center]
    for i in range(tiles):
        w = [weight(k, i) for k in range(7)]
        for f in range(fields):
            mid = center[f]
            above = load(f, 0, i + 1) if i + 1 < tiles else wrapped[f]
            xm = pltpu.roll(mid, 1, 1)
            xp = pltpu.roll(mid, lanes - 1, 1)
            out = w[0] * mid
            out = out + (w[1] * xm + w[2] * xp)
            out = out + (w[3] * below[f] + w[4] * above)
            out = out + (w[5] * load(f, -1, i) + w[6] * load(f, 1, i))
            store(f, i, out)
            below[f], center[f] = mid, above


def at_row(value, step):
    return pl.multiple_of(value * step, 8)


def slice_kernel(c_hbm, iterate_hbm, c_ref, send_ref, sem):
    half = lax.rem(lax.axis_index("tm"), 2)
    own = send_ref.shape[1]
    window = pl.ds(at_row(half, c_hbm.shape[1] - c_ref.shape[1]), c_ref.shape[1])
    send = pltpu.make_async_copy(iterate_hbm.at[:, pl.ds(at_row(1 - half, own), own), :], send_ref, sem.at[0])
    keep = pltpu.make_async_copy(c_hbm.at[:, window, :], c_ref, sem.at[1])
    send.start()
    keep.start()
    send.wait()
    keep.wait()


def fine_kernel(planes, flag_ref, c_hbm, partner_hbm, other_hbm, iterate_hbm, initial_hbm, received_hbm,
                own_ref, to_partner_ref, to_other_ref, cc_scr,
                c_raw, v_raw, c_scr, w_scr, a_scr, b_scr, coarse_ref, keep_scr, c_sem, v_sem):
    half, upper, last = flag_ref[0], flag_ref[1], flag_ref[2]
    depth, rows, lanes = c_scr.shape
    own_rows = rows - MARGIN
    tiles = rows // 8
    columns = [slice(128 * j, 128 * j + 128) for j in range(lanes // 128)]
    select = pairing(lanes)
    coarse_planes, reach = depth // 2, planes // 2
    coarse_rows, coarse_lanes = rows // 2, lanes // 2
    last_plane = depth - 1

    slabs = ((c_hbm, planes), (partner_hbm, upper * (2 * planes)), (other_hbm, (1 - upper) * (2 * planes)))
    c_copies = [
        pltpu.make_async_copy(ref.at[:, :, column], c_raw.at[pl.ds(at, planes), j], c_sem.at[n, j])
        for n, (ref, at) in enumerate(slabs)
        for j, column in enumerate(columns)
    ]
    for copy in c_copies:
        copy.start()
    into = pl.ds(at_row(half, MARGIN), own_rows)
    source = pl.ds(at_row(half, own_rows), own_rows)

    def fetch(ref, f):
        for j in range(len(columns)):
            pltpu.make_async_copy(ref[j], v_raw.at[f, :, j, into, :], v_sem.at[f, j]).start()

    def halves(ref):
        return [ref.at[:, source, column] for column in columns]

    received = [received_hbm.at[:, :, column] for column in columns]

    first_kept = (last == 0) & (half == 0)
    first_got = (last == 0) & (half == 1)
    second_kept = (last == 1) == (half == 0)
    for f, choices in enumerate(
        (
            ((last == 1, halves(initial_hbm)), (first_kept, halves(iterate_hbm)), (first_got, received)),
            ((second_kept, halves(iterate_hbm)), (jnp.logical_not(second_kept), received)),
        )
    ):
        for condition, ref in choices:
            @pl.when(condition)
            def _():
                fetch(ref, f)

    outside = pl.ds(at_row(1 - half, own_rows), MARGIN)
    v_raw[:, :, :, outside, :] = jnp.zeros(v_raw.shape[:3] + (MARGIN, 128), F32)
    idle = jnp.zeros((2,) + a_scr.shape[2:], F32)
    for number in range(STEPS):
        v_in = (a_scr, b_scr)[number % 2]
        v_in[:, planes - 1 - number] = idle
        v_in[:, 2 * planes + number] = idle
    for copy in c_copies:
        copy.wait()

    def deal_c(z, _):
        for j, column in enumerate(columns):
            for i in range(tiles):
                c_scr[z, tile(i), column] = GAIN * c_raw[z, j, pl.ds(i, 8, tiles), :]
        return 0

    lax.fori_loop(0, depth, deal_c, 0)

    def weigh(z, _):
        below, above = jnp.maximum(z - 1, 0), jnp.minimum(z + 1, last_plane)

        def load(dz, i):
            at = z if dz == 0 else (below if dz < 0 else above)
            return c_scr[at, tile(i), :]

        def store(k, i, w):
            w_scr[k, z, tile(i), :] = w

        weights_plane(load, store, rows, lanes)
        return 0

    lax.fori_loop(1, last_plane, weigh, 0)
    for k, z, inner in ((6, 0, 1), (5, last_plane, last_plane - 1)):
        for i in range(tiles):
            c = c_scr[z, tile(i), :]
            w_scr[k, z, tile(i), :] = jnp.where(c > 0.0, c + c_scr[inner, tile(i), :], 0.0)

    def restrict_c(q, _):
        cc_scr[q] = dealt_mean(lambda dz, i: c_scr[2 * q + dz, tile(i), :], tiles, select)
        return 0

    lax.fori_loop(0, coarse_planes, restrict_c, 0)
    for q in range(reach):
        def load(dz, i):
            return cc_scr[reach + q + dz, tile(i), :]

        def store(k, i, w):
            coarse_ref[k, q, tile(i), :] = w

        weights_plane(load, store, coarse_rows, coarse_lanes)

    for f in range(2):
        for j in range(len(columns)):
            pltpu.make_async_copy(received[j], v_raw.at[f, :, j, into, :], v_sem.at[f, j]).wait()

    def deal_v(z, _):
        for f in range(2):
            for j, column in enumerate(columns):
                for i in range(tiles):
                    a_scr[f, planes + z, tile(i), column] = v_raw[f, z, j, pl.ds(i, 8, tiles), :]
        return 0

    lax.fori_loop(0, planes, deal_v, 0)

    def keep(n, _):
        f, q = n // reach, n % reach
        keep_scr[n] = dealt_mean(lambda dz, i: a_scr[f, planes + 2 * q + dz, tile(i), :], tiles, select)
        return 0

    lax.fori_loop(0, 2 * reach, keep, 0)
    for number in range(STEPS):
        v_in, v_out = (a_scr, b_scr) if number % 2 == 0 else (b_scr, a_scr)

        def advance(z, _):
            below, above = jnp.maximum(z - 1, 0), jnp.minimum(z + 1, last_plane)

            def load(f, dz, i):
                at = z if dz == 0 else (below if dz < 0 else above)
                return v_in[f, at, tile(i), :]

            def weight(k, i):
                return w_scr[k, z, tile(i), :]

            def store(f, i, v):
                v_out[f, z, tile(i), :] = v

            step_plane(weight, load, store, rows, lanes, 2)
            return 0

        lax.fori_loop(planes - number, 2 * planes + number, advance, 0)
        for k, z, inner in ((6, planes - 1 - number, planes - number), (5, 2 * planes + number, 2 * planes + number - 1)):
            for i in range(tiles):
                w = w_scr[k, z, tile(i), :]
                for f in range(2):
                    v_out[f, z, tile(i), :] = w * v_in[f, inner, tile(i), :]
    result = a_scr if STEPS % 2 == 0 else b_scr

    scale = jnp.where(last == 1, 0.0, 1.0).astype(F32)
    for q in range(reach):
        keep_scr[q] = keep_scr[q] * scale
    zero = jnp.zeros((8, coarse_lanes), F32)
    for q in range(reach):
        def load(f, dz, i):
            at = q + dz
            return zero if at < 0 or at >= reach else keep_scr[f * reach + at, tile(i), :]

        def weight(k, i):
            return coarse_ref[k, q, tile(i), :]

        def store(f, i, v):
            own_ref[f, q, tile(i), :] = v

        step_plane(weight, load, store, coarse_rows, coarse_lanes, 2)

    def mean_of(f, q):
        return dealt_mean(lambda dz, i: result[f, 2 * q + dz, tile(i), :], tiles, select)

    low_c, high_c = cc_scr[reach - 1], cc_scr[2 * reach]
    low_w = jnp.where(low_c > 0.0, low_c + cc_scr[reach], 0.0)
    high_w = jnp.where(high_c > 0.0, high_c + cc_scr[2 * reach - 1], 0.0)
    for f in range(2):
        for q in range(reach):
            own_ref[f, q] = mean_of(f, reach + q) - own_ref[f, q]
        for q in range(reach):
            low, high = mean_of(f, q), mean_of(f, 2 * reach + q)
            if q == reach - 1:
                low = low - low_w * keep_scr[f * reach]
            if q == 0:
                high = high - high_w * keep_scr[f * reach + reach - 1]

            @pl.when(upper == 1)
            def _():
                to_partner_ref[f, q] = high
                to_other_ref[f, q] = low

            @pl.when(upper == 0)
            def _():
                to_partner_ref[f, q] = low
                to_other_ref[f, q] = high


def weight_kernel(cc_ref, weight_ref):
    planes, rows, lanes = cc_ref.shape
    for q in range(planes - 2):
        def load(dz, i):
            return cc_ref[q + 1 + dz, tile(i), :]

        def store(k, i, w):
            weight_ref[k, q, tile(i), :] = w

        weights_plane(load, store, rows, lanes)


def sum_kernel(flag_ref, own_ref, partner_ref, other_ref, val_ref, extra_ref, to_partner_ref, to_other_ref):
    upper = flag_ref[1]
    planes = val_ref.shape[0]
    val = own_ref[0] + partner_ref[0] + other_ref[0]
    extra = own_ref[1] + partner_ref[1] + other_ref[1]
    val_ref[...] = val
    extra_ref[...] = extra
    to_partner_ref[0:planes] = val
    to_other_ref[0:planes] = val
    to_partner_ref[planes] = jnp.where(upper == 1, extra[-1], extra[0])
    to_other_ref[planes] = jnp.where(upper == 1, extra[0], extra[-1])


def coarse_advance(weight_ref, offset, source, into, count, extra, add, rows, lanes):
    for q in range(count):
        def load(f, dz, i):
            return source[q + 1 + dz, tile(i), :]

        def weight(k, i):
            return weight_ref[k, offset + q, tile(i), :]

        def store(f, i, v):
            into[q, tile(i), :] = v + add * extra[q, tile(i), :]

        step_plane(weight, load, store, rows, lanes)


def double_kernel(slots, flag_ref, weight_ref, partner_ref, other_ref, extra_ref, val_ref,
                  first_ref, second_ref, to_partner_ref, to_other_ref, wide, extra_wide, middle):
    upper = flag_ref[1]
    planes, rows, lanes = val_ref.shape
    extra_wide[1 : planes + 1] = extra_ref[...]
    wide[planes : 2 * planes] = val_ref[...]
    for ref, above in ((partner_ref, upper), (other_ref, 1 - upper)):
        wide[pl.ds(above * (2 * planes), planes)] = ref[0:planes]
        extra_wide[above * (planes + 1)] = ref[planes]
    add = [flag_ref[slot].astype(F32) for slot in slots]
    coarse_advance(weight_ref, 0, wide.at[planes - 2 :], middle, planes + 2, extra_wide, add[0], rows, lanes)
    first_ref[...] = middle[1 : planes + 1]
    coarse_advance(weight_ref, 1, middle, second_ref, planes, extra_ref, add[1], rows, lanes)
    low, high = second_ref[0], second_ref[planes - 1]
    to_partner_ref[0] = jnp.where(upper == 1, high, low)
    to_other_ref[0] = jnp.where(upper == 1, low, high)


def single_kernel(slot, flag_ref, weight_ref, partner_ref, other_ref, extra_ref, val_ref,
                  next_ref, to_partner_ref, to_other_ref, wide):
    upper = flag_ref[1]
    planes, rows, lanes = val_ref.shape
    wide[1 : planes + 1] = val_ref[...]
    wide[upper * (planes + 1)] = partner_ref[0]
    wide[(1 - upper) * (planes + 1)] = other_ref[0]
    coarse_advance(weight_ref, 1, wide, next_ref, planes, extra_ref, flag_ref[slot].astype(F32), rows, lanes)
    low, high = next_ref[0], next_ref[planes - 1]
    to_partner_ref[0] = jnp.where(upper == 1, high, low)
    to_other_ref[0] = jnp.where(upper == 1, low, high)


def pick_kernel(slots, count, flag_ref, *refs):
    for slot, ref in zip(slots, refs[count:]):
        which = flag_ref[slot]

        @pl.when(which < 0)
        def _():
            ref[...] = jnp.zeros(ref.shape, F32)

        for m, source in enumerate(refs[:count]):
            @pl.when(which == m)
            def _():
                ref[...] = source[...]


def base_kernel(iterate_ref, out_ref, rows_scr, fine_scr):
    planes, rows, lanes = iterate_ref.shape
    select, spread = pairing(lanes), spreading(lanes)
    for q in range(planes // 2):
        mean = natural_mean(iterate_ref[2 * q], iterate_ref[2 * q + 1], rows_scr, select)
        wide = split_dot(mean, spread)
        for j in range(lanes // 128):
            column = slice(128 * j, 128 * j + 128)
            fine_scr[j, pl.ds(0, rows // 2, 2), :] = wide[:, column]
            fine_scr[j, pl.ds(1, rows // 2, 2), :] = wide[:, column]
            for part in range(2):
                out_ref[2 * q + part, :, column] = iterate_ref[2 * q + part, :, column] - fine_scr[j]


def final_kernel(slots, flag_ref, base_ref, *refs):
    count = len(slots)
    pieces, out_ref, fine_scr, sum_scr, error_scr = refs[:count], *refs[count:]
    planes, rows, lanes = base_ref.shape
    spread = spreading(lanes)
    piece_rows = pieces[0].shape[1]
    tiles = piece_rows // 8
    sum_scr[...] = jnp.zeros(sum_scr.shape, F32)
    for slot, ref in zip(slots, pieces):
        side = flag_ref[slot]
        sum_scr[side] = sum_scr[side] + ref[...]
    for q in range(planes // 2):
        for j in range(lanes // 256):
            column = slice(128 * j, 128 * j + 128)
            error_scr[j] = jnp.zeros(error_scr.shape[1:], F32)
            for side in range(2):
                first = side * (rows // 2 - piece_rows)
                for i in range(tiles):
                    at = pl.ds(first + i, 8, tiles)
                    error_scr[j, at, :] = error_scr[j, at, :] + sum_scr[side, q, tile(i), column]
        error = jnp.concatenate([error_scr[j] for j in range(lanes // 256)], axis=1)
        wide = split_dot(error, spread)
        for j in range(lanes // 128):
            column = slice(128 * j, 128 * j + 128)
            fine_scr[j, pl.ds(0, rows // 2, 2), :] = wide[:, column]
            fine_scr[j, pl.ds(1, rows // 2, 2), :] = wide[:, column]
            for part in range(2):
                out_ref[2 * q + part, :, column] = base_ref[2 * q + part, :, column] + fine_scr[j]


def swap_pairs(count, first):
    pairs = []
    for i in range(first, count - 1, 2):
        pairs += [(i, i + 1), (i + 1, i)]
    return pairs


def roles(layers):
    last_group = layers // 2 - 1
    rows = []
    for t in range(layers):
        half, last = t % 2, int(t // 2 == last_group)
        adds = [int(number == (layers - 1 if last else 1)) for number in range(1, layers)]
        sends = []
        for shift in range(layers):
            k = (t + shift) % layers
            m = k if last else k - 1 - (t - half)
            sends.append(m if m >= 0 else -1)
        halves = [(t - shift) % layers % 2 for shift in range(layers)]
        rows.append([half, last, *adds, *sends, *halves])
    return rows


def local(initial, iterate, diffusivity):
    layers, slabs = lax.axis_size("tm"), lax.axis_size("space")
    t, s = lax.axis_index("tm"), lax.axis_index("space")
    planes, all_rows, lanes = initial.shape
    assert layers % 2 == 0 and slabs % 2 == 0 and planes == STEPS
    own_rows = all_rows // 2
    rows = own_rows + MARGIN
    coarse_rows, coarse_lanes = rows // 2, lanes // 2
    reach = planes // 2
    upper = 1 - s % 2
    field = iterate[0]

    def partner_swap(x):
        return lax.ppermute(x, "space", swap_pairs(slabs, 0))

    def other_swap(x):
        return lax.ppermute(x, "space", swap_pairs(slabs, 1))

    anywhere = pl.BlockSpec(memory_space=pl.ANY)
    in_hbm = pl.BlockSpec(memory_space=pltpu.HBM)
    c, to_row_partner = pl.pallas_call(
        slice_kernel,
        out_shape=(shape(planes, rows, lanes), shape(planes, own_rows, lanes)),
        in_specs=[in_hbm] * 2,
        out_specs=tuple(whole(2)),
        scratch_shapes=[pltpu.SemaphoreType.DMA((2,))],
        compiler_params=params(VMEM_LIMITS["slices"]),
        name="slices",
    )(diffusivity, field)
    row_pairs = swap_pairs(layers, 0)
    row_pairs.remove((layers - 1, layers - 2))
    received = lax.ppermute(to_row_partner, "tm", row_pairs)
    c_other = other_swap(c)
    c_partner = partner_swap(c)

    table = roles(layers)
    mine = jnp.asarray(table, jnp.int32)[t]
    flags = jnp.concatenate([mine[:1], jnp.reshape(upper, (1,)).astype(jnp.int32), mine[1:]])
    add_at, send_at, half_at = 3, 2 + layers, 2 + 2 * layers
    smem = pl.BlockSpec(memory_space=pltpu.SMEM)

    fields = shape(2, reach, coarse_rows, coarse_lanes)
    blocks = lanes // 128
    own, to_partner, to_other, cc = pl.pallas_call(
        functools.partial(fine_kernel, planes),
        out_shape=(fields, fields, fields, shape(3 * reach, coarse_rows, coarse_lanes)),
        in_specs=[smem] + [anywhere] * 3 + [in_hbm] * 2 + [anywhere],
        out_specs=tuple(whole(4)),
        scratch_shapes=[
            VMEM((3 * planes, blocks, rows, 128), F32),
            VMEM((2, planes, blocks, rows, 128), F32),
            VMEM((3 * planes, rows, lanes), F32),
            VMEM((7, 3 * planes, rows, lanes), F32),
            VMEM((2, 3 * planes, rows, lanes), F32),
            VMEM((2, 3 * planes, rows, lanes), F32),
            VMEM((7, reach, coarse_rows, coarse_lanes), F32),
            VMEM((2 * reach, coarse_rows, coarse_lanes), F32),
            pltpu.SemaphoreType.DMA((3, blocks)),
            pltpu.SemaphoreType.DMA((2, blocks)),
        ],
        compiler_params=params(VMEM_LIMITS["fine"]),
        name="fine",
    )(flags, c, c_partner, c_other, field, initial, received)

    def cost(microseconds):
        return pl.CostEstimate(flops=int(microseconds * 4e6), bytes_accessed=0, transcendentals=0)

    base = pl.pallas_call(
        base_kernel,
        out_shape=shape(planes, all_rows, lanes),
        in_specs=whole(1),
        out_specs=pl.BlockSpec(memory_space=VMEM),
        scratch_shapes=[VMEM((coarse_lanes // 128, all_rows, 128), F32), VMEM((lanes // 128, all_rows, 128), F32)],
        compiler_params=params(VMEM_LIMITS["final"]),
        cost_estimate=cost(4),
        name="base",
    )(field)

    from_other = other_swap(to_other)
    from_partner = partner_swap(to_partner)
    plane = shape(1, coarse_rows, coarse_lanes)
    block = shape(reach, coarse_rows, coarse_lanes)
    thick = shape(reach + 1, coarse_rows, coarse_lanes)
    weights = pl.pallas_call(
        weight_kernel,
        out_shape=shape(7, 3 * reach - 2, coarse_rows, coarse_lanes),
        in_specs=whole(1),
        out_specs=pl.BlockSpec(memory_space=VMEM),
        compiler_params=params(VMEM_LIMITS["small"]),
        cost_estimate=cost(2),
        name="weights",
    )(cc)
    val, extra, to_partner, to_other = pl.pallas_call(
        sum_kernel,
        out_shape=(block, block, thick, thick),
        in_specs=[smem] + whole(3),
        out_specs=tuple(whole(4)),
        compiler_params=params(VMEM_LIMITS["small"]),
        name="gather",
    )(flags, own, from_partner, from_other)

    ready = [max(row[1 + layers + shift] for row in table) for shift in range(layers)]
    arrived = [None] * layers
    values = [val]
    done = -1

    def deliver():
        upto = len(values) - 1
        shifts = [shift for shift in range(layers) if done < max(ready[shift], 0) <= upto]
        if not shifts:
            return upto
        sends = pl.pallas_call(
            functools.partial(pick_kernel, [send_at + shift for shift in shifts], len(values)),
            out_shape=(block,) * len(shifts),
            in_specs=[smem] + whole(len(values)),
            out_specs=tuple(whole(len(shifts))),
            compiler_params=params(VMEM_LIMITS["small"]),
        )(flags, *values)
        for shift, send in zip(shifts, sends):
            pairs = [
                (source, (source + shift) % layers)
                for source in range(layers)
                if table[source][1 + layers + shift] >= 0
            ]
            arrived[shift] = lax.ppermute(send, "tm", pairs) if shift else send
        return upto

    number = 1
    while number < layers:
        from_other = other_swap(to_other)
        from_partner = partner_swap(to_partner)
        if number > 1:
            done = deliver()
        double = number == 1 and number + 1 < layers
        slots = [add_at + number - 1 + n for n in range(1 + double)]
        *made, to_partner, to_other = pl.pallas_call(
            functools.partial(double_kernel, slots) if double else functools.partial(single_kernel, slots[0]),
            out_shape=(*[block] * len(slots), plane, plane),
            in_specs=[smem] + whole(5),
            out_specs=tuple(whole(2 + len(slots))),
            scratch_shapes=[
                VMEM((3 * reach, coarse_rows, coarse_lanes), F32),
                VMEM((reach + 2, coarse_rows, coarse_lanes), F32),
                VMEM((reach + 2, coarse_rows, coarse_lanes), F32),
            ] if double else [VMEM((reach + 2, coarse_rows, coarse_lanes), F32)],
            compiler_params=params(VMEM_LIMITS["small"]),
        )(flags, weights, from_partner, from_other, extra, values[-1])
        values += made
        number += len(slots)
    deliver()

    corrected = pl.pallas_call(
        functools.partial(final_kernel, [half_at + shift for shift in range(layers)]),
        out_shape=shape(planes, all_rows, lanes),
        in_specs=[smem] + whole(1 + layers),
        out_specs=pl.BlockSpec(memory_space=VMEM),
        scratch_shapes=[
            VMEM((lanes // 128, all_rows, 128), F32),
            VMEM((2, reach, coarse_rows, coarse_lanes), F32),
            VMEM((coarse_lanes // 128, all_rows // 2, 128), F32),
        ],
        compiler_params=params(VMEM_LIMITS["final"]),
        name="final",
    )(flags, base, *arrived)
    return corrected[None]


def solution(mesh):
    placed = (P("space", None, None), P("tm", "space", None, None), P("space", None, None))

    return jax.shard_map(local, mesh=mesh, in_specs=placed, out_specs=P("tm", "space", None, None), check_vma=False)
```

```python
import functools

import jax
import jax.numpy as jnp
from jax import lax
from jax.experimental import pallas as pl
from jax.experimental.pallas import tpu as pltpu
from jax.sharding import PartitionSpec as P


STEPS = 4
courant = 0.15
GAIN = 0.5 * courant
MARGIN = 16
F32 = jnp.float32
VMEM = pltpu.VMEM
MIB = 1024 * 1024
VMEM_LIMITS = {"slices": 50 * MIB, "fine": 50 * MIB, "small": 10 * MIB, "final": 16 * MIB}


def params(limit):
    return pltpu.CompilerParams(vmem_limit_bytes=limit)


def whole(count):
    return [pl.BlockSpec(memory_space=VMEM)] * count


def shape(*dims):
    return jax.ShapeDtypeStruct(dims, F32)


def split_dot(x, selection):
    high = x.astype(jnp.bfloat16)
    rest = x - high.astype(F32)
    middle = rest.astype(jnp.bfloat16)
    low = (rest - middle.astype(F32)).astype(jnp.bfloat16)
    dot = functools.partial(jnp.dot, preferred_element_type=F32)
    return dot(high, selection) + dot(middle, selection) + dot(low, selection)


def pairing(width):
    fine = lax.broadcasted_iota(jnp.int32, (width, width // 2), 0)
    coarse = lax.broadcasted_iota(jnp.int32, (width, width // 2), 1)
    return jnp.where((fine == 2 * coarse) | (fine == 2 * coarse + 1), 1.0, 0.0).astype(jnp.bfloat16)


def spreading(width):
    coarse = lax.broadcasted_iota(jnp.int32, (width // 2, width), 0)
    fine = lax.broadcasted_iota(jnp.int32, (width // 2, width), 1)
    return jnp.where((fine == 2 * coarse) | (fine == 2 * coarse + 1), 1.0, 0.0).astype(jnp.bfloat16)


def natural_mean(first, second, rows_scr, select):
    rows = first.shape[0]
    lanes = split_dot(first + second, select)
    parts = []
    for j in range(lanes.shape[1] // 128):
        rows_scr[j, 0:rows, :] = lanes[:, 128 * j : 128 * j + 128]
        even = rows_scr[j, pl.ds(0, rows // 2, 2), :]
        odd = rows_scr[j, pl.ds(1, rows // 2, 2), :]
        parts.append(0.125 * (even + odd))
    return jnp.concatenate(parts, axis=1)


def tile(i):
    return slice(8 * i, 8 * i + 8)


def pair_lanes(blocks):
    lane = lax.broadcasted_iota(jnp.int32, (8, 128), 1)
    place = 2 * (lane % 64)
    out = []
    for first, second in zip(blocks[::2], blocks[1::2]):
        halves = [
            jnp.take_along_axis(x + pltpu.roll(x, 127, 1), place, axis=1, mode="promise_in_bounds") for x in (first, second)
        ]
        out.append(jnp.where(lane < 64, *halves))
    return out


def dealt_mean(load, tiles, store):
    for i in range(tiles // 2):
        total = (load(0, 2 * i) + load(1, 2 * i)) + (load(0, 2 * i + 1) + load(1, 2 * i + 1))
        blocks = [total[:, 128 * j : 128 * j + 128] for j in range(total.shape[1] // 128)]
        store(i, 0.125 * jnp.concatenate(pair_lanes(blocks), axis=1))


def weights_plane(load, store, rows, lanes):
    sub = lax.broadcasted_iota(jnp.int32, (8, 128), 0)
    lane = lax.broadcasted_iota(jnp.int32, (8, 128), 1)
    tiles, blocks = rows // 8, lanes // 128

    def cut(x):
        return [x[:, 128 * j : 128 * j + 128] for j in range(blocks)]

    c = cut(load(0, 0))
    below = [pltpu.roll(x, 1, 0) for x in cut(load(0, tiles - 1))]
    wrapped = [pltpu.roll(x, 7, 0) for x in c]
    for i in range(tiles):
        above = cut(load(0, i + 1)) if i + 1 < tiles else wrapped
        czm, czp = cut(load(-1, i)), cut(load(1, i))
        right = [pltpu.roll(x, 1, 1) for x in c]
        left = [pltpu.roll(x, 127, 1) for x in c]
        w = [[] for _ in range(7)]
        for j in range(blocks):
            mid = c[j]
            xm = mid + jnp.where(lane == 0, right[j - 1] if j else 0.0, right[j])
            xp = mid + jnp.where(lane == 127, left[j + 1] if j + 1 < blocks else 0.0, left[j])
            ym = mid + (jnp.where(sub == 0, 0.0, below[j]) if i == 0 else below[j])
            yp = mid + (jnp.where(sub == 7, 0.0, above[j]) if i + 1 == tiles else above[j])
            zm, zp = mid + czm[j], mid + czp[j]
            w[0].append(1.0 - ((xm + xp) + (ym + yp) + (zm + zp)))
            w[1].append(xm if j else jnp.where(lane == 0, 0.0, xm))
            w[2].append(xp if j + 1 < blocks else jnp.where(lane == 127, 0.0, xp))
            w[3].append(jnp.where(sub == 0, 0.0, ym) if i == 0 else ym)
            w[4].append(jnp.where(sub == 7, 0.0, yp) if i + 1 == tiles else yp)
            inside = mid > 0.0
            w[5].append(jnp.where(inside, zm, 0.0))
            w[6].append(jnp.where(inside, zp, 0.0))
        for k in range(7):
            store(k, i, jnp.concatenate(w[k], axis=1))
        below, c = c, above


def step_plane(weight, load, store, rows, lanes, fields=1):
    tiles = rows // 8
    below = [pltpu.roll(load(f, 0, tiles - 1), 1, 0) for f in range(fields)]
    center = [load(f, 0, 0) for f in range(fields)]
    wrapped = [pltpu.roll(v, 7, 0) for v in center]
    for i in range(tiles):
        w = [weight(k, i) for k in range(7)]
        for f in range(fields):
            mid = center[f]
            above = load(f, 0, i + 1) if i + 1 < tiles else wrapped[f]
            xm = pltpu.roll(mid, 1, 1)
            xp = pltpu.roll(mid, lanes - 1, 1)
            out = w[0] * mid
            out = out + (w[1] * xm + w[2] * xp)
            out = out + (w[3] * below[f] + w[4] * above)
            out = out + (w[5] * load(f, -1, i) + w[6] * load(f, 1, i))
            store(f, i, out)
            below[f], center[f] = mid, above


def at_row(value, step):
    return pl.multiple_of(value * step, 8)


def slice_kernel(c_hbm, iterate_hbm, c_ref, send_ref, sem):
    half = lax.rem(lax.axis_index("tm"), 2)
    own = send_ref.shape[1]
    window = pl.ds(at_row(half, c_hbm.shape[1] - c_ref.shape[1]), c_ref.shape[1])
    send = pltpu.make_async_copy(iterate_hbm.at[:, pl.ds(at_row(1 - half, own), own), :], send_ref, sem.at[0])
    keep = pltpu.make_async_copy(c_hbm.at[:, window, :], c_ref, sem.at[1])
    send.start()
    keep.start()
    send.wait()
    keep.wait()


def fine_kernel(planes, flag_ref, c_hbm, partner_hbm, other_hbm, iterate_hbm, initial_hbm, received_hbm,
                own_ref, to_partner_ref, to_other_ref, cc_scr,
                c_raw, v_raw, c_scr, w_scr, a_scr, b_scr, coarse_ref, keep_scr, c_sem, v_sem):
    half, upper, last = flag_ref[0], flag_ref[1], flag_ref[2]
    depth, rows, lanes = c_scr.shape
    own_rows = rows - MARGIN
    tiles = rows // 8
    columns = [slice(128 * j, 128 * j + 128) for j in range(lanes // 128)]
    coarse_planes, reach = depth // 2, planes // 2
    coarse_rows, coarse_lanes = rows // 2, lanes // 2
    last_plane = depth - 1

    slabs = ((c_hbm, planes), (partner_hbm, upper * (2 * planes)), (other_hbm, (1 - upper) * (2 * planes)))
    c_copies = [
        pltpu.make_async_copy(ref.at[:, :, column], c_raw.at[pl.ds(at, planes), j], c_sem.at[n, j])
        for n, (ref, at) in enumerate(slabs)
        for j, column in enumerate(columns)
    ]
    for copy in c_copies:
        copy.start()
    into = pl.ds(at_row(half, MARGIN), own_rows)
    source = pl.ds(at_row(half, own_rows), own_rows)

    def fetch(ref, f):
        for j in range(len(columns)):
            pltpu.make_async_copy(ref[j], v_raw.at[f, :, j, into, :], v_sem.at[f, j]).start()

    def halves(ref):
        return [ref.at[:, source, column] for column in columns]

    received = [received_hbm.at[:, :, column] for column in columns]

    first_kept = (last == 0) & (half == 0)
    first_got = (last == 0) & (half == 1)
    second_kept = (last == 1) == (half == 0)
    for f, choices in enumerate(
        (
            ((last == 1, halves(initial_hbm)), (first_kept, halves(iterate_hbm)), (first_got, received)),
            ((second_kept, halves(iterate_hbm)), (jnp.logical_not(second_kept), received)),
        )
    ):
        for condition, ref in choices:
            @pl.when(condition)
            def _():
                fetch(ref, f)

    outside = pl.ds(at_row(1 - half, own_rows), MARGIN)
    v_raw[:, :, :, outside, :] = jnp.zeros(v_raw.shape[:3] + (MARGIN, 128), F32)
    idle = jnp.zeros((2,) + a_scr.shape[2:], F32)
    for number in range(STEPS):
        v_in = (a_scr, b_scr)[number % 2]
        v_in[:, planes - 1 - number] = idle
        v_in[:, 2 * planes + number] = idle
    for copy in c_copies:
        copy.wait()

    def deal_c(z, _):
        for j, column in enumerate(columns):
            for i in range(tiles):
                c_scr[z, tile(i), column] = GAIN * c_raw[z, j, pl.ds(i, 8, tiles), :]
        return 0

    lax.fori_loop(0, depth, deal_c, 0)

    def weigh(z, _):
        below, above = jnp.maximum(z - 1, 0), jnp.minimum(z + 1, last_plane)

        def load(dz, i):
            at = z if dz == 0 else (below if dz < 0 else above)
            return c_scr[at, tile(i), :]

        def store(k, i, w):
            w_scr[k, z, tile(i), :] = w

        weights_plane(load, store, rows, lanes)
        return 0

    lax.fori_loop(1, last_plane, weigh, 0)
    for k, z, inner in ((6, 0, 1), (5, last_plane, last_plane - 1)):
        for i in range(tiles):
            c = c_scr[z, tile(i), :]
            w_scr[k, z, tile(i), :] = jnp.where(c > 0.0, c + c_scr[inner, tile(i), :], 0.0)

    def restrict_c(n, _):
        for q in range(reach):
            at = n * reach + q

            def store(i, mean):
                cc_scr[at, tile(i), :] = mean

            dealt_mean(lambda dz, i: c_scr[2 * at + dz, tile(i), :], tiles, store)
        return 0

    lax.fori_loop(0, coarse_planes // reach, restrict_c, 0)
    for q in range(reach):
        def load(dz, i):
            return cc_scr[reach + q + dz, tile(i), :]

        def store(k, i, w):
            coarse_ref[k, q, tile(i), :] = w

        weights_plane(load, store, coarse_rows, coarse_lanes)

    for f in range(2):
        for j in range(len(columns)):
            pltpu.make_async_copy(received[j], v_raw.at[f, :, j, into, :], v_sem.at[f, j]).wait()

    def deal_v(z, _):
        for f in range(2):
            for j, column in enumerate(columns):
                for i in range(tiles):
                    a_scr[f, planes + z, tile(i), column] = v_raw[f, z, j, pl.ds(i, 8, tiles), :]
        return 0

    lax.fori_loop(0, planes, deal_v, 0)

    def keep(f, _):
        for q in range(reach):
            def store(i, mean):
                keep_scr[f * reach + q, tile(i), :] = mean

            dealt_mean(lambda dz, i: a_scr[f, planes + 2 * q + dz, tile(i), :], tiles, store)
        return 0

    lax.fori_loop(0, 2, keep, 0)
    for number in range(STEPS):
        v_in, v_out = (a_scr, b_scr) if number % 2 == 0 else (b_scr, a_scr)

        def advance(z, _):
            below, above = jnp.maximum(z - 1, 0), jnp.minimum(z + 1, last_plane)

            def load(f, dz, i):
                at = z if dz == 0 else (below if dz < 0 else above)
                return v_in[f, at, tile(i), :]

            def weight(k, i):
                return w_scr[k, z, tile(i), :]

            def store(f, i, v):
                v_out[f, z, tile(i), :] = v

            step_plane(weight, load, store, rows, lanes, 2)
            return 0

        lax.fori_loop(planes - number, 2 * planes + number, advance, 0)
        for k, z, inner in ((6, planes - 1 - number, planes - number), (5, 2 * planes + number, 2 * planes + number - 1)):
            for i in range(tiles):
                w = w_scr[k, z, tile(i), :]
                for f in range(2):
                    v_out[f, z, tile(i), :] = w * v_in[f, inner, tile(i), :]
    result = a_scr if STEPS % 2 == 0 else b_scr

    scale = jnp.where(last == 1, 0.0, 1.0).astype(F32)
    for q in range(reach):
        keep_scr[q] = keep_scr[q] * scale
    zero = jnp.zeros((8, coarse_lanes), F32)
    for q in range(reach):
        def load(f, dz, i):
            at = q + dz
            return zero if at < 0 or at >= reach else keep_scr[f * reach + at, tile(i), :]

        def weight(k, i):
            return coarse_ref[k, q, tile(i), :]

        def store(f, i, v):
            own_ref[f, q, tile(i), :] = v

        step_plane(weight, load, store, coarse_rows, coarse_lanes, 2)

    def finish(f, q, put):
        dealt_mean(lambda dz, i: result[f, 2 * q + dz, tile(i), :], tiles, put)

    low_c, high_c = cc_scr[reach - 1], cc_scr[2 * reach]
    coarse_ref[0, 0] = jnp.where(low_c > 0.0, low_c + cc_scr[reach], 0.0)
    coarse_ref[0, 1] = jnp.where(high_c > 0.0, high_c + cc_scr[2 * reach - 1], 0.0)

    def own_planes(f, _):
        for q in range(reach):
            def put(i, mean):
                own_ref[f, q, tile(i), :] = mean - own_ref[f, q, tile(i), :]

            finish(f, reach + q, put)
        return 0

    lax.fori_loop(0, 2, own_planes, 0)

    def far_planes(into_ref, side, base, edge, kept):
        def one(f, _):
            for q in range(reach):
                def put(i, mean):
                    into_ref[f, q, tile(i), :] = mean

                finish(f, base + q, put)
            return 0

        lax.fori_loop(0, 2, one, 0)
        for f in range(2):
            into_ref[f, edge] = into_ref[f, edge] - coarse_ref[0, side] * keep_scr[f * reach + kept]

    @pl.when(upper == 1)
    def _():
        far_planes(to_partner_ref, 1, 2 * reach, 0, reach - 1)
        far_planes(to_other_ref, 0, 0, reach - 1, 0)

    @pl.when(upper == 0)
    def _():
        far_planes(to_partner_ref, 0, 0, reach - 1, 0)
        far_planes(to_other_ref, 1, 2 * reach, 0, reach - 1)


def weight_kernel(cc_ref, weight_ref):
    planes, rows, lanes = cc_ref.shape
    for q in range(planes - 2):
        def load(dz, i):
            return cc_ref[q + 1 + dz, tile(i), :]

        def store(k, i, w):
            weight_ref[k, q, tile(i), :] = w

        weights_plane(load, store, rows, lanes)


def sum_kernel(flag_ref, own_ref, partner_ref, other_ref, val_ref, extra_ref, to_partner_ref, to_other_ref):
    upper = flag_ref[1]
    planes = val_ref.shape[0]
    val = own_ref[0] + partner_ref[0] + other_ref[0]
    extra = own_ref[1] + partner_ref[1] + other_ref[1]
    val_ref[...] = val
    extra_ref[...] = extra
    to_partner_ref[0:planes] = val
    to_other_ref[0:planes] = val
    to_partner_ref[planes] = jnp.where(upper == 1, extra[-1], extra[0])
    to_other_ref[planes] = jnp.where(upper == 1, extra[0], extra[-1])


def coarse_advance(weight_ref, offset, source, into, count, extra, add, rows, lanes):
    for q in range(count):
        def load(f, dz, i):
            return source[q + 1 + dz, tile(i), :]

        def weight(k, i):
            return weight_ref[k, offset + q, tile(i), :]

        def store(f, i, v):
            into[q, tile(i), :] = v + add * extra[q, tile(i), :]

        step_plane(weight, load, store, rows, lanes)


def pick(flag_ref, slots, sources, sends):
    for slot, ref in zip(slots, sends):
        which = flag_ref[slot]

        @pl.when(which < 0)
        def _():
            ref[...] = jnp.zeros(ref.shape, F32)

        for m, source in enumerate(sources):
            @pl.when(which == m)
            def _():
                ref[...] = source[...]


def chain_kernel(slots, send_slots, count, edges, flag_ref, weight_ref, partner_ref, other_ref, extra_ref, *refs):
    upper = flag_ref[1]
    refs = list(refs)
    values = refs[:count]
    made = refs[count : count + len(slots)]
    rest = refs[count + len(slots) :]
    to_sides, rest = rest[: 2 * edges], rest[2 * edges :]
    sends, (wide, extra_wide, middle) = rest[: len(send_slots)], rest[len(send_slots) :]
    val_ref = values[-1]
    planes, rows, lanes = val_ref.shape
    add = [flag_ref[slot].astype(F32) for slot in slots]
    wide[planes : 2 * planes] = val_ref[...]
    sides = ((partner_ref, upper), (other_ref, 1 - upper))
    if len(slots) == 2:
        extra_wide[1 : planes + 1] = extra_ref[...]
        for ref, above in sides:
            wide[pl.ds(above * (2 * planes), planes)] = ref[0:planes]
            extra_wide[above * (planes + 1)] = ref[planes]
        coarse_advance(weight_ref, 0, wide.at[planes - 2 :], middle, planes + 2, extra_wide, add[0], rows, lanes)
        made[0][...] = middle[1 : planes + 1]
        coarse_advance(weight_ref, 1, middle, made[1], planes, extra_ref, add[1], rows, lanes)
    else:
        for ref, above in sides:
            wide[planes - 1 + above * (planes + 1)] = ref[0]
        coarse_advance(weight_ref, 1, wide.at[planes - 1 :], made[0], planes, extra_ref, add[0], rows, lanes)
    if edges:
        low, high = made[-1][0], made[-1][planes - 1]
        to_sides[0][0] = jnp.where(upper == 1, high, low)
        to_sides[1][0] = jnp.where(upper == 1, low, high)
    pick(flag_ref, send_slots, values + made, sends)


def base_kernel(iterate_ref, out_ref, rows_scr, fine_scr):
    planes, rows, lanes = iterate_ref.shape
    select, spread = pairing(lanes), spreading(lanes)
    for q in range(planes // 2):
        mean = natural_mean(iterate_ref[2 * q], iterate_ref[2 * q + 1], rows_scr, select)
        wide = split_dot(mean, spread)
        for j in range(lanes // 128):
            column = slice(128 * j, 128 * j + 128)
            fine_scr[j, pl.ds(0, rows // 2, 2), :] = wide[:, column]
            fine_scr[j, pl.ds(1, rows // 2, 2), :] = wide[:, column]
            for part in range(2):
                out_ref[2 * q + part, :, column] = iterate_ref[2 * q + part, :, column] - fine_scr[j]


def final_kernel(slots, flag_ref, base_ref, *refs):
    count = len(slots)
    pieces, out_ref, fine_scr, sum_scr, error_scr = refs[:count], *refs[count:]
    planes, rows, lanes = base_ref.shape
    spread = spreading(lanes)
    piece_rows = pieces[0].shape[1]
    tiles = piece_rows // 8
    sum_scr[...] = jnp.zeros(sum_scr.shape, F32)
    for slot, ref in zip(slots, pieces):
        side = flag_ref[slot]
        sum_scr[side] = sum_scr[side] + ref[...]
    for q in range(planes // 2):
        for j in range(lanes // 256):
            column = slice(128 * j, 128 * j + 128)
            error_scr[j] = jnp.zeros(error_scr.shape[1:], F32)
            for side in range(2):
                first = side * (rows // 2 - piece_rows)
                for i in range(tiles):
                    at = pl.ds(first + i, 8, tiles)
                    error_scr[j, at, :] = error_scr[j, at, :] + sum_scr[side, q, tile(i), column]
        error = jnp.concatenate([error_scr[j] for j in range(lanes // 256)], axis=1)
        wide = split_dot(error, spread)
        for j in range(lanes // 128):
            column = slice(128 * j, 128 * j + 128)
            fine_scr[j, pl.ds(0, rows // 2, 2), :] = wide[:, column]
            fine_scr[j, pl.ds(1, rows // 2, 2), :] = wide[:, column]
            for part in range(2):
                out_ref[2 * q + part, :, column] = base_ref[2 * q + part, :, column] + fine_scr[j]


def swap_pairs(count, first):
    pairs = []
    for i in range(first, count - 1, 2):
        pairs += [(i, i + 1), (i + 1, i)]
    return pairs


def roles(layers):
    last_group = layers // 2 - 1
    rows = []
    for t in range(layers):
        half, last = t % 2, int(t // 2 == last_group)
        adds = [int(number == (layers - 1 if last else 1)) for number in range(1, layers)]
        sends = []
        for shift in range(layers):
            k = (t + shift) % layers
            m = k if last else k - 1 - (t - half)
            sends.append(m if m >= 0 else -1)
        halves = [(t - shift) % layers % 2 for shift in range(layers)]
        rows.append([half, last, *adds, *sends, *halves])
    return rows


def local(initial, iterate, diffusivity):
    layers, slabs = lax.axis_size("tm"), lax.axis_size("space")
    t, s = lax.axis_index("tm"), lax.axis_index("space")
    planes, all_rows, lanes = initial.shape
    assert layers % 2 == 0 and slabs % 2 == 0 and planes == STEPS
    own_rows = all_rows // 2
    rows = own_rows + MARGIN
    coarse_rows, coarse_lanes = rows // 2, lanes // 2
    reach = planes // 2
    upper = 1 - s % 2
    field = iterate[0]

    def partner_swap(x):
        return lax.ppermute(x, "space", swap_pairs(slabs, 0))

    def other_swap(x):
        return lax.ppermute(x, "space", swap_pairs(slabs, 1))

    anywhere = pl.BlockSpec(memory_space=pl.ANY)
    in_hbm = pl.BlockSpec(memory_space=pltpu.HBM)
    c, to_row_partner = pl.pallas_call(
        slice_kernel,
        out_shape=(shape(planes, rows, lanes), shape(planes, own_rows, lanes)),
        in_specs=[in_hbm] * 2,
        out_specs=tuple(whole(2)),
        scratch_shapes=[pltpu.SemaphoreType.DMA((2,))],
        compiler_params=params(VMEM_LIMITS["slices"]),
        name="slices",
    )(diffusivity, field)
    row_pairs = swap_pairs(layers, 0)
    row_pairs.remove((layers - 1, layers - 2))
    received = lax.ppermute(to_row_partner, "tm", row_pairs)
    c_other = other_swap(c)
    c_partner = partner_swap(c)

    table = roles(layers)
    mine = jnp.asarray(table, jnp.int32)[t]
    flags = jnp.concatenate([mine[:1], jnp.reshape(upper, (1,)).astype(jnp.int32), mine[1:]])
    add_at, send_at, half_at = 3, 2 + layers, 2 + 2 * layers
    smem = pl.BlockSpec(memory_space=pltpu.SMEM)

    fields = shape(2, reach, coarse_rows, coarse_lanes)
    blocks = lanes // 128
    own, to_partner, to_other, cc = pl.pallas_call(
        functools.partial(fine_kernel, planes),
        out_shape=(fields, fields, fields, shape(3 * reach, coarse_rows, coarse_lanes)),
        in_specs=[smem] + [anywhere] * 3 + [in_hbm] * 2 + [anywhere],
        out_specs=tuple(whole(4)),
        scratch_shapes=[
            VMEM((3 * planes, blocks, rows, 128), F32),
            VMEM((2, planes, blocks, rows, 128), F32),
            VMEM((3 * planes, rows, lanes), F32),
            VMEM((7, 3 * planes, rows, lanes), F32),
            VMEM((2, 3 * planes, rows, lanes), F32),
            VMEM((2, 3 * planes, rows, lanes), F32),
            VMEM((7, reach, coarse_rows, coarse_lanes), F32),
            VMEM((2 * reach, coarse_rows, coarse_lanes), F32),
            pltpu.SemaphoreType.DMA((3, blocks)),
            pltpu.SemaphoreType.DMA((2, blocks)),
        ],
        compiler_params=params(VMEM_LIMITS["fine"]),
        name="fine",
    )(flags, c, c_partner, c_other, field, initial, received)

    def cost(microseconds):
        return pl.CostEstimate(flops=int(microseconds * 4e6), bytes_accessed=0, transcendentals=0)

    base = pl.pallas_call(
        base_kernel,
        out_shape=shape(planes, all_rows, lanes),
        in_specs=whole(1),
        out_specs=pl.BlockSpec(memory_space=VMEM),
        scratch_shapes=[VMEM((coarse_lanes // 128, all_rows, 128), F32), VMEM((lanes // 128, all_rows, 128), F32)],
        compiler_params=params(VMEM_LIMITS["final"]),
        cost_estimate=cost(4),
        name="base",
    )(field)

    from_other = other_swap(to_other)
    from_partner = partner_swap(to_partner)
    plane = shape(1, coarse_rows, coarse_lanes)
    block = shape(reach, coarse_rows, coarse_lanes)
    thick = shape(reach + 1, coarse_rows, coarse_lanes)
    weights = pl.pallas_call(
        weight_kernel,
        out_shape=shape(7, 3 * reach - 2, coarse_rows, coarse_lanes),
        in_specs=whole(1),
        out_specs=pl.BlockSpec(memory_space=VMEM),
        compiler_params=params(VMEM_LIMITS["small"]),
        cost_estimate=cost(2),
        name="weights",
    )(cc)
    val, extra, to_partner, to_other = pl.pallas_call(
        sum_kernel,
        out_shape=(block, block, thick, thick),
        in_specs=[smem] + whole(3),
        out_specs=tuple(whole(4)),
        compiler_params=params(VMEM_LIMITS["small"]),
        name="gather",
    )(flags, own, from_partner, from_other)

    ready = [max(row[1 + layers + shift] for row in table) for shift in range(layers)]
    arrived = [None] * layers
    values = [val]
    sent = []
    while len(values) < layers:
        from_other = other_swap(to_other)
        from_partner = partner_swap(to_partner)
        for shift, send in sent:
            pairs = [
                (source, (source + shift) % layers)
                for source in range(layers)
                if table[source][1 + layers + shift] >= 0
            ]
            arrived[shift] = lax.ppermute(send, "tm", pairs) if shift else send
        count = len(values)
        steps = 2 if count == 1 and layers > 2 else 1
        more = count + steps < layers
        slots = [add_at + count - 1 + n for n in range(steps)]
        shifts = [shift for shift in range(layers) if arrived[shift] is None and ready[shift] < count + steps]
        made = pl.pallas_call(
            functools.partial(chain_kernel, slots, [send_at + shift for shift in shifts], count, int(more)),
            out_shape=(*[block] * steps, *[plane] * (2 * more), *[block] * len(shifts)),
            in_specs=[smem] + whole(4 + count),
            out_specs=tuple(whole(steps + 2 * more + len(shifts))),
            scratch_shapes=[
                VMEM((3 * reach, coarse_rows, coarse_lanes), F32),
                VMEM((reach + 2, coarse_rows, coarse_lanes), F32),
                VMEM((reach + 2, coarse_rows, coarse_lanes), F32),
            ],
            compiler_params=params(VMEM_LIMITS["small"]),
        )(flags, weights, from_partner, from_other, extra, *values)
        values += made[:steps]
        if more:
            to_partner, to_other = made[steps : steps + 2]
        sent = list(zip(shifts, made[steps + 2 * more :]))
    for shift, send in sent:
        pairs = [
            (source, (source + shift) % layers) for source in range(layers) if table[source][1 + layers + shift] >= 0
        ]
        arrived[shift] = lax.ppermute(send, "tm", pairs) if shift else send

    corrected = pl.pallas_call(
        functools.partial(final_kernel, [half_at + shift for shift in range(layers)]),
        out_shape=shape(planes, all_rows, lanes),
        in_specs=[smem] + whole(1 + layers),
        out_specs=pl.BlockSpec(memory_space=VMEM),
        scratch_shapes=[
            VMEM((lanes // 128, all_rows, 128), F32),
            VMEM((2, reach, coarse_rows, coarse_lanes), F32),
            VMEM((coarse_lanes // 128, all_rows // 2, 128), F32),
        ],
        compiler_params=params(VMEM_LIMITS["final"]),
        name="final",
    )(flags, base, *arrived)
    return corrected[None]


def solution(mesh):
    placed = (P("space", None, None), P("tm", "space", None, None), P("space", None, None))

    return jax.shard_map(local, mesh=mesh, in_specs=placed, out_specs=P("tm", "space", None, None), check_vma=False)
```

```python
import functools

import jax
import jax.numpy as jnp
from jax import lax
from jax.experimental import pallas as pl
from jax.experimental.pallas import tpu as pltpu
from jax.sharding import PartitionSpec as P


STEPS = 4
courant = 0.15
GAIN = 0.5 * courant
MARGIN = 16
F32 = jnp.float32
VMEM = pltpu.VMEM
MIB = 1024 * 1024
VMEM_LIMITS = {"slices": 50 * MIB, "near": 6 * MIB, "fine": 34 * MIB, "small": 10 * MIB, "final": 16 * MIB}


def params(limit):
    return pltpu.CompilerParams(vmem_limit_bytes=limit)


def whole(count):
    return [pl.BlockSpec(memory_space=VMEM)] * count


def shape(*dims):
    return jax.ShapeDtypeStruct(dims, F32)


def split_dot(x, selection):
    high = x.astype(jnp.bfloat16)
    rest = x - high.astype(F32)
    middle = rest.astype(jnp.bfloat16)
    low = (rest - middle.astype(F32)).astype(jnp.bfloat16)
    dot = functools.partial(jnp.dot, preferred_element_type=F32)
    return dot(high, selection) + dot(middle, selection) + dot(low, selection)


def pairing(width):
    fine = lax.broadcasted_iota(jnp.int32, (width, width // 2), 0)
    coarse = lax.broadcasted_iota(jnp.int32, (width, width // 2), 1)
    return jnp.where((fine == 2 * coarse) | (fine == 2 * coarse + 1), 1.0, 0.0).astype(jnp.bfloat16)


def spreading(width):
    coarse = lax.broadcasted_iota(jnp.int32, (width // 2, width), 0)
    fine = lax.broadcasted_iota(jnp.int32, (width // 2, width), 1)
    return jnp.where((fine == 2 * coarse) | (fine == 2 * coarse + 1), 1.0, 0.0).astype(jnp.bfloat16)


def natural_mean(first, second, rows_scr, select):
    rows = first.shape[0]
    lanes = split_dot(first + second, select)
    parts = []
    for j in range(lanes.shape[1] // 128):
        rows_scr[j, 0:rows, :] = lanes[:, 128 * j : 128 * j + 128]
        even = rows_scr[j, pl.ds(0, rows // 2, 2), :]
        odd = rows_scr[j, pl.ds(1, rows // 2, 2), :]
        parts.append(0.125 * (even + odd))
    return jnp.concatenate(parts, axis=1)


def tile(i):
    return slice(8 * i, 8 * i + 8)


def pair_lanes(blocks):
    lane = lax.broadcasted_iota(jnp.int32, (8, 128), 1)
    place = 2 * (lane % 64)
    out = []
    for first, second in zip(blocks[::2], blocks[1::2]):
        halves = [
            jnp.take_along_axis(x + pltpu.roll(x, 127, 1), place, axis=1, mode="promise_in_bounds") for x in (first, second)
        ]
        out.append(jnp.where(lane < 64, *halves))
    return out


def dealt_mean(load, tiles, store):
    for i in range(tiles // 2):
        total = (load(0, 2 * i) + load(1, 2 * i)) + (load(0, 2 * i + 1) + load(1, 2 * i + 1))
        blocks = [total[:, 128 * j : 128 * j + 128] for j in range(total.shape[1] // 128)]
        store(i, 0.125 * jnp.concatenate(pair_lanes(blocks), axis=1))


def weights_plane(load, store, rows, lanes):
    sub = lax.broadcasted_iota(jnp.int32, (8, 128), 0)
    lane = lax.broadcasted_iota(jnp.int32, (8, 128), 1)
    tiles, blocks = rows // 8, lanes // 128

    def cut(x):
        return [x[:, 128 * j : 128 * j + 128] for j in range(blocks)]

    c = cut(load(0, 0))
    below = [pltpu.roll(x, 1, 0) for x in cut(load(0, tiles - 1))]
    wrapped = [pltpu.roll(x, 7, 0) for x in c]
    for i in range(tiles):
        above = cut(load(0, i + 1)) if i + 1 < tiles else wrapped
        czm, czp = cut(load(-1, i)), cut(load(1, i))
        right = [pltpu.roll(x, 1, 1) for x in c]
        left = [pltpu.roll(x, 127, 1) for x in c]
        w = [[] for _ in range(7)]
        for j in range(blocks):
            mid = c[j]
            xm = mid + jnp.where(lane == 0, right[j - 1] if j else 0.0, right[j])
            xp = mid + jnp.where(lane == 127, left[j + 1] if j + 1 < blocks else 0.0, left[j])
            ym = mid + (jnp.where(sub == 0, 0.0, below[j]) if i == 0 else below[j])
            yp = mid + (jnp.where(sub == 7, 0.0, above[j]) if i + 1 == tiles else above[j])
            zm, zp = mid + czm[j], mid + czp[j]
            w[0].append(1.0 - ((xm + xp) + (ym + yp) + (zm + zp)))
            w[1].append(xm if j else jnp.where(lane == 0, 0.0, xm))
            w[2].append(xp if j + 1 < blocks else jnp.where(lane == 127, 0.0, xp))
            w[3].append(jnp.where(sub == 0, 0.0, ym) if i == 0 else ym)
            w[4].append(jnp.where(sub == 7, 0.0, yp) if i + 1 == tiles else yp)
            inside = mid > 0.0
            w[5].append(jnp.where(inside, zm, 0.0))
            w[6].append(jnp.where(inside, zp, 0.0))
        for k in range(7):
            store(k, i, jnp.concatenate(w[k], axis=1))
        below, c = c, above


def step_plane(weight, load, store, rows, lanes, fields=1):
    tiles = rows // 8
    below = [pltpu.roll(load(f, 0, tiles - 1), 1, 0) for f in range(fields)]
    center = [load(f, 0, 0) for f in range(fields)]
    wrapped = [pltpu.roll(v, 7, 0) for v in center]
    for i in range(tiles):
        w = [weight(k, i) for k in range(7)]
        for f in range(fields):
            mid = center[f]
            above = load(f, 0, i + 1) if i + 1 < tiles else wrapped[f]
            xm = pltpu.roll(mid, 1, 1)
            xp = pltpu.roll(mid, lanes - 1, 1)
            out = w[0] * mid
            out = out + (w[1] * xm + w[2] * xp)
            out = out + (w[3] * below[f] + w[4] * above)
            out = out + (w[5] * load(f, -1, i) + w[6] * load(f, 1, i))
            store(f, i, out)
            below[f], center[f] = mid, above


def at_row(value, step):
    return pl.multiple_of(value * step, 8)


def slice_kernel(c_hbm, iterate_hbm, c_ref, send_ref, sem):
    half = lax.rem(lax.axis_index("tm"), 2)
    own = send_ref.shape[1]
    window = pl.ds(at_row(half, c_hbm.shape[1] - c_ref.shape[1]), c_ref.shape[1])
    send = pltpu.make_async_copy(iterate_hbm.at[:, pl.ds(at_row(1 - half, own), own), :], send_ref, sem.at[0])
    keep = pltpu.make_async_copy(c_hbm.at[:, window, :], c_ref, sem.at[1])
    send.start()
    keep.start()
    send.wait()
    keep.wait()


def weigh_planes(c_ref, w_refs, shift, count):
    planes, rows, lanes = c_ref.shape
    tiles = rows // 8

    def one(n, _):
        def load(dz, i):
            return c_ref[n + 1 + dz, tile(i), :]

        def store(k, i, w):
            w_refs[k][n + 1 - shift, tile(i), :] = w

        weights_plane(load, store, rows, lanes)
        return 0

    lax.fori_loop(0, count, one, 0)

    def edge(k, z, inner, at):
        for i in range(tiles):
            c = c_ref[z, tile(i), :]
            w_refs[k][at, tile(i), :] = jnp.where(c > 0.0, c + c_ref[inner, tile(i), :], 0.0)

    @pl.when(shift == 1)
    def _():
        edge(5, planes - 1, planes - 2, planes - 2)

    @pl.when(shift == 0)
    def _():
        edge(6, 0, 1, 0)


def deal_planes(raw, c_ref, start, count):
    tiles, blocks = c_ref.shape[1] // 8, raw.shape[1]

    def one(z, _):
        for j in range(blocks):
            for i in range(tiles):
                c_ref[start + z, tile(i), 128 * j : 128 * j + 128] = GAIN * raw[z, j, pl.ds(i, 8, tiles), :]
        return 0

    lax.fori_loop(0, count, one, 0)


def coarse_means(c_ref, c_start, cc_ref, cc_start, count, reach):
    tiles = c_ref.shape[1] // 8

    def one(n, _):
        for q in range(reach):
            at = n * reach + q

            def store(i, mean):
                cc_ref[cc_start + at, tile(i), :] = mean

            dealt_mean(lambda dz, i: c_ref[c_start + 2 * at + dz, tile(i), :], tiles, store)
        return 0

    lax.fori_loop(0, count // reach, one, 0)


def near_kernel(planes, flag_ref, c_hbm, partner_hbm, *refs):
    w_refs, (edge_ref, cc_ref, c_ref, raw, sem) = refs[:7], refs[7:]
    upper = flag_ref[1]
    blocks, reach = raw.shape[1], planes // 2
    copies = [
        pltpu.make_async_copy(ref.at[:, :, 128 * j : 128 * j + 128], raw.at[planes * n : planes * (n + 1), j], sem.at[n, j])
        for n, ref in enumerate((c_hbm, partner_hbm))
        for j in range(blocks)
    ]
    for copy in copies:
        copy.start()
    for copy in copies:
        copy.wait()
    deal_planes(raw.at[0:planes], c_ref, (1 - upper) * planes, planes)
    deal_planes(raw.at[planes:], c_ref, upper * planes, planes)
    weigh_planes(c_ref, w_refs, upper, 2 * planes - 2)
    coarse_means(c_ref, 0, cc_ref, 0, 2 * reach, reach)
    edge_ref[...] = c_ref[pl.ds((1 - upper) * (2 * planes - 2), 2)]


def fine_kernel(planes, flag_ref, other_hbm, iterate_hbm, initial_hbm, received_hbm, *refs):
    near_w, (edge_c, near_cc), refs = refs[:7], refs[7:9], refs[9:]
    own_ref, to_partner_ref, to_other_ref, cc_scr, c_raw, v_raw, far_c, far_w, a_scr, b_scr = refs[:10]
    coarse_ref, keep_scr, c_sem, v_sem = refs[10:]
    far_w = [far_w.at[k] for k in range(7)]
    half, upper, last = flag_ref[0], flag_ref[1], flag_ref[2]
    rows, lanes = edge_c.shape[1:]
    own_rows = rows - MARGIN
    tiles = rows // 8
    columns = [slice(128 * j, 128 * j + 128) for j in range(lanes // 128)]
    reach = planes // 2
    coarse_rows, coarse_lanes = rows // 2, lanes // 2

    c_copies = [
        pltpu.make_async_copy(other_hbm.at[:, :, column], c_raw.at[:, j], c_sem.at[j]) for j, column in enumerate(columns)
    ]
    for copy in c_copies:
        copy.start()
    into = pl.ds(at_row(half, MARGIN), own_rows)
    source = pl.ds(at_row(half, own_rows), own_rows)

    def fetch(ref, f):
        for j in range(len(columns)):
            pltpu.make_async_copy(ref[j], v_raw.at[f, :, j, into, :], v_sem.at[f, j]).start()

    def halves(ref):
        return [ref.at[:, source, column] for column in columns]

    received = [received_hbm.at[:, :, column] for column in columns]

    first_kept = (last == 0) & (half == 0)
    first_got = (last == 0) & (half == 1)
    second_kept = (last == 1) == (half == 0)
    for f, choices in enumerate(
        (
            ((last == 1, halves(initial_hbm)), (first_kept, halves(iterate_hbm)), (first_got, received)),
            ((second_kept, halves(iterate_hbm)), (jnp.logical_not(second_kept), received)),
        )
    ):
        for condition, ref in choices:
            @pl.when(condition)
            def _():
                fetch(ref, f)

    outside = pl.ds(at_row(1 - half, own_rows), MARGIN)
    v_raw[:, :, :, outside, :] = jnp.zeros(v_raw.shape[:3] + (MARGIN, 128), F32)
    idle = jnp.zeros((2,) + a_scr.shape[2:], F32)
    for number in range(STEPS):
        v_in = (a_scr, b_scr)[number % 2]
        v_in[:, planes - 1 - number] = idle
        v_in[:, 2 * planes + number] = idle
    for copy in c_copies:
        copy.wait()

    deal_planes(c_raw, far_c, (1 - upper) * 2, planes)
    far_c[pl.ds(upper * planes, 2)] = edge_c[...]
    weigh_planes(far_c, far_w, 1 - upper, planes)
    cc_scr[pl.ds(upper * reach, 2 * reach)] = near_cc[...]
    coarse_means(far_c, (1 - upper) * 2, cc_scr, (1 - upper) * (2 * reach), reach, reach)
    for q in range(reach):
        def load(dz, i):
            return cc_scr[reach + q + dz, tile(i), :]

        def store(k, i, w):
            coarse_ref[k, q, tile(i), :] = w

        weights_plane(load, store, coarse_rows, coarse_lanes)

    for f in range(2):
        for j in range(len(columns)):
            pltpu.make_async_copy(received[j], v_raw.at[f, :, j, into, :], v_sem.at[f, j]).wait()

    def deal_v(z, _):
        for f in range(2):
            for j, column in enumerate(columns):
                for i in range(tiles):
                    a_scr[f, planes + z, tile(i), column] = v_raw[f, z, j, pl.ds(i, 8, tiles), :]
        return 0

    lax.fori_loop(0, planes, deal_v, 0)

    def keep(f, _):
        for q in range(reach):
            def store(i, mean):
                keep_scr[f * reach + q, tile(i), :] = mean

            dealt_mean(lambda dz, i: a_scr[f, planes + 2 * q + dz, tile(i), :], tiles, store)
        return 0

    lax.fori_loop(0, 2, keep, 0)
    near_at, far_at = upper * (planes + 1), (1 - upper) * (2 * planes - 1)
    for number in range(STEPS):
        v_in, v_out = (a_scr, b_scr) if number % 2 == 0 else (b_scr, a_scr)
        low, high = planes - number, 2 * planes + number

        def advance_all(w_refs, w_at, start, count):
            def advance(n, _):
                z = start + n

                def load(f, dz, i):
                    return v_in[f, z + dz, tile(i), :]

                def weight(k, i):
                    return w_refs[k][z - w_at, tile(i), :]

                def store(f, i, v):
                    v_out[f, z, tile(i), :] = v

                step_plane(weight, load, store, rows, lanes, 2)
                return 0

            lax.fori_loop(0, count, advance, 0)

        advance_all(near_w, near_at, jnp.where(upper == 1, planes + 1, low), planes - 1 + number)
        advance_all(far_w, far_at, jnp.where(upper == 1, low, 2 * planes - 1), 1 + number)

        def reach_out(w_ref, w_at, z, inner):
            for i in range(tiles):
                w = w_ref[z - w_at, tile(i), :]
                for f in range(2):
                    v_out[f, z, tile(i), :] = w * v_in[f, inner, tile(i), :]

        @pl.when(upper == 1)
        def _():
            reach_out(far_w[6], 0, low - 1, low)
            reach_out(near_w[5], planes + 1, high, high - 1)

        @pl.when(upper == 0)
        def _():
            reach_out(near_w[6], 0, low - 1, low)
            reach_out(far_w[5], 2 * planes - 1, high, high - 1)

    result = a_scr if STEPS % 2 == 0 else b_scr

    scale = jnp.where(last == 1, 0.0, 1.0).astype(F32)
    for q in range(reach):
        keep_scr[q] = keep_scr[q] * scale
    zero = jnp.zeros((8, coarse_lanes), F32)
    for q in range(reach):
        def load(f, dz, i):
            at = q + dz
            return zero if at < 0 or at >= reach else keep_scr[f * reach + at, tile(i), :]

        def weight(k, i):
            return coarse_ref[k, q, tile(i), :]

        def store(f, i, v):
            own_ref[f, q, tile(i), :] = v

        step_plane(weight, load, store, coarse_rows, coarse_lanes, 2)

    def finish(f, q, put):
        dealt_mean(lambda dz, i: result[f, 2 * q + dz, tile(i), :], tiles, put)

    low_c, high_c = cc_scr[reach - 1], cc_scr[2 * reach]
    coarse_ref[0, 0] = jnp.where(low_c > 0.0, low_c + cc_scr[reach], 0.0)
    coarse_ref[0, 1] = jnp.where(high_c > 0.0, high_c + cc_scr[2 * reach - 1], 0.0)

    def own_planes(f, _):
        for q in range(reach):
            def put(i, mean):
                own_ref[f, q, tile(i), :] = mean - own_ref[f, q, tile(i), :]

            finish(f, reach + q, put)
        return 0

    lax.fori_loop(0, 2, own_planes, 0)

    def far_planes(into_ref, side, base, edge, kept):
        def one(f, _):
            for q in range(reach):
                def put(i, mean):
                    into_ref[f, q, tile(i), :] = mean

                finish(f, base + q, put)
            return 0

        lax.fori_loop(0, 2, one, 0)
        for f in range(2):
            into_ref[f, edge] = into_ref[f, edge] - coarse_ref[0, side] * keep_scr[f * reach + kept]

    @pl.when(upper == 1)
    def _():
        far_planes(to_partner_ref, 1, 2 * reach, 0, reach - 1)
        far_planes(to_other_ref, 0, 0, reach - 1, 0)

    @pl.when(upper == 0)
    def _():
        far_planes(to_partner_ref, 0, 0, reach - 1, 0)
        far_planes(to_other_ref, 1, 2 * reach, 0, reach - 1)


def weight_kernel(cc_ref, weight_ref):
    planes, rows, lanes = cc_ref.shape
    for q in range(planes - 2):
        def load(dz, i):
            return cc_ref[q + 1 + dz, tile(i), :]

        def store(k, i, w):
            weight_ref[k, q, tile(i), :] = w

        weights_plane(load, store, rows, lanes)


def sum_kernel(flag_ref, own_ref, partner_ref, other_ref, val_ref, extra_ref, to_partner_ref, to_other_ref):
    upper = flag_ref[1]
    planes = val_ref.shape[0]
    val = own_ref[0] + partner_ref[0] + other_ref[0]
    extra = own_ref[1] + partner_ref[1] + other_ref[1]
    val_ref[...] = val
    extra_ref[...] = extra
    to_partner_ref[0:planes] = val
    to_other_ref[0:planes] = val
    to_partner_ref[planes] = jnp.where(upper == 1, extra[-1], extra[0])
    to_other_ref[planes] = jnp.where(upper == 1, extra[0], extra[-1])


def coarse_advance(weight_ref, offset, source, into, count, extra, add, rows, lanes):
    for q in range(count):
        def load(f, dz, i):
            return source[q + 1 + dz, tile(i), :]

        def weight(k, i):
            return weight_ref[k, offset + q, tile(i), :]

        def store(f, i, v):
            into[q, tile(i), :] = v + add * extra[q, tile(i), :]

        step_plane(weight, load, store, rows, lanes)


def pick(flag_ref, slots, sources, sends):
    for slot, ref in zip(slots, sends):
        which = flag_ref[slot]

        @pl.when(which < 0)
        def _():
            ref[...] = jnp.zeros(ref.shape, F32)

        for m, source in enumerate(sources):
            @pl.when(which == m)
            def _():
                ref[...] = source[...]


def chain_kernel(slots, send_slots, count, edges, flag_ref, weight_ref, partner_ref, other_ref, extra_ref, *refs):
    upper = flag_ref[1]
    refs = list(refs)
    values = refs[:count]
    made = refs[count : count + len(slots)]
    rest = refs[count + len(slots) :]
    to_sides, rest = rest[: 2 * edges], rest[2 * edges :]
    sends, (wide, extra_wide, middle) = rest[: len(send_slots)], rest[len(send_slots) :]
    val_ref = values[-1]
    planes, rows, lanes = val_ref.shape
    add = [flag_ref[slot].astype(F32) for slot in slots]
    wide[planes : 2 * planes] = val_ref[...]
    sides = ((partner_ref, upper), (other_ref, 1 - upper))
    if len(slots) == 2:
        extra_wide[1 : planes + 1] = extra_ref[...]
        for ref, above in sides:
            wide[pl.ds(above * (2 * planes), planes)] = ref[0:planes]
            extra_wide[above * (planes + 1)] = ref[planes]
        coarse_advance(weight_ref, 0, wide.at[planes - 2 :], middle, planes + 2, extra_wide, add[0], rows, lanes)
        made[0][...] = middle[1 : planes + 1]
        coarse_advance(weight_ref, 1, middle, made[1], planes, extra_ref, add[1], rows, lanes)
    else:
        for ref, above in sides:
            wide[planes - 1 + above * (planes + 1)] = ref[0]
        coarse_advance(weight_ref, 1, wide.at[planes - 1 :], made[0], planes, extra_ref, add[0], rows, lanes)
    if edges:
        low, high = made[-1][0], made[-1][planes - 1]
        to_sides[0][0] = jnp.where(upper == 1, high, low)
        to_sides[1][0] = jnp.where(upper == 1, low, high)
    pick(flag_ref, send_slots, values + made, sends)


def base_kernel(iterate_ref, out_ref, rows_scr, fine_scr):
    planes, rows, lanes = iterate_ref.shape
    select, spread = pairing(lanes), spreading(lanes)
    for q in range(planes // 2):
        mean = natural_mean(iterate_ref[2 * q], iterate_ref[2 * q + 1], rows_scr, select)
        wide = split_dot(mean, spread)
        for j in range(lanes // 128):
            column = slice(128 * j, 128 * j + 128)
            fine_scr[j, pl.ds(0, rows // 2, 2), :] = wide[:, column]
            fine_scr[j, pl.ds(1, rows // 2, 2), :] = wide[:, column]
            for part in range(2):
                out_ref[2 * q + part, :, column] = iterate_ref[2 * q + part, :, column] - fine_scr[j]


def final_kernel(slots, flag_ref, base_ref, *refs):
    count = len(slots)
    pieces, out_ref, fine_scr, sum_scr, error_scr = refs[:count], *refs[count:]
    planes, rows, lanes = base_ref.shape
    spread = spreading(lanes)
    piece_rows = pieces[0].shape[1]
    tiles = piece_rows // 8
    sum_scr[...] = jnp.zeros(sum_scr.shape, F32)
    for slot, ref in zip(slots, pieces):
        side = flag_ref[slot]
        sum_scr[side] = sum_scr[side] + ref[...]
    for q in range(planes // 2):
        for j in range(lanes // 256):
            column = slice(128 * j, 128 * j + 128)
            error_scr[j] = jnp.zeros(error_scr.shape[1:], F32)
            for side in range(2):
                first = side * (rows // 2 - piece_rows)
                for i in range(tiles):
                    at = pl.ds(first + i, 8, tiles)
                    error_scr[j, at, :] = error_scr[j, at, :] + sum_scr[side, q, tile(i), column]
        error = jnp.concatenate([error_scr[j] for j in range(lanes // 256)], axis=1)
        wide = split_dot(error, spread)
        for j in range(lanes // 128):
            column = slice(128 * j, 128 * j + 128)
            fine_scr[j, pl.ds(0, rows // 2, 2), :] = wide[:, column]
            fine_scr[j, pl.ds(1, rows // 2, 2), :] = wide[:, column]
            for part in range(2):
                out_ref[2 * q + part, :, column] = base_ref[2 * q + part, :, column] + fine_scr[j]


def swap_pairs(count, first):
    pairs = []
    for i in range(first, count - 1, 2):
        pairs += [(i, i + 1), (i + 1, i)]
    return pairs


def roles(layers):
    last_group = layers // 2 - 1
    rows = []
    for t in range(layers):
        half, last = t % 2, int(t // 2 == last_group)
        adds = [int(number == (layers - 1 if last else 1)) for number in range(1, layers)]
        sends = []
        for shift in range(layers):
            k = (t + shift) % layers
            m = k if last else k - 1 - (t - half)
            sends.append(m if m >= 0 else -1)
        halves = [(t - shift) % layers % 2 for shift in range(layers)]
        rows.append([half, last, *adds, *sends, *halves])
    return rows


def local(initial, iterate, diffusivity):
    layers, slabs = lax.axis_size("tm"), lax.axis_size("space")
    t, s = lax.axis_index("tm"), lax.axis_index("space")
    planes, all_rows, lanes = initial.shape
    assert layers % 2 == 0 and slabs % 2 == 0 and planes == STEPS
    own_rows = all_rows // 2
    rows = own_rows + MARGIN
    coarse_rows, coarse_lanes = rows // 2, lanes // 2
    reach = planes // 2
    upper = 1 - s % 2
    field = iterate[0]

    def partner_swap(x):
        return lax.ppermute(x, "space", swap_pairs(slabs, 0))

    def other_swap(x):
        return lax.ppermute(x, "space", swap_pairs(slabs, 1))

    anywhere = pl.BlockSpec(memory_space=pl.ANY)
    in_hbm = pl.BlockSpec(memory_space=pltpu.HBM)
    c, to_row_partner = pl.pallas_call(
        slice_kernel,
        out_shape=(shape(planes, rows, lanes), shape(planes, own_rows, lanes)),
        in_specs=[in_hbm] * 2,
        out_specs=tuple(whole(2)),
        scratch_shapes=[pltpu.SemaphoreType.DMA((2,))],
        compiler_params=params(VMEM_LIMITS["slices"]),
        name="slices",
    )(diffusivity, field)
    row_pairs = swap_pairs(layers, 0)
    row_pairs.remove((layers - 1, layers - 2))
    received = lax.ppermute(to_row_partner, "tm", row_pairs)
    c_other = other_swap(c)
    c_partner = partner_swap(c)

    table = roles(layers)
    mine = jnp.asarray(table, jnp.int32)[t]
    flags = jnp.concatenate([mine[:1], jnp.reshape(upper, (1,)).astype(jnp.int32), mine[1:]])
    add_at, send_at, half_at = 3, 2 + layers, 2 + 2 * layers
    smem = pl.BlockSpec(memory_space=pltpu.SMEM)

    def cost(microseconds):
        return pl.CostEstimate(flops=int(microseconds * 4e6), bytes_accessed=0, transcendentals=0)

    fields = shape(2, reach, coarse_rows, coarse_lanes)
    blocks = lanes // 128
    prepared = pl.pallas_call(
        functools.partial(near_kernel, planes),
        out_shape=(
            *[shape(2 * planes - 1, rows, lanes)] * 7,
            shape(2, rows, lanes),
            shape(2 * reach, coarse_rows, coarse_lanes),
        ),
        in_specs=[smem] + [anywhere] * 2,
        out_specs=tuple(whole(9)),
        scratch_shapes=[
            VMEM((2 * planes, rows, lanes), F32),
            VMEM((2 * planes, blocks, rows, 128), F32),
            pltpu.SemaphoreType.DMA((2, blocks)),
        ],
        compiler_params=params(VMEM_LIMITS["near"]),
        cost_estimate=cost(6),
        name="near",
    )(flags, c, c_partner)
    own, to_partner, to_other, cc = pl.pallas_call(
        functools.partial(fine_kernel, planes),
        out_shape=(fields, fields, fields, shape(3 * reach, coarse_rows, coarse_lanes)),
        in_specs=[smem] + [anywhere] + [in_hbm] * 2 + [anywhere] + whole(9),
        out_specs=tuple(whole(4)),
        scratch_shapes=[
            VMEM((planes, blocks, rows, 128), F32),
            VMEM((2, planes, blocks, rows, 128), F32),
            VMEM((planes + 2, rows, lanes), F32),
            VMEM((7, planes + 1, rows, lanes), F32),
            VMEM((2, 3 * planes, rows, lanes), F32),
            VMEM((2, 3 * planes, rows, lanes), F32),
            VMEM((7, reach, coarse_rows, coarse_lanes), F32),
            VMEM((2 * reach, coarse_rows, coarse_lanes), F32),
            pltpu.SemaphoreType.DMA((blocks,)),
            pltpu.SemaphoreType.DMA((2, blocks)),
        ],
        compiler_params=params(VMEM_LIMITS["fine"]),
        name="fine",
    )(flags, c_other, field, initial, received, *prepared)

    base = pl.pallas_call(
        base_kernel,
        out_shape=shape(planes, all_rows, lanes),
        in_specs=whole(1),
        out_specs=pl.BlockSpec(memory_space=VMEM),
        scratch_shapes=[VMEM((coarse_lanes // 128, all_rows, 128), F32), VMEM((lanes // 128, all_rows, 128), F32)],
        compiler_params=params(VMEM_LIMITS["final"]),
        cost_estimate=cost(4),
        name="base",
    )(field)

    from_other = other_swap(to_other)
    from_partner = partner_swap(to_partner)
    plane = shape(1, coarse_rows, coarse_lanes)
    block = shape(reach, coarse_rows, coarse_lanes)
    thick = shape(reach + 1, coarse_rows, coarse_lanes)
    weights = pl.pallas_call(
        weight_kernel,
        out_shape=shape(7, 3 * reach - 2, coarse_rows, coarse_lanes),
        in_specs=whole(1),
        out_specs=pl.BlockSpec(memory_space=VMEM),
        compiler_params=params(VMEM_LIMITS["small"]),
        cost_estimate=cost(2),
        name="weights",
    )(cc)
    val, extra, to_partner, to_other = pl.pallas_call(
        sum_kernel,
        out_shape=(block, block, thick, thick),
        in_specs=[smem] + whole(3),
        out_specs=tuple(whole(4)),
        compiler_params=params(VMEM_LIMITS["small"]),
        name="gather",
    )(flags, own, from_partner, from_other)

    ready = [max(row[1 + layers + shift] for row in table) for shift in range(layers)]
    arrived = [None] * layers
    values = [val]
    sent = []
    while len(values) < layers:
        from_other = other_swap(to_other)
        from_partner = partner_swap(to_partner)
        for shift, send in sent:
            pairs = [
                (source, (source + shift) % layers)
                for source in range(layers)
                if table[source][1 + layers + shift] >= 0
            ]
            arrived[shift] = lax.ppermute(send, "tm", pairs) if shift else send
        count = len(values)
        steps = 2 if count == 1 and layers > 2 else 1
        more = count + steps < layers
        slots = [add_at + count - 1 + n for n in range(steps)]
        shifts = [shift for shift in range(layers) if arrived[shift] is None and ready[shift] < count + steps]
        made = pl.pallas_call(
            functools.partial(chain_kernel, slots, [send_at + shift for shift in shifts], count, int(more)),
            out_shape=(*[block] * steps, *[plane] * (2 * more), *[block] * len(shifts)),
            in_specs=[smem] + whole(4 + count),
            out_specs=tuple(whole(steps + 2 * more + len(shifts))),
            scratch_shapes=[
                VMEM((3 * reach, coarse_rows, coarse_lanes), F32),
                VMEM((reach + 2, coarse_rows, coarse_lanes), F32),
                VMEM((reach + 2, coarse_rows, coarse_lanes), F32),
            ],
            compiler_params=params(VMEM_LIMITS["small"]),
        )(flags, weights, from_partner, from_other, extra, *values)
        values += made[:steps]
        if more:
            to_partner, to_other = made[steps : steps + 2]
        sent = list(zip(shifts, made[steps + 2 * more :]))
    for shift, send in sent:
        pairs = [
            (source, (source + shift) % layers) for source in range(layers) if table[source][1 + layers + shift] >= 0
        ]
        arrived[shift] = lax.ppermute(send, "tm", pairs) if shift else send

    corrected = pl.pallas_call(
        functools.partial(final_kernel, [half_at + shift for shift in range(layers)]),
        out_shape=shape(planes, all_rows, lanes),
        in_specs=[smem] + whole(1 + layers),
        out_specs=pl.BlockSpec(memory_space=VMEM),
        scratch_shapes=[
            VMEM((lanes // 128, all_rows, 128), F32),
            VMEM((2, reach, coarse_rows, coarse_lanes), F32),
            VMEM((coarse_lanes // 128, all_rows // 2, 128), F32),
        ],
        compiler_params=params(VMEM_LIMITS["final"]),
        name="final",
    )(flags, base, *arrived)
    return corrected[None]


def solution(mesh):
    placed = (P("space", None, None), P("tm", "space", None, None), P("space", None, None))

    return jax.shard_map(local, mesh=mesh, in_specs=placed, out_specs=P("tm", "space", None, None), check_vma=False)
```

```python
import functools

import jax
import jax.numpy as jnp
from jax import lax
from jax.experimental import pallas as pl
from jax.experimental.pallas import tpu as pltpu
from jax.sharding import PartitionSpec as P


STEPS = 4
courant = 0.15
GAIN = 0.5 * courant
MARGIN = 16
F32 = jnp.float32
VMEM = pltpu.VMEM
MIB = 1024 * 1024
VMEM_LIMITS = {"slices": 50 * MIB, "near": 6 * MIB, "fine": 34 * MIB, "small": 10 * MIB, "final": 16 * MIB}


def params(limit):
    return pltpu.CompilerParams(vmem_limit_bytes=limit)


def whole(count):
    return [pl.BlockSpec(memory_space=VMEM)] * count


def shape(*dims):
    return jax.ShapeDtypeStruct(dims, F32)


def split_dot(x, selection):
    high = x.astype(jnp.bfloat16)
    rest = x - high.astype(F32)
    middle = rest.astype(jnp.bfloat16)
    low = (rest - middle.astype(F32)).astype(jnp.bfloat16)
    dot = functools.partial(jnp.dot, preferred_element_type=F32)
    return dot(high, selection) + dot(middle, selection) + dot(low, selection)


def pairing(width):
    fine = lax.broadcasted_iota(jnp.int32, (width, width // 2), 0)
    coarse = lax.broadcasted_iota(jnp.int32, (width, width // 2), 1)
    return jnp.where((fine == 2 * coarse) | (fine == 2 * coarse + 1), 1.0, 0.0).astype(jnp.bfloat16)


def spreading(width):
    coarse = lax.broadcasted_iota(jnp.int32, (width // 2, width), 0)
    fine = lax.broadcasted_iota(jnp.int32, (width // 2, width), 1)
    return jnp.where((fine == 2 * coarse) | (fine == 2 * coarse + 1), 1.0, 0.0).astype(jnp.bfloat16)


def natural_mean(first, second, rows_scr, select):
    rows = first.shape[0]
    lanes = split_dot(first + second, select)
    parts = []
    for j in range(lanes.shape[1] // 128):
        rows_scr[j, 0:rows, :] = lanes[:, 128 * j : 128 * j + 128]
        even = rows_scr[j, pl.ds(0, rows // 2, 2), :]
        odd = rows_scr[j, pl.ds(1, rows // 2, 2), :]
        parts.append(0.125 * (even + odd))
    return jnp.concatenate(parts, axis=1)


def tile(i):
    return slice(8 * i, 8 * i + 8)


def pair_lanes(blocks):
    lane = lax.broadcasted_iota(jnp.int32, (8, 128), 1)
    place = 2 * (lane % 64)
    out = []
    for first, second in zip(blocks[::2], blocks[1::2]):
        halves = [
            jnp.take_along_axis(x + pltpu.roll(x, 127, 1), place, axis=1, mode="promise_in_bounds") for x in (first, second)
        ]
        out.append(jnp.where(lane < 64, *halves))
    return out


def dealt_mean(load, tiles, store):
    for i in range(tiles // 2):
        total = (load(0, 2 * i) + load(1, 2 * i)) + (load(0, 2 * i + 1) + load(1, 2 * i + 1))
        blocks = [total[:, 128 * j : 128 * j + 128] for j in range(total.shape[1] // 128)]
        store(i, 0.125 * jnp.concatenate(pair_lanes(blocks), axis=1))


def weights_plane(load, store, rows, lanes):
    sub = lax.broadcasted_iota(jnp.int32, (8, 128), 0)
    lane = lax.broadcasted_iota(jnp.int32, (8, 128), 1)
    tiles, blocks = rows // 8, lanes // 128

    def cut(x):
        return [x[:, 128 * j : 128 * j + 128] for j in range(blocks)]

    c = cut(load(0, 0))
    below = [pltpu.roll(x, 1, 0) for x in cut(load(0, tiles - 1))]
    wrapped = [pltpu.roll(x, 7, 0) for x in c]
    for i in range(tiles):
        above = cut(load(0, i + 1)) if i + 1 < tiles else wrapped
        czm, czp = cut(load(-1, i)), cut(load(1, i))
        right = [pltpu.roll(x, 1, 1) for x in c]
        left = [pltpu.roll(x, 127, 1) for x in c]
        w = [[] for _ in range(7)]
        for j in range(blocks):
            mid = c[j]
            xm = mid + jnp.where(lane == 0, right[j - 1] if j else 0.0, right[j])
            xp = mid + jnp.where(lane == 127, left[j + 1] if j + 1 < blocks else 0.0, left[j])
            ym = mid + (jnp.where(sub == 0, 0.0, below[j]) if i == 0 else below[j])
            yp = mid + (jnp.where(sub == 7, 0.0, above[j]) if i + 1 == tiles else above[j])
            zm, zp = mid + czm[j], mid + czp[j]
            w[0].append(1.0 - ((xm + xp) + (ym + yp) + (zm + zp)))
            w[1].append(xm if j else jnp.where(lane == 0, 0.0, xm))
            w[2].append(xp if j + 1 < blocks else jnp.where(lane == 127, 0.0, xp))
            w[3].append(jnp.where(sub == 0, 0.0, ym) if i == 0 else ym)
            w[4].append(jnp.where(sub == 7, 0.0, yp) if i + 1 == tiles else yp)
            inside = mid > 0.0
            w[5].append(jnp.where(inside, zm, 0.0))
            w[6].append(jnp.where(inside, zp, 0.0))
        for k in range(7):
            store(k, i, jnp.concatenate(w[k], axis=1))
        below, c = c, above


def step_plane(weight, load, store, rows, lanes, fields=1):
    tiles = rows // 8
    below = [pltpu.roll(load(f, 0, tiles - 1), 1, 0) for f in range(fields)]
    center = [load(f, 0, 0) for f in range(fields)]
    wrapped = [pltpu.roll(v, 7, 0) for v in center]
    for i in range(tiles):
        w = [weight(k, i) for k in range(7)]
        for f in range(fields):
            mid = center[f]
            above = load(f, 0, i + 1) if i + 1 < tiles else wrapped[f]
            xm = pltpu.roll(mid, 1, 1)
            xp = pltpu.roll(mid, lanes - 1, 1)
            out = w[0] * mid
            out = out + (w[1] * xm + w[2] * xp)
            out = out + (w[3] * below[f] + w[4] * above)
            out = out + (w[5] * load(f, -1, i) + w[6] * load(f, 1, i))
            store(f, i, out)
            below[f], center[f] = mid, above


def at_row(value, step):
    return pl.multiple_of(value * step, 8)


def window_kernel(c_hbm, c_ref, sem):
    half = lax.rem(lax.axis_index("tm"), 2)
    window = pl.ds(at_row(half, c_hbm.shape[1] - c_ref.shape[1]), c_ref.shape[1])
    copy = pltpu.make_async_copy(c_hbm.at[:, window, :], c_ref, sem)
    copy.start()
    copy.wait()


def send_kernel(iterate_hbm, send_ref, sem):
    half = lax.rem(lax.axis_index("tm"), 2)
    own = send_ref.shape[1]
    copy = pltpu.make_async_copy(iterate_hbm.at[:, pl.ds(at_row(1 - half, own), own), :], send_ref, sem)
    copy.start()
    copy.wait()


def weigh_planes(c_ref, w_refs, shift, count):
    planes, rows, lanes = c_ref.shape
    tiles = rows // 8

    def one(n, _):
        def load(dz, i):
            return c_ref[n + 1 + dz, tile(i), :]

        def store(k, i, w):
            w_refs[k][n + 1 - shift, tile(i), :] = w

        weights_plane(load, store, rows, lanes)
        return 0

    lax.fori_loop(0, count, one, 0)

    def edge(k, z, inner, at):
        for i in range(tiles):
            c = c_ref[z, tile(i), :]
            w_refs[k][at, tile(i), :] = jnp.where(c > 0.0, c + c_ref[inner, tile(i), :], 0.0)

    @pl.when(shift == 1)
    def _():
        edge(5, planes - 1, planes - 2, planes - 2)

    @pl.when(shift == 0)
    def _():
        edge(6, 0, 1, 0)


def deal_planes(raw, c_ref, start, count):
    tiles, blocks = c_ref.shape[1] // 8, raw.shape[1]

    def one(z, _):
        for j in range(blocks):
            for i in range(tiles):
                c_ref[start + z, tile(i), 128 * j : 128 * j + 128] = GAIN * raw[z, j, pl.ds(i, 8, tiles), :]
        return 0

    lax.fori_loop(0, count, one, 0)


def coarse_means(c_ref, c_start, cc_ref, cc_start, count, reach):
    tiles = c_ref.shape[1] // 8

    def one(n, _):
        for q in range(reach):
            at = n * reach + q

            def store(i, mean):
                cc_ref[cc_start + at, tile(i), :] = mean

            dealt_mean(lambda dz, i: c_ref[c_start + 2 * at + dz, tile(i), :], tiles, store)
        return 0

    lax.fori_loop(0, count // reach, one, 0)


def near_kernel(planes, flag_ref, c_hbm, partner_hbm, *refs):
    w_refs, (edge_ref, cc_ref, c_ref, raw, sem) = refs[:7], refs[7:]
    upper = flag_ref[1]
    blocks, reach = raw.shape[1], planes // 2
    copies = [
        pltpu.make_async_copy(ref.at[:, :, 128 * j : 128 * j + 128], raw.at[planes * n : planes * (n + 1), j], sem.at[n, j])
        for n, ref in enumerate((c_hbm, partner_hbm))
        for j in range(blocks)
    ]
    for copy in copies:
        copy.start()
    for copy in copies:
        copy.wait()
    deal_planes(raw.at[0:planes], c_ref, (1 - upper) * planes, planes)
    deal_planes(raw.at[planes:], c_ref, upper * planes, planes)
    weigh_planes(c_ref, w_refs, upper, 2 * planes - 2)
    coarse_means(c_ref, 0, cc_ref, 0, 2 * reach, reach)
    edge_ref[...] = c_ref[pl.ds((1 - upper) * (2 * planes - 2), 2)]


def fine_kernel(planes, flag_ref, other_hbm, iterate_hbm, initial_hbm, received_hbm, *refs):
    near_w, (edge_c, near_cc), refs = refs[:7], refs[7:9], refs[9:]
    own_ref, to_partner_ref, to_other_ref, cc_scr, c_raw, v_raw, far_c, far_w, a_scr, b_scr = refs[:10]
    coarse_ref, keep_scr, c_sem, v_sem = refs[10:]
    far_w = [far_w.at[k] for k in range(7)]
    half, upper, last = flag_ref[0], flag_ref[1], flag_ref[2]
    rows, lanes = edge_c.shape[1:]
    own_rows = rows - MARGIN
    tiles = rows // 8
    columns = [slice(128 * j, 128 * j + 128) for j in range(lanes // 128)]
    reach = planes // 2
    coarse_rows, coarse_lanes = rows // 2, lanes // 2

    c_copies = [
        pltpu.make_async_copy(other_hbm.at[:, :, column], c_raw.at[:, j], c_sem.at[j]) for j, column in enumerate(columns)
    ]
    for copy in c_copies:
        copy.start()
    into = pl.ds(at_row(half, MARGIN), own_rows)
    source = pl.ds(at_row(half, own_rows), own_rows)

    def fetch(ref, f):
        for j in range(len(columns)):
            pltpu.make_async_copy(ref[j], v_raw.at[f, :, j, into, :], v_sem.at[f, j]).start()

    def halves(ref):
        return [ref.at[:, source, column] for column in columns]

    received = [received_hbm.at[:, :, column] for column in columns]

    first_kept = (last == 0) & (half == 0)
    first_got = (last == 0) & (half == 1)
    second_kept = (last == 1) == (half == 0)
    for f, choices in enumerate(
        (
            ((last == 1, halves(initial_hbm)), (first_kept, halves(iterate_hbm)), (first_got, received)),
            ((second_kept, halves(iterate_hbm)), (jnp.logical_not(second_kept), received)),
        )
    ):
        for condition, ref in choices:
            @pl.when(condition)
            def _():
                fetch(ref, f)

    outside = pl.ds(at_row(1 - half, own_rows), MARGIN)
    v_raw[:, :, :, outside, :] = jnp.zeros(v_raw.shape[:3] + (MARGIN, 128), F32)
    idle = jnp.zeros((2,) + a_scr.shape[2:], F32)
    for number in range(STEPS):
        v_in = (a_scr, b_scr)[number % 2]
        v_in[:, planes - 1 - number] = idle
        v_in[:, 2 * planes + number] = idle
    for copy in c_copies:
        copy.wait()

    deal_planes(c_raw, far_c, (1 - upper) * 2, planes)
    far_c[pl.ds(upper * planes, 2)] = edge_c[...]
    weigh_planes(far_c, far_w, 1 - upper, planes)
    cc_scr[pl.ds(upper * reach, 2 * reach)] = near_cc[...]
    coarse_means(far_c, (1 - upper) * 2, cc_scr, (1 - upper) * (2 * reach), reach, reach)
    for q in range(reach):
        def load(dz, i):
            return cc_scr[reach + q + dz, tile(i), :]

        def store(k, i, w):
            coarse_ref[k, q, tile(i), :] = w

        weights_plane(load, store, coarse_rows, coarse_lanes)

    for f in range(2):
        for j in range(len(columns)):
            pltpu.make_async_copy(received[j], v_raw.at[f, :, j, into, :], v_sem.at[f, j]).wait()

    def deal_v(z, _):
        for f in range(2):
            for j, column in enumerate(columns):
                for i in range(tiles):
                    a_scr[f, planes + z, tile(i), column] = v_raw[f, z, j, pl.ds(i, 8, tiles), :]
        return 0

    lax.fori_loop(0, planes, deal_v, 0)

    def keep(f, _):
        for q in range(reach):
            def store(i, mean):
                keep_scr[f * reach + q, tile(i), :] = mean

            dealt_mean(lambda dz, i: a_scr[f, planes + 2 * q + dz, tile(i), :], tiles, store)
        return 0

    lax.fori_loop(0, 2, keep, 0)
    near_at, far_at = upper * (planes + 1), (1 - upper) * (2 * planes - 1)
    for number in range(STEPS):
        v_in, v_out = (a_scr, b_scr) if number % 2 == 0 else (b_scr, a_scr)
        low, high = planes - number, 2 * planes + number

        def advance_all(w_refs, w_at, start, count):
            def advance(n, _):
                z = start + n

                def load(f, dz, i):
                    return v_in[f, z + dz, tile(i), :]

                def weight(k, i):
                    return w_refs[k][z - w_at, tile(i), :]

                def store(f, i, v):
                    v_out[f, z, tile(i), :] = v

                step_plane(weight, load, store, rows, lanes, 2)
                return 0

            lax.fori_loop(0, count, advance, 0)

        advance_all(near_w, near_at, jnp.where(upper == 1, planes + 1, low), planes - 1 + number)
        advance_all(far_w, far_at, jnp.where(upper == 1, low, 2 * planes - 1), 1 + number)

        def reach_out(w_ref, w_at, z, inner):
            for i in range(tiles):
                w = w_ref[z - w_at, tile(i), :]
                for f in range(2):
                    v_out[f, z, tile(i), :] = w * v_in[f, inner, tile(i), :]

        @pl.when(upper == 1)
        def _():
            reach_out(far_w[6], 0, low - 1, low)
            reach_out(near_w[5], planes + 1, high, high - 1)

        @pl.when(upper == 0)
        def _():
            reach_out(near_w[6], 0, low - 1, low)
            reach_out(far_w[5], 2 * planes - 1, high, high - 1)

    result = a_scr if STEPS % 2 == 0 else b_scr

    scale = jnp.where(last == 1, 0.0, 1.0).astype(F32)
    for q in range(reach):
        keep_scr[q] = keep_scr[q] * scale
    zero = jnp.zeros((8, coarse_lanes), F32)
    for q in range(reach):
        def load(f, dz, i):
            at = q + dz
            return zero if at < 0 or at >= reach else keep_scr[f * reach + at, tile(i), :]

        def weight(k, i):
            return coarse_ref[k, q, tile(i), :]

        def store(f, i, v):
            own_ref[f, q, tile(i), :] = v

        step_plane(weight, load, store, coarse_rows, coarse_lanes, 2)

    def finish(f, q, put):
        dealt_mean(lambda dz, i: result[f, 2 * q + dz, tile(i), :], tiles, put)

    low_c, high_c = cc_scr[reach - 1], cc_scr[2 * reach]
    coarse_ref[0, 0] = jnp.where(low_c > 0.0, low_c + cc_scr[reach], 0.0)
    coarse_ref[0, 1] = jnp.where(high_c > 0.0, high_c + cc_scr[2 * reach - 1], 0.0)

    def own_planes(f, _):
        for q in range(reach):
            def put(i, mean):
                own_ref[f, q, tile(i), :] = mean - own_ref[f, q, tile(i), :]

            finish(f, reach + q, put)
        return 0

    lax.fori_loop(0, 2, own_planes, 0)

    def far_planes(into_ref, side, base, edge, kept):
        def one(f, _):
            for q in range(reach):
                def put(i, mean):
                    into_ref[f, q, tile(i), :] = mean

                finish(f, base + q, put)
            return 0

        lax.fori_loop(0, 2, one, 0)
        for f in range(2):
            into_ref[f, edge] = into_ref[f, edge] - coarse_ref[0, side] * keep_scr[f * reach + kept]

    @pl.when(upper == 1)
    def _():
        far_planes(to_partner_ref, 1, 2 * reach, 0, reach - 1)
        far_planes(to_other_ref, 0, 0, reach - 1, 0)

    @pl.when(upper == 0)
    def _():
        far_planes(to_partner_ref, 0, 0, reach - 1, 0)
        far_planes(to_other_ref, 1, 2 * reach, 0, reach - 1)


def weight_kernel(cc_ref, weight_ref):
    planes, rows, lanes = cc_ref.shape
    for q in range(planes - 2):
        def load(dz, i):
            return cc_ref[q + 1 + dz, tile(i), :]

        def store(k, i, w):
            weight_ref[k, q, tile(i), :] = w

        weights_plane(load, store, rows, lanes)


def sum_kernel(flag_ref, own_ref, partner_ref, other_ref, val_ref, extra_ref, to_partner_ref, to_other_ref):
    upper = flag_ref[1]
    planes = val_ref.shape[0]
    val = own_ref[0] + partner_ref[0] + other_ref[0]
    extra = own_ref[1] + partner_ref[1] + other_ref[1]
    val_ref[...] = val
    extra_ref[...] = extra
    to_partner_ref[0:planes] = val
    to_other_ref[0:planes] = val
    to_partner_ref[planes] = jnp.where(upper == 1, extra[-1], extra[0])
    to_other_ref[planes] = jnp.where(upper == 1, extra[0], extra[-1])


def coarse_advance(weight_ref, offset, source, into, count, extra, add, rows, lanes):
    for q in range(count):
        def load(f, dz, i):
            return source[q + 1 + dz, tile(i), :]

        def weight(k, i):
            return weight_ref[k, offset + q, tile(i), :]

        def store(f, i, v):
            into[q, tile(i), :] = v + add * extra[q, tile(i), :]

        step_plane(weight, load, store, rows, lanes)


def pick(flag_ref, slots, sources, sends):
    for slot, ref in zip(slots, sends):
        which = flag_ref[slot]

        @pl.when(which < 0)
        def _():
            ref[...] = jnp.zeros(ref.shape, F32)

        for m, source in enumerate(sources):
            @pl.when(which == m)
            def _():
                ref[...] = source[...]


def chain_kernel(slots, send_slots, count, edges, flag_ref, weight_ref, partner_ref, other_ref, extra_ref, *refs):
    upper = flag_ref[1]
    refs = list(refs)
    values = refs[:count]
    outs = len(slots) if edges else len(slots) - 1
    made = refs[count : count + outs]
    rest = refs[count + outs :]
    to_sides, rest = rest[: 2 * edges], rest[2 * edges :]
    sends, (wide, extra_wide, middle, final_scr) = rest[: len(send_slots)], rest[len(send_slots) :]
    val_ref = values[-1]
    planes, rows, lanes = val_ref.shape
    if not edges:
        made = [*made, final_scr]
    add = [flag_ref[slot].astype(F32) for slot in slots]
    wide[planes : 2 * planes] = val_ref[...]
    sides = ((partner_ref, upper), (other_ref, 1 - upper))
    if len(slots) == 2:
        extra_wide[1 : planes + 1] = extra_ref[...]
        for ref, above in sides:
            wide[pl.ds(above * (2 * planes), planes)] = ref[0:planes]
            extra_wide[above * (planes + 1)] = ref[planes]
        coarse_advance(weight_ref, 0, wide.at[planes - 2 :], middle, planes + 2, extra_wide, add[0], rows, lanes)
        made[0][...] = middle[1 : planes + 1]
        coarse_advance(weight_ref, 1, middle, made[1], planes, extra_ref, add[1], rows, lanes)
    else:
        for ref, above in sides:
            wide[planes - 1 + above * (planes + 1)] = ref[0]
        coarse_advance(weight_ref, 1, wide.at[planes - 1 :], made[0], planes, extra_ref, add[0], rows, lanes)
    if edges:
        low, high = made[-1][0], made[-1][planes - 1]
        to_sides[0][0] = jnp.where(upper == 1, high, low)
        to_sides[1][0] = jnp.where(upper == 1, low, high)
    pick(flag_ref, send_slots, values + made, sends)


def base_kernel(iterate_ref, out_ref, rows_scr, fine_scr):
    planes, rows, lanes = iterate_ref.shape
    select, spread = pairing(lanes), spreading(lanes)
    for q in range(planes // 2):
        mean = natural_mean(iterate_ref[2 * q], iterate_ref[2 * q + 1], rows_scr, select)
        wide = split_dot(mean, spread)
        for j in range(lanes // 128):
            column = slice(128 * j, 128 * j + 128)
            fine_scr[j, pl.ds(0, rows // 2, 2), :] = wide[:, column]
            fine_scr[j, pl.ds(1, rows // 2, 2), :] = wide[:, column]
            for part in range(2):
                out_ref[2 * q + part, :, column] = iterate_ref[2 * q + part, :, column] - fine_scr[j]


def final_kernel(slots, flag_ref, base_ref, *refs):
    count = len(slots)
    pieces, out_ref, fine_scr, sum_scr, error_scr = refs[:count], *refs[count:]
    planes, rows, lanes = base_ref.shape
    spread = spreading(lanes)
    piece_rows = pieces[0].shape[1]
    tiles = piece_rows // 8
    sum_scr[...] = jnp.zeros(sum_scr.shape, F32)
    for slot, ref in zip(slots, pieces):
        side = flag_ref[slot]
        sum_scr[side] = sum_scr[side] + ref[...]
    for q in range(planes // 2):
        for j in range(lanes // 256):
            column = slice(128 * j, 128 * j + 128)
            error_scr[j] = jnp.zeros(error_scr.shape[1:], F32)
            for side in range(2):
                first = side * (rows // 2 - piece_rows)
                for i in range(tiles):
                    at = pl.ds(first + i, 8, tiles)
                    error_scr[j, at, :] = error_scr[j, at, :] + sum_scr[side, q, tile(i), column]
        error = jnp.concatenate([error_scr[j] for j in range(lanes // 256)], axis=1)
        wide = split_dot(error, spread)
        for j in range(lanes // 128):
            column = slice(128 * j, 128 * j + 128)
            fine_scr[j, pl.ds(0, rows // 2, 2), :] = wide[:, column]
            fine_scr[j, pl.ds(1, rows // 2, 2), :] = wide[:, column]
            for part in range(2):
                out_ref[2 * q + part, :, column] = base_ref[2 * q + part, :, column] + fine_scr[j]


def swap_pairs(count, first):
    pairs = []
    for i in range(first, count - 1, 2):
        pairs += [(i, i + 1), (i + 1, i)]
    return pairs


def roles(layers):
    last_group = layers // 2 - 1
    rows = []
    for t in range(layers):
        half, last = t % 2, int(t // 2 == last_group)
        adds = [int(number == (layers - 1 if last else 1)) for number in range(1, layers)]
        sends = []
        for shift in range(layers):
            k = (t + shift) % layers
            m = k if last else k - 1 - (t - half)
            sends.append(m if m >= 0 else -1)
        halves = [(t - shift) % layers % 2 for shift in range(layers)]
        rows.append([half, last, *adds, *sends, *halves])
    return rows


def local(initial, iterate, diffusivity):
    layers, slabs = lax.axis_size("tm"), lax.axis_size("space")
    t, s = lax.axis_index("tm"), lax.axis_index("space")
    planes, all_rows, lanes = initial.shape
    assert layers % 2 == 0 and slabs % 2 == 0 and planes == STEPS
    own_rows = all_rows // 2
    rows = own_rows + MARGIN
    coarse_rows, coarse_lanes = rows // 2, lanes // 2
    reach = planes // 2
    upper = 1 - s % 2
    field = iterate[0]

    def partner_swap(x):
        return lax.ppermute(x, "space", swap_pairs(slabs, 0))

    def other_swap(x):
        return lax.ppermute(x, "space", swap_pairs(slabs, 1))

    anywhere = pl.BlockSpec(memory_space=pl.ANY)
    in_hbm = pl.BlockSpec(memory_space=pltpu.HBM)

    def cut(kernel, count, source):
        return pl.pallas_call(
            kernel,
            out_shape=shape(planes, count, lanes),
            in_specs=[in_hbm],
            out_specs=pl.BlockSpec(memory_space=VMEM),
            scratch_shapes=[pltpu.SemaphoreType.DMA],
            compiler_params=params(VMEM_LIMITS["slices"]),
        )(source)

    c = cut(window_kernel, rows, diffusivity)
    to_row_partner = cut(send_kernel, own_rows, field)
    row_pairs = swap_pairs(layers, 0)
    row_pairs.remove((layers - 1, layers - 2))
    received = lax.ppermute(to_row_partner, "tm", row_pairs)
    c_other = other_swap(c)
    c_partner = partner_swap(c)

    table = roles(layers)
    mine = jnp.asarray(table, jnp.int32)[t]
    flags = jnp.concatenate([mine[:1], jnp.reshape(upper, (1,)).astype(jnp.int32), mine[1:]])
    add_at, send_at, half_at = 3, 2 + layers, 2 + 2 * layers
    smem = pl.BlockSpec(memory_space=pltpu.SMEM)

    def cost(microseconds):
        return pl.CostEstimate(flops=int(microseconds * 4e6), bytes_accessed=0, transcendentals=0)

    fields = shape(2, reach, coarse_rows, coarse_lanes)
    blocks = lanes // 128
    prepared = pl.pallas_call(
        functools.partial(near_kernel, planes),
        out_shape=(
            *[shape(2 * planes - 1, rows, lanes)] * 7,
            shape(2, rows, lanes),
            shape(2 * reach, coarse_rows, coarse_lanes),
        ),
        in_specs=[smem] + [anywhere] * 2,
        out_specs=tuple(whole(9)),
        scratch_shapes=[
            VMEM((2 * planes, rows, lanes), F32),
            VMEM((2 * planes, blocks, rows, 128), F32),
            pltpu.SemaphoreType.DMA((2, blocks)),
        ],
        compiler_params=params(VMEM_LIMITS["near"]),
        cost_estimate=cost(6),
        name="near",
    )(flags, c, c_partner)
    own, to_partner, to_other, cc = pl.pallas_call(
        functools.partial(fine_kernel, planes),
        out_shape=(fields, fields, fields, shape(3 * reach, coarse_rows, coarse_lanes)),
        in_specs=[smem] + [anywhere] + [in_hbm] * 2 + [anywhere] + whole(9),
        out_specs=tuple(whole(4)),
        scratch_shapes=[
            VMEM((planes, blocks, rows, 128), F32),
            VMEM((2, planes, blocks, rows, 128), F32),
            VMEM((planes + 2, rows, lanes), F32),
            VMEM((7, planes + 1, rows, lanes), F32),
            VMEM((2, 3 * planes, rows, lanes), F32),
            VMEM((2, 3 * planes, rows, lanes), F32),
            VMEM((7, reach, coarse_rows, coarse_lanes), F32),
            VMEM((2 * reach, coarse_rows, coarse_lanes), F32),
            pltpu.SemaphoreType.DMA((blocks,)),
            pltpu.SemaphoreType.DMA((2, blocks)),
        ],
        compiler_params=params(VMEM_LIMITS["fine"]),
        name="fine",
    )(flags, c_other, field, initial, received, *prepared)

    base = pl.pallas_call(
        base_kernel,
        out_shape=shape(planes, all_rows, lanes),
        in_specs=whole(1),
        out_specs=pl.BlockSpec(memory_space=VMEM),
        scratch_shapes=[VMEM((coarse_lanes // 128, all_rows, 128), F32), VMEM((lanes // 128, all_rows, 128), F32)],
        compiler_params=params(VMEM_LIMITS["final"]),
        cost_estimate=cost(4),
        name="base",
    )(field)

    from_other = other_swap(to_other)
    from_partner = partner_swap(to_partner)
    plane = shape(1, coarse_rows, coarse_lanes)
    block = shape(reach, coarse_rows, coarse_lanes)
    thick = shape(reach + 1, coarse_rows, coarse_lanes)
    weights = pl.pallas_call(
        weight_kernel,
        out_shape=shape(7, 3 * reach - 2, coarse_rows, coarse_lanes),
        in_specs=whole(1),
        out_specs=pl.BlockSpec(memory_space=VMEM),
        compiler_params=params(VMEM_LIMITS["small"]),
        cost_estimate=cost(2),
        name="weights",
    )(cc)
    val, extra, to_partner, to_other = pl.pallas_call(
        sum_kernel,
        out_shape=(block, block, thick, thick),
        in_specs=[smem] + whole(3),
        out_specs=tuple(whole(4)),
        compiler_params=params(VMEM_LIMITS["small"]),
        name="gather",
    )(flags, own, from_partner, from_other)

    ready = [max(row[1 + layers + shift] for row in table) for shift in range(layers)]
    arrived = [None] * layers
    values = [val]
    sent = []
    while len(values) < layers:
        from_other = other_swap(to_other)
        from_partner = partner_swap(to_partner)
        for shift, send in sent:
            pairs = [
                (source, (source + shift) % layers)
                for source in range(layers)
                if table[source][1 + layers + shift] >= 0
            ]
            arrived[shift] = lax.ppermute(send, "tm", pairs) if shift else send
        count = len(values)
        steps = 2 if count == 1 and layers > 2 else 1
        more = count + steps < layers
        kept = steps if more else steps - 1
        slots = [add_at + count - 1 + n for n in range(steps)]
        shifts = [shift for shift in range(layers) if arrived[shift] is None and ready[shift] < count + steps]
        made = pl.pallas_call(
            functools.partial(chain_kernel, slots, [send_at + shift for shift in shifts], count, int(more)),
            out_shape=(*[block] * kept, *[plane] * (2 * more), *[block] * len(shifts)),
            in_specs=[smem] + whole(4 + count),
            out_specs=tuple(whole(kept + 2 * more + len(shifts))),
            scratch_shapes=[
                VMEM((3 * reach, coarse_rows, coarse_lanes), F32),
                VMEM((reach + 2, coarse_rows, coarse_lanes), F32),
                VMEM((reach + 2, coarse_rows, coarse_lanes), F32),
                VMEM((reach, coarse_rows, coarse_lanes), F32),
            ],
            compiler_params=params(VMEM_LIMITS["small"]),
        )(flags, weights, from_partner, from_other, extra, *values)
        values += made[:kept] if more else [None] * steps
        if more:
            to_partner, to_other = made[kept : kept + 2]
        sent = list(zip(shifts, made[kept + 2 * more :]))
    for shift, send in sent:
        pairs = [
            (source, (source + shift) % layers) for source in range(layers) if table[source][1 + layers + shift] >= 0
        ]
        arrived[shift] = lax.ppermute(send, "tm", pairs) if shift else send

    corrected = pl.pallas_call(
        functools.partial(final_kernel, [half_at + shift for shift in range(layers)]),
        out_shape=shape(planes, all_rows, lanes),
        in_specs=[smem] + whole(1 + layers),
        out_specs=pl.BlockSpec(memory_space=VMEM),
        scratch_shapes=[
            VMEM((lanes // 128, all_rows, 128), F32),
            VMEM((2, reach, coarse_rows, coarse_lanes), F32),
            VMEM((coarse_lanes // 128, all_rows // 2, 128), F32),
        ],
        compiler_params=params(VMEM_LIMITS["final"]),
        name="final",
    )(flags, base, *arrived)
    return corrected[None]


def solution(mesh):
    placed = (P("space", None, None), P("tm", "space", None, None), P("space", None, None))

    return jax.shard_map(local, mesh=mesh, in_specs=placed, out_specs=P("tm", "space", None, None), check_vma=False)
```

```python
import functools

import jax
import jax.numpy as jnp
from jax import lax
from jax.experimental import pallas as pl
from jax.experimental.pallas import tpu as pltpu
from jax.sharding import PartitionSpec as P


STEPS = 4
courant = 0.15
GAIN = 0.5 * courant
MARGIN = 16
F32 = jnp.float32
VMEM = pltpu.VMEM
MIB = 1024 * 1024
VMEM_LIMITS = {"slices": 50 * MIB, "near": 6 * MIB, "fine": 34 * MIB, "small": 10 * MIB, "final": 16 * MIB}


def params(limit):
    return pltpu.CompilerParams(vmem_limit_bytes=limit)


def whole(count):
    return [pl.BlockSpec(memory_space=VMEM)] * count


def shape(*dims):
    return jax.ShapeDtypeStruct(dims, F32)


def split_dot(x, selection):
    high = x.astype(jnp.bfloat16)
    rest = x - high.astype(F32)
    middle = rest.astype(jnp.bfloat16)
    low = (rest - middle.astype(F32)).astype(jnp.bfloat16)
    dot = functools.partial(jnp.dot, preferred_element_type=F32)
    return dot(high, selection) + dot(middle, selection) + dot(low, selection)


def pairing(width):
    fine = lax.broadcasted_iota(jnp.int32, (width, width // 2), 0)
    coarse = lax.broadcasted_iota(jnp.int32, (width, width // 2), 1)
    return jnp.where((fine == 2 * coarse) | (fine == 2 * coarse + 1), 1.0, 0.0).astype(jnp.bfloat16)


def spreading(width):
    coarse = lax.broadcasted_iota(jnp.int32, (width // 2, width), 0)
    fine = lax.broadcasted_iota(jnp.int32, (width // 2, width), 1)
    return jnp.where((fine == 2 * coarse) | (fine == 2 * coarse + 1), 1.0, 0.0).astype(jnp.bfloat16)


def natural_mean(first, second, rows_scr, select):
    rows = first.shape[0]
    lanes = split_dot(first + second, select)
    parts = []
    for j in range(lanes.shape[1] // 128):
        rows_scr[j, 0:rows, :] = lanes[:, 128 * j : 128 * j + 128]
        even = rows_scr[j, pl.ds(0, rows // 2, 2), :]
        odd = rows_scr[j, pl.ds(1, rows // 2, 2), :]
        parts.append(0.125 * (even + odd))
    return jnp.concatenate(parts, axis=1)


def tile(i):
    return slice(8 * i, 8 * i + 8)


def pair_lanes(blocks):
    lane = lax.broadcasted_iota(jnp.int32, (8, 128), 1)
    place = 2 * (lane % 64)
    out = []
    for first, second in zip(blocks[::2], blocks[1::2]):
        halves = [
            jnp.take_along_axis(x + pltpu.roll(x, 127, 1), place, axis=1, mode="promise_in_bounds") for x in (first, second)
        ]
        out.append(jnp.where(lane < 64, *halves))
    return out


def dealt_mean(load, tiles, store):
    for i in range(tiles // 2):
        total = (load(0, 2 * i) + load(1, 2 * i)) + (load(0, 2 * i + 1) + load(1, 2 * i + 1))
        blocks = [total[:, 128 * j : 128 * j + 128] for j in range(total.shape[1] // 128)]
        store(i, 0.125 * jnp.concatenate(pair_lanes(blocks), axis=1))


def weights_plane(load, store, rows, lanes):
    sub = lax.broadcasted_iota(jnp.int32, (8, 128), 0)
    lane = lax.broadcasted_iota(jnp.int32, (8, 128), 1)
    tiles, blocks = rows // 8, lanes // 128

    def cut(x):
        return [x[:, 128 * j : 128 * j + 128] for j in range(blocks)]

    c = cut(load(0, 0))
    below = [pltpu.roll(x, 1, 0) for x in cut(load(0, tiles - 1))]
    wrapped = [pltpu.roll(x, 7, 0) for x in c]
    for i in range(tiles):
        above = cut(load(0, i + 1)) if i + 1 < tiles else wrapped
        czm, czp = cut(load(-1, i)), cut(load(1, i))
        right = [pltpu.roll(x, 1, 1) for x in c]
        left = [pltpu.roll(x, 127, 1) for x in c]
        w = [[] for _ in range(7)]
        for j in range(blocks):
            mid = c[j]
            xm = mid + jnp.where(lane == 0, right[j - 1] if j else 0.0, right[j])
            xp = mid + jnp.where(lane == 127, left[j + 1] if j + 1 < blocks else 0.0, left[j])
            ym = mid + (jnp.where(sub == 0, 0.0, below[j]) if i == 0 else below[j])
            yp = mid + (jnp.where(sub == 7, 0.0, above[j]) if i + 1 == tiles else above[j])
            zm, zp = mid + czm[j], mid + czp[j]
            w[0].append(1.0 - ((xm + xp) + (ym + yp) + (zm + zp)))
            w[1].append(xm if j else jnp.where(lane == 0, 0.0, xm))
            w[2].append(xp if j + 1 < blocks else jnp.where(lane == 127, 0.0, xp))
            w[3].append(jnp.where(sub == 0, 0.0, ym) if i == 0 else ym)
            w[4].append(jnp.where(sub == 7, 0.0, yp) if i + 1 == tiles else yp)
            inside = mid > 0.0
            w[5].append(jnp.where(inside, zm, 0.0))
            w[6].append(jnp.where(inside, zp, 0.0))
        for k in range(7):
            store(k, i, jnp.concatenate(w[k], axis=1))
        below, c = c, above


def step_plane(weight, load, store, rows, lanes, fields=1):
    tiles = rows // 8
    below = [pltpu.roll(load(f, 0, tiles - 1), 1, 0) for f in range(fields)]
    center = [load(f, 0, 0) for f in range(fields)]
    wrapped = [pltpu.roll(v, 7, 0) for v in center]
    for i in range(tiles):
        w = [weight(k, i) for k in range(7)]
        for f in range(fields):
            mid = center[f]
            above = load(f, 0, i + 1) if i + 1 < tiles else wrapped[f]
            xm = pltpu.roll(mid, 1, 1)
            xp = pltpu.roll(mid, lanes - 1, 1)
            out = w[0] * mid
            out = out + (w[1] * xm + w[2] * xp)
            out = out + (w[3] * below[f] + w[4] * above)
            out = out + (w[5] * load(f, -1, i) + w[6] * load(f, 1, i))
            store(f, i, out)
            below[f], center[f] = mid, above


def at_row(value, step):
    return pl.multiple_of(value * step, 8)


def slice_kernel(c_hbm, iterate_hbm, c_ref, send_ref, sem):
    half = lax.rem(lax.axis_index("tm"), 2)
    own = send_ref.shape[1]
    window = pl.ds(at_row(half, c_hbm.shape[1] - c_ref.shape[1]), c_ref.shape[1])
    send = pltpu.make_async_copy(iterate_hbm.at[:, pl.ds(at_row(1 - half, own), own), :], send_ref, sem.at[0])
    keep = pltpu.make_async_copy(c_hbm.at[:, window, :], c_ref, sem.at[1])
    send.start()
    keep.start()
    send.wait()
    keep.wait()


def weigh_planes(c_ref, w_refs, shift, count):
    planes, rows, lanes = c_ref.shape
    tiles = rows // 8

    def one(n, _):
        def load(dz, i):
            return c_ref[n + 1 + dz, tile(i), :]

        def store(k, i, w):
            w_refs[k][n + 1 - shift, tile(i), :] = w

        weights_plane(load, store, rows, lanes)
        return 0

    lax.fori_loop(0, count, one, 0)

    def edge(k, z, inner, at):
        for i in range(tiles):
            c = c_ref[z, tile(i), :]
            w_refs[k][at, tile(i), :] = jnp.where(c > 0.0, c + c_ref[inner, tile(i), :], 0.0)

    @pl.when(shift == 1)
    def _():
        edge(5, planes - 1, planes - 2, planes - 2)

    @pl.when(shift == 0)
    def _():
        edge(6, 0, 1, 0)


def deal_planes(raw, c_ref, start, count):
    tiles, blocks = c_ref.shape[1] // 8, raw.shape[1]

    def one(z, _):
        for j in range(blocks):
            for i in range(tiles):
                c_ref[start + z, tile(i), 128 * j : 128 * j + 128] = GAIN * raw[z, j, pl.ds(i, 8, tiles), :]
        return 0

    lax.fori_loop(0, count, one, 0)


def coarse_means(c_ref, c_start, cc_ref, cc_start, count, reach):
    tiles = c_ref.shape[1] // 8

    def one(n, _):
        for q in range(reach):
            at = n * reach + q

            def store(i, mean):
                cc_ref[cc_start + at, tile(i), :] = mean

            dealt_mean(lambda dz, i: c_ref[c_start + 2 * at + dz, tile(i), :], tiles, store)
        return 0

    lax.fori_loop(0, count // reach, one, 0)


def near_kernel(planes, flag_ref, c_hbm, partner_hbm, *refs):
    w_refs, (edge_ref, cc_ref, c_ref, raw, sem) = refs[:7], refs[7:]
    upper = flag_ref[1]
    blocks, reach = raw.shape[1], planes // 2
    copies = [
        pltpu.make_async_copy(ref.at[:, :, 128 * j : 128 * j + 128], raw.at[planes * n : planes * (n + 1), j], sem.at[n, j])
        for n, ref in enumerate((c_hbm, partner_hbm))
        for j in range(blocks)
    ]
    for copy in copies:
        copy.start()
    for copy in copies:
        copy.wait()
    deal_planes(raw.at[0:planes], c_ref, (1 - upper) * planes, planes)
    deal_planes(raw.at[planes:], c_ref, upper * planes, planes)
    weigh_planes(c_ref, w_refs, upper, 2 * planes - 2)
    coarse_means(c_ref, 0, cc_ref, 0, 2 * reach, reach)
    edge_ref[...] = c_ref[pl.ds((1 - upper) * (2 * planes - 2), 2)]


def fine_kernel(planes, flag_ref, other_hbm, iterate_hbm, initial_hbm, received_hbm, *refs):
    near_w, (edge_c, near_cc), refs = refs[:7], refs[7:9], refs[9:]
    own_ref, to_partner_ref, to_other_ref, cc_scr, c_raw, v_raw, far_c, far_w, a_scr, b_scr = refs[:10]
    coarse_ref, keep_scr, c_sem, v_sem = refs[10:]
    far_w = [far_w.at[k] for k in range(7)]
    half, upper, last = flag_ref[0], flag_ref[1], flag_ref[2]
    rows, lanes = edge_c.shape[1:]
    own_rows = rows - MARGIN
    tiles = rows // 8
    columns = [slice(128 * j, 128 * j + 128) for j in range(lanes // 128)]
    reach = planes // 2
    coarse_rows, coarse_lanes = rows // 2, lanes // 2

    c_copies = [
        pltpu.make_async_copy(other_hbm.at[:, :, column], c_raw.at[:, j], c_sem.at[j]) for j, column in enumerate(columns)
    ]
    for copy in c_copies:
        copy.start()
    into = pl.ds(at_row(half, MARGIN), own_rows)
    source = pl.ds(at_row(half, own_rows), own_rows)

    def fetch(ref, f):
        for j in range(len(columns)):
            pltpu.make_async_copy(ref[j], v_raw.at[f, :, j, into, :], v_sem.at[f, j]).start()

    def halves(ref):
        return [ref.at[:, source, column] for column in columns]

    received = [received_hbm.at[:, :, column] for column in columns]

    first_kept = (last == 0) & (half == 0)
    first_got = (last == 0) & (half == 1)
    second_kept = (last == 1) == (half == 0)
    for f, choices in enumerate(
        (
            ((last == 1, halves(initial_hbm)), (first_kept, halves(iterate_hbm)), (first_got, received)),
            ((second_kept, halves(iterate_hbm)), (jnp.logical_not(second_kept), received)),
        )
    ):
        for condition, ref in choices:
            @pl.when(condition)
            def _():
                fetch(ref, f)

    outside = pl.ds(at_row(1 - half, own_rows), MARGIN)
    v_raw[:, :, :, outside, :] = jnp.zeros(v_raw.shape[:3] + (MARGIN, 128), F32)
    idle = jnp.zeros((2,) + a_scr.shape[2:], F32)
    for number in range(STEPS):
        v_in = (a_scr, b_scr)[number % 2]
        v_in[:, planes - 1 - number] = idle
        v_in[:, 2 * planes + number] = idle
    for copy in c_copies:
        copy.wait()

    deal_planes(c_raw, far_c, (1 - upper) * 2, planes)
    far_c[pl.ds(upper * planes, 2)] = edge_c[...]
    weigh_planes(far_c, far_w, 1 - upper, planes)
    cc_scr[pl.ds(upper * reach, 2 * reach)] = near_cc[...]
    coarse_means(far_c, (1 - upper) * 2, cc_scr, (1 - upper) * (2 * reach), reach, reach)
    for q in range(reach):
        def load(dz, i):
            return cc_scr[reach + q + dz, tile(i), :]

        def store(k, i, w):
            coarse_ref[k, q, tile(i), :] = w

        weights_plane(load, store, coarse_rows, coarse_lanes)

    for f in range(2):
        for j in range(len(columns)):
            pltpu.make_async_copy(received[j], v_raw.at[f, :, j, into, :], v_sem.at[f, j]).wait()

    def deal_v(z, _):
        for f in range(2):
            for j, column in enumerate(columns):
                for i in range(tiles):
                    a_scr[f, planes + z, tile(i), column] = v_raw[f, z, j, pl.ds(i, 8, tiles), :]
        return 0

    lax.fori_loop(0, planes, deal_v, 0)

    def keep(f, _):
        for q in range(reach):
            def store(i, mean):
                keep_scr[f * reach + q, tile(i), :] = mean

            dealt_mean(lambda dz, i: a_scr[f, planes + 2 * q + dz, tile(i), :], tiles, store)
        return 0

    lax.fori_loop(0, 2, keep, 0)
    near_at, far_at = upper * (planes + 1), (1 - upper) * (2 * planes - 1)
    for number in range(STEPS):
        v_in, v_out = (a_scr, b_scr) if number % 2 == 0 else (b_scr, a_scr)
        low, high = planes - number, 2 * planes + number

        def advance_all(w_refs, w_at, start, count):
            def advance(n, _):
                z = start + n

                def load(f, dz, i):
                    return v_in[f, z + dz, tile(i), :]

                def weight(k, i):
                    return w_refs[k][z - w_at, tile(i), :]

                def store(f, i, v):
                    v_out[f, z, tile(i), :] = v

                step_plane(weight, load, store, rows, lanes, 2)
                return 0

            lax.fori_loop(0, count, advance, 0)

        advance_all(near_w, near_at, jnp.where(upper == 1, planes + 1, low), planes - 1 + number)
        advance_all(far_w, far_at, jnp.where(upper == 1, low, 2 * planes - 1), 1 + number)

        def reach_out(w_ref, w_at, z, inner):
            for i in range(tiles):
                w = w_ref[z - w_at, tile(i), :]
                for f in range(2):
                    v_out[f, z, tile(i), :] = w * v_in[f, inner, tile(i), :]

        @pl.when(upper == 1)
        def _():
            reach_out(far_w[6], 0, low - 1, low)
            reach_out(near_w[5], planes + 1, high, high - 1)

        @pl.when(upper == 0)
        def _():
            reach_out(near_w[6], 0, low - 1, low)
            reach_out(far_w[5], 2 * planes - 1, high, high - 1)

    result = a_scr if STEPS % 2 == 0 else b_scr

    scale = jnp.where(last == 1, 0.0, 1.0).astype(F32)
    for q in range(reach):
        keep_scr[q] = keep_scr[q] * scale
    zero = jnp.zeros((8, coarse_lanes), F32)
    for q in range(reach):
        def load(f, dz, i):
            at = q + dz
            return zero if at < 0 or at >= reach else keep_scr[f * reach + at, tile(i), :]

        def weight(k, i):
            return coarse_ref[k, q, tile(i), :]

        def store(f, i, v):
            own_ref[f, q, tile(i), :] = v

        step_plane(weight, load, store, coarse_rows, coarse_lanes, 2)

    def finish(f, q, put):
        dealt_mean(lambda dz, i: result[f, 2 * q + dz, tile(i), :], tiles, put)

    low_c, high_c = cc_scr[reach - 1], cc_scr[2 * reach]
    coarse_ref[0, 0] = jnp.where(low_c > 0.0, low_c + cc_scr[reach], 0.0)
    coarse_ref[0, 1] = jnp.where(high_c > 0.0, high_c + cc_scr[2 * reach - 1], 0.0)

    def own_planes(f, _):
        for q in range(reach):
            def put(i, mean):
                own_ref[f, q, tile(i), :] = mean - own_ref[f, q, tile(i), :]

            finish(f, reach + q, put)
        return 0

    lax.fori_loop(0, 2, own_planes, 0)

    def far_planes(into_ref, side, base, edge, kept):
        def one(f, _):
            for q in range(reach):
                def put(i, mean):
                    into_ref[f, q, tile(i), :] = mean

                finish(f, base + q, put)
            return 0

        lax.fori_loop(0, 2, one, 0)
        for f in range(2):
            into_ref[f, edge] = into_ref[f, edge] - coarse_ref[0, side] * keep_scr[f * reach + kept]

    @pl.when(upper == 1)
    def _():
        far_planes(to_partner_ref, 1, 2 * reach, 0, reach - 1)
        far_planes(to_other_ref, 0, 0, reach - 1, 0)

    @pl.when(upper == 0)
    def _():
        far_planes(to_partner_ref, 0, 0, reach - 1, 0)
        far_planes(to_other_ref, 1, 2 * reach, 0, reach - 1)


def weight_kernel(cc_ref, weight_ref):
    planes, rows, lanes = cc_ref.shape
    for q in range(planes - 2):
        def load(dz, i):
            return cc_ref[q + 1 + dz, tile(i), :]

        def store(k, i, w):
            weight_ref[k, q, tile(i), :] = w

        weights_plane(load, store, rows, lanes)


def sum_kernel(flag_ref, own_ref, partner_ref, other_ref, val_ref, extra_ref, to_partner_ref, to_other_ref):
    upper = flag_ref[1]
    planes = val_ref.shape[0]
    val = own_ref[0] + partner_ref[0] + other_ref[0]
    extra = own_ref[1] + partner_ref[1] + other_ref[1]
    val_ref[...] = val
    extra_ref[...] = extra
    to_partner_ref[0:planes] = val
    to_other_ref[0:planes] = val
    to_partner_ref[planes] = jnp.where(upper == 1, extra[-1], extra[0])
    to_other_ref[planes] = jnp.where(upper == 1, extra[0], extra[-1])


def coarse_advance(weight_ref, offset, source, into, count, extra, add, rows, lanes):
    for q in range(count):
        def load(f, dz, i):
            return source[q + 1 + dz, tile(i), :]

        def weight(k, i):
            return weight_ref[k, offset + q, tile(i), :]

        def store(f, i, v):
            into[q, tile(i), :] = v + add * extra[q, tile(i), :]

        step_plane(weight, load, store, rows, lanes)


def pick(flag_ref, slots, sources, sends):
    for slot, ref in zip(slots, sends):
        which = flag_ref[slot]

        @pl.when(which < 0)
        def _():
            ref[...] = jnp.zeros(ref.shape, F32)

        for m, source in enumerate(sources):
            @pl.when(which == m)
            def _():
                ref[...] = source[...]


def chain_kernel(slots, send_slots, count, edges, flag_ref, weight_ref, partner_ref, other_ref, extra_ref, *refs):
    upper = flag_ref[1]
    refs = list(refs)
    values = refs[:count]
    outs = len(slots) if edges else len(slots) - 1
    made = refs[count : count + outs]
    rest = refs[count + outs :]
    to_sides, rest = rest[: 2 * edges], rest[2 * edges :]
    sends, (wide, extra_wide, middle, final_scr) = rest[: len(send_slots)], rest[len(send_slots) :]
    val_ref = values[-1]
    planes, rows, lanes = val_ref.shape
    if not edges:
        made = [*made, final_scr]
    add = [flag_ref[slot].astype(F32) for slot in slots]
    wide[planes : 2 * planes] = val_ref[...]
    sides = ((partner_ref, upper), (other_ref, 1 - upper))
    if len(slots) == 2:
        extra_wide[1 : planes + 1] = extra_ref[...]
        for ref, above in sides:
            wide[pl.ds(above * (2 * planes), planes)] = ref[0:planes]
            extra_wide[above * (planes + 1)] = ref[planes]
        coarse_advance(weight_ref, 0, wide.at[planes - 2 :], middle, planes + 2, extra_wide, add[0], rows, lanes)
        made[0][...] = middle[1 : planes + 1]
        coarse_advance(weight_ref, 1, middle, made[1], planes, extra_ref, add[1], rows, lanes)
    else:
        for ref, above in sides:
            wide[planes - 1 + above * (planes + 1)] = ref[0]
        coarse_advance(weight_ref, 1, wide.at[planes - 1 :], made[0], planes, extra_ref, add[0], rows, lanes)
    if edges:
        low, high = made[-1][0], made[-1][planes - 1]
        to_sides[0][0] = jnp.where(upper == 1, high, low)
        to_sides[1][0] = jnp.where(upper == 1, low, high)
    pick(flag_ref, send_slots, values + made, sends)


def base_kernel(iterate_ref, out_ref, rows_scr, fine_scr):
    planes, rows, lanes = iterate_ref.shape
    select, spread = pairing(lanes), spreading(lanes)
    for q in range(planes // 2):
        mean = natural_mean(iterate_ref[2 * q], iterate_ref[2 * q + 1], rows_scr, select)
        wide = split_dot(mean, spread)
        for j in range(lanes // 128):
            column = slice(128 * j, 128 * j + 128)
            fine_scr[j, pl.ds(0, rows // 2, 2), :] = wide[:, column]
            fine_scr[j, pl.ds(1, rows // 2, 2), :] = wide[:, column]
            for part in range(2):
                out_ref[2 * q + part, :, column] = iterate_ref[2 * q + part, :, column] - fine_scr[j]


def final_kernel(slots, flag_ref, base_ref, *refs):
    count = len(slots)
    pieces, out_ref, fine_scr, sum_scr, error_scr = refs[:count], *refs[count:]
    planes, rows, lanes = base_ref.shape
    spread = spreading(lanes)
    piece_rows = pieces[0].shape[1]
    tiles = piece_rows // 8
    sum_scr[...] = jnp.zeros(sum_scr.shape, F32)
    for slot, ref in zip(slots, pieces):
        side = flag_ref[slot]
        sum_scr[side] = sum_scr[side] + ref[...]
    for q in range(planes // 2):
        for j in range(lanes // 256):
            column = slice(128 * j, 128 * j + 128)
            error_scr[j] = jnp.zeros(error_scr.shape[1:], F32)
            for side in range(2):
                first = side * (rows // 2 - piece_rows)
                for i in range(tiles):
                    at = pl.ds(first + i, 8, tiles)
                    error_scr[j, at, :] = error_scr[j, at, :] + sum_scr[side, q, tile(i), column]
        error = jnp.concatenate([error_scr[j] for j in range(lanes // 256)], axis=1)
        wide = split_dot(error, spread)
        for j in range(lanes // 128):
            column = slice(128 * j, 128 * j + 128)
            fine_scr[j, pl.ds(0, rows // 2, 2), :] = wide[:, column]
            fine_scr[j, pl.ds(1, rows // 2, 2), :] = wide[:, column]
            for part in range(2):
                out_ref[2 * q + part, :, column] = base_ref[2 * q + part, :, column] + fine_scr[j]


def swap_pairs(count, first):
    pairs = []
    for i in range(first, count - 1, 2):
        pairs += [(i, i + 1), (i + 1, i)]
    return pairs


def roles(layers):
    last_group = layers // 2 - 1
    rows = []
    for t in range(layers):
        half, last = t % 2, int(t // 2 == last_group)
        adds = [int(number == (layers - 1 if last else 1)) for number in range(1, layers)]
        sends = []
        for shift in range(layers):
            k = (t + shift) % layers
            m = k if last else k - 1 - (t - half)
            sends.append(m if m >= 0 else -1)
        halves = [(t - shift) % layers % 2 for shift in range(layers)]
        rows.append([half, last, *adds, *sends, *halves])
    return rows


def local(initial, iterate, diffusivity):
    layers, slabs = lax.axis_size("tm"), lax.axis_size("space")
    t, s = lax.axis_index("tm"), lax.axis_index("space")
    planes, all_rows, lanes = initial.shape
    assert layers % 2 == 0 and slabs % 2 == 0 and planes == STEPS
    own_rows = all_rows // 2
    rows = own_rows + MARGIN
    coarse_rows, coarse_lanes = rows // 2, lanes // 2
    reach = planes // 2
    upper = 1 - s % 2
    field = iterate[0]

    def partner_swap(x):
        return lax.ppermute(x, "space", swap_pairs(slabs, 0))

    def other_swap(x):
        return lax.ppermute(x, "space", swap_pairs(slabs, 1))

    anywhere = pl.BlockSpec(memory_space=pl.ANY)
    in_hbm = pl.BlockSpec(memory_space=pltpu.HBM)
    c, to_row_partner = pl.pallas_call(
        slice_kernel,
        out_shape=(shape(planes, rows, lanes), shape(planes, own_rows, lanes)),
        in_specs=[in_hbm] * 2,
        out_specs=tuple(whole(2)),
        scratch_shapes=[pltpu.SemaphoreType.DMA((2,))],
        compiler_params=params(VMEM_LIMITS["slices"]),
        name="slices",
    )(diffusivity, field)
    row_pairs = swap_pairs(layers, 0)
    row_pairs.remove((layers - 1, layers - 2))
    received = lax.ppermute(to_row_partner, "tm", row_pairs)
    c_other = other_swap(c)
    c_partner = partner_swap(c)

    table = roles(layers)
    mine = jnp.asarray(table, jnp.int32)[t]
    flags = jnp.concatenate([mine[:1], jnp.reshape(upper, (1,)).astype(jnp.int32), mine[1:]])
    add_at, send_at, half_at = 3, 2 + layers, 2 + 2 * layers
    smem = pl.BlockSpec(memory_space=pltpu.SMEM)

    def cost(microseconds):
        return pl.CostEstimate(flops=int(microseconds * 4e6), bytes_accessed=0, transcendentals=0)

    fields = shape(2, reach, coarse_rows, coarse_lanes)
    blocks = lanes // 128
    prepared = pl.pallas_call(
        functools.partial(near_kernel, planes),
        out_shape=(
            *[shape(2 * planes - 1, rows, lanes)] * 7,
            shape(2, rows, lanes),
            shape(2 * reach, coarse_rows, coarse_lanes),
        ),
        in_specs=[smem] + [anywhere] * 2,
        out_specs=tuple(whole(9)),
        scratch_shapes=[
            VMEM((2 * planes, rows, lanes), F32),
            VMEM((2 * planes, blocks, rows, 128), F32),
            pltpu.SemaphoreType.DMA((2, blocks)),
        ],
        compiler_params=params(VMEM_LIMITS["near"]),
        cost_estimate=cost(6),
        name="near",
    )(flags, c, c_partner)
    own, to_partner, to_other, cc = pl.pallas_call(
        functools.partial(fine_kernel, planes),
        out_shape=(fields, fields, fields, shape(3 * reach, coarse_rows, coarse_lanes)),
        in_specs=[smem] + [anywhere] + [in_hbm] * 2 + [anywhere] + whole(9),
        out_specs=tuple(whole(4)),
        scratch_shapes=[
            VMEM((planes, blocks, rows, 128), F32),
            VMEM((2, planes, blocks, rows, 128), F32),
            VMEM((planes + 2, rows, lanes), F32),
            VMEM((7, planes + 1, rows, lanes), F32),
            VMEM((2, 3 * planes, rows, lanes), F32),
            VMEM((2, 3 * planes, rows, lanes), F32),
            VMEM((7, reach, coarse_rows, coarse_lanes), F32),
            VMEM((2 * reach, coarse_rows, coarse_lanes), F32),
            pltpu.SemaphoreType.DMA((blocks,)),
            pltpu.SemaphoreType.DMA((2, blocks)),
        ],
        compiler_params=params(VMEM_LIMITS["fine"]),
        name="fine",
    )(flags, c_other, field, initial, received, *prepared)

    base = pl.pallas_call(
        base_kernel,
        out_shape=shape(planes, all_rows, lanes),
        in_specs=whole(1),
        out_specs=pl.BlockSpec(memory_space=VMEM),
        scratch_shapes=[VMEM((coarse_lanes // 128, all_rows, 128), F32), VMEM((lanes // 128, all_rows, 128), F32)],
        compiler_params=params(VMEM_LIMITS["final"]),
        cost_estimate=cost(4),
        name="base",
    )(field)

    from_other = other_swap(to_other)
    from_partner = partner_swap(to_partner)
    plane = shape(1, coarse_rows, coarse_lanes)
    block = shape(reach, coarse_rows, coarse_lanes)
    thick = shape(reach + 1, coarse_rows, coarse_lanes)
    weights = pl.pallas_call(
        weight_kernel,
        out_shape=shape(7, 3 * reach - 2, coarse_rows, coarse_lanes),
        in_specs=whole(1),
        out_specs=pl.BlockSpec(memory_space=VMEM),
        compiler_params=params(VMEM_LIMITS["small"]),
        cost_estimate=cost(2),
        name="weights",
    )(cc)
    val, extra, to_partner, to_other = pl.pallas_call(
        sum_kernel,
        out_shape=(block, block, thick, thick),
        in_specs=[smem] + whole(3),
        out_specs=tuple(whole(4)),
        compiler_params=params(VMEM_LIMITS["small"]),
        name="gather",
    )(flags, own, from_partner, from_other)

    ready = [max(row[1 + layers + shift] for row in table) for shift in range(layers)]
    arrived = [None] * layers
    values = [val]
    sent = []
    while len(values) < layers:
        from_other = other_swap(to_other)
        from_partner = partner_swap(to_partner)
        for shift, send in sent:
            pairs = [
                (source, (source + shift) % layers)
                for source in range(layers)
                if table[source][1 + layers + shift] >= 0
            ]
            arrived[shift] = lax.ppermute(send, "tm", pairs) if shift else send
        count = len(values)
        steps = 2 if count == 1 and layers > 2 else 1
        more = count + steps < layers
        kept = steps if more else steps - 1
        slots = [add_at + count - 1 + n for n in range(steps)]
        shifts = [shift for shift in range(layers) if arrived[shift] is None and ready[shift] < count + steps]
        made = pl.pallas_call(
            functools.partial(chain_kernel, slots, [send_at + shift for shift in shifts], count, int(more)),
            out_shape=(*[block] * kept, *[plane] * (2 * more), *[block] * len(shifts)),
            in_specs=[smem] + whole(4 + count),
            out_specs=tuple(whole(kept + 2 * more + len(shifts))),
            scratch_shapes=[
                VMEM((3 * reach, coarse_rows, coarse_lanes), F32),
                VMEM((reach + 2, coarse_rows, coarse_lanes), F32),
                VMEM((reach + 2, coarse_rows, coarse_lanes), F32),
                VMEM((reach, coarse_rows, coarse_lanes), F32),
            ],
            compiler_params=params(VMEM_LIMITS["small"]),
        )(flags, weights, from_partner, from_other, extra, *values)
        values += made[:kept] if more else [None] * steps
        if more:
            to_partner, to_other = made[kept : kept + 2]
        sent = list(zip(shifts, made[kept + 2 * more :]))
    for shift, send in sent:
        pairs = [
            (source, (source + shift) % layers) for source in range(layers) if table[source][1 + layers + shift] >= 0
        ]
        arrived[shift] = lax.ppermute(send, "tm", pairs) if shift else send

    corrected = pl.pallas_call(
        functools.partial(final_kernel, [half_at + shift for shift in range(layers)]),
        out_shape=shape(planes, all_rows, lanes),
        in_specs=[smem] + whole(1 + layers),
        out_specs=pl.BlockSpec(memory_space=VMEM),
        scratch_shapes=[
            VMEM((lanes // 128, all_rows, 128), F32),
            VMEM((2, reach, coarse_rows, coarse_lanes), F32),
            VMEM((coarse_lanes // 128, all_rows // 2, 128), F32),
        ],
        compiler_params=params(VMEM_LIMITS["final"]),
        name="final",
    )(flags, base, *arrived)
    return corrected[None]


def solution(mesh):
    placed = (P("space", None, None), P("tm", "space", None, None), P("space", None, None))

    return jax.shard_map(local, mesh=mesh, in_specs=placed, out_specs=P("tm", "space", None, None), check_vma=False)
```
